256 devices in a mesh: leaf: 256 (over x, z, y, core).
Axes of the slice: x: 4, y: 4, z: 8, core: 2. Of those that a mesh axis runs over, the one named last changes fastest.
Arguments:
- right_side: float32 [262144, 128], P('leaf'), may hold values from -6 to 6
- diag_blocks: bfloat16 [256, 1024, 1024], P('leaf'), may hold values from -0.1875 to 0.1875
- row_bases: bfloat16 [256, 200, 1024], P('leaf'), may hold values from -0.4375 to 0.4375
- column_bases: bfloat16 [256, 200, 1024], P('leaf'), may hold values from -0.1875 to 0.1875
- transfer: bfloat16 [8, 2, 200, 200], replicated, may hold values from -0.375 to 0.375
- coupling: bfloat16 [8, 2, 200, 200], replicated, may hold values from -0.4375 to 0.4375
- inverse_blocks: bfloat16 [256, 1024, 1024], P('leaf'), may hold values from -0.1875 to 0.1875
- inverse_rows: bfloat16 [256, 200, 1024], P('leaf'), may hold values from -0.4375 to 0.4375
- inverse_columns: bfloat16 [256, 200, 1024], P('leaf'), may hold values from -0.1875 to 0.1875
- inverse_transfer: bfloat16 [8, 2, 200, 200], replicated, may hold values from -0.375 to 0.375
- inverse_coupling: bfloat16 [8, 2, 200, 200], replicated, may hold values from -0.4375 to 0.4375
Outputs:
- solution: float32 [262144, 128], P('leaf')
- hessenberg: float32 [4, 3, 128], replicated
The draws below stay inside these ranges and needn't reach their ends.
All inputs are finite; a program needn't handle non-finite values.
Results may differ from the reference program's by a relative error of at most 0.0003.
Values sent between devices are 32-bit elements; how exact they have to be, the bound alone decides.
A program may use at most 128 MiB of HBM per device.

```python
import jax
import jax.numpy as jnp
from jax import lax

LEAF = 1024
K = 200
NRHS = 128
ITERS = 3
LEVELS = 8
ORDER = 262144
N_LEAF = 256


def block_levels(key, dims, shards, smallest, high):
    def one(position, blocks):
        draws = jax.random.uniform(jax.random.fold_in(jax.random.fold_in(key, 6), position), (blocks,), jnp.float32, smallest / len(shards), high / len(shards))
        return jnp.repeat(jnp.exp(draws), dims[position] // blocks).reshape((-1,) + (1,) * (len(dims) - position - 1))

    level = one(*shards[0])
    for cut in shards[1:]:
        level = level * one(*cut)
    return level


def centred(rng, extent, scale, limit, shards=(), held_as=jnp.bfloat16):
    gain = block_levels(rng, extent, shards, -0.22, 0.18) if shards else 1.0
    result = jax.random.normal(rng, extent, jnp.float32) * scale * gain
    return jnp.minimum(jnp.maximum(result, -limit), limit).astype(held_as)


def setup_inputs(seed: int = 0) -> dict:
    splits = jax.random.split(jax.random.key(seed), 12)
    return {
        "right_side": centred(splits[0], (ORDER, NRHS), 1.0, 6.0, ((0, 256),), jnp.float32),
        "diag_blocks": centred(splits[1], (N_LEAF, LEAF, LEAF), LEAF ** -0.5, 0.1875, ((0, 256),)),
        "row_bases": centred(splits[2], (N_LEAF, K, LEAF), K ** -0.5, 0.4375, ((0, 256),)),
        "column_bases": centred(splits[3], (N_LEAF, K, LEAF), LEAF ** -0.5, 0.1875, ((0, 256),)),
        "transfer": centred(splits[4], (LEVELS, 2, K, K), (K * 7 // 5) ** -0.5, 0.375),
        "coupling": centred(splits[5], (LEVELS, 2, K, K), K ** -0.5, 0.4375),
        "inverse_blocks": centred(splits[6], (N_LEAF, LEAF, LEAF), LEAF ** -0.5, 0.1875, ((0, 256),)),
        "inverse_rows": centred(splits[7], (N_LEAF, K, LEAF), K ** -0.5, 0.4375, ((0, 256),)),
        "inverse_columns": centred(splits[8], (N_LEAF, K, LEAF), LEAF ** -0.5, 0.1875, ((0, 256),)),
        "inverse_transfer": centred(splits[9], (LEVELS, 2, K, K), (K * 7 // 5) ** -0.5, 0.375),
        "inverse_coupling": centred(splits[10], (LEVELS, 2, K, K), K ** -0.5, 0.4375),
    }


EPSILON = 1e-06

def transpose_apply(matrix, vectors):
    return lax.dot_general(matrix, vectors, (((0,), (0,)), ((), ())), precision=lax.Precision.HIGHEST)

def hss_apply(vectors, blocks, row_side, column_side, transfer, coupling):
    leaves = blocks.shape[0]
    leaf_width = blocks.shape[1]
    basis_rank = transfer.shape[2]
    columns = vectors.shape[1]
    levels = transfer.shape[0]
    pieces = vectors.reshape(leaves, leaf_width, columns)

    def leaf_terms(bundle):
        square, column_base, portion = bundle
        direct = jnp.dot(square.astype(jnp.float32), portion, precision=lax.Precision.HIGHEST)
        summary = jnp.dot(column_base.astype(jnp.float32), portion, precision=lax.Precision.HIGHEST)
        return (direct, summary)
    direct, summary = lax.map(leaf_terms, (blocks, column_side, pieces))
    siblings = []
    for height in range(levels):
        paired = summary.reshape(-1, 2, basis_rank, columns)
        siblings.append(paired[:, ::-1])
        if height < levels - 1:
            translate = transfer[height].astype(jnp.float32)
            summary = jnp.einsum('ij,nir->njr', translate[0], paired[:, 0], precision=lax.Precision.HIGHEST) + jnp.einsum('ij,nir->njr', translate[1], paired[:, 1], precision=lax.Precision.HIGHEST)
    downward = None
    for height in reversed(range(levels)):
        bridge = coupling[height].astype(jnp.float32)
        incoming = jnp.einsum('sij,psjr->psir', bridge, siblings[height], precision=lax.Precision.HIGHEST)
        if downward is not None:
            translate = transfer[height].astype(jnp.float32)
            incoming = incoming + jnp.einsum('sij,pjr->psir', translate, downward, precision=lax.Precision.HIGHEST)
        downward = incoming.reshape(-1, basis_rank, columns)

    def leaf_out(bundle):
        row_base, portion = bundle
        return transpose_apply(row_base.astype(jnp.float32), portion)
    spread = lax.map(leaf_out, (row_side, downward))
    return (direct + spread).reshape(leaves * leaf_width, columns)

def least_squares(entries, beta_first):
    unknowns = len(entries[0])
    matrix = [list(line) for line in entries]
    target = [beta_first] + [jnp.zeros_like(beta_first) for column in range(unknowns)]
    for column in range(unknowns):
        upper_entry = matrix[column][column]
        lower_entry = matrix[column + 1][column]
        radius = jnp.sqrt(upper_entry * upper_entry + lower_entry * lower_entry)
        cosine = upper_entry / radius
        sine_value = lower_entry / radius
        for following in range(column, unknowns):
            top_value = matrix[column][following]
            bottom_value = matrix[column + 1][following]
            matrix[column][following] = cosine * top_value + sine_value * bottom_value
            matrix[column + 1][following] = cosine * bottom_value - sine_value * top_value
        top_value = target[column]
        bottom_value = target[column + 1]
        target[column] = cosine * top_value + sine_value * bottom_value
        target[column + 1] = cosine * bottom_value - sine_value * top_value
    coefficients = [None] * unknowns
    for current_row in reversed(range(unknowns)):
        remainder = target[current_row]
        for following in range(current_row + 1, unknowns):
            remainder = remainder - matrix[current_row][following] * coefficients[following]
        coefficients[current_row] = remainder / matrix[current_row][current_row]
    return coefficients

def reference(right_side, diag_blocks, row_bases, column_bases, transfer, coupling, inverse_blocks, inverse_rows, inverse_columns, inverse_transfer, inverse_coupling):
    beta_first = jnp.sqrt(lax.optimization_barrier(jnp.sum(right_side * right_side, axis=0)) + EPSILON)
    krylov = [right_side / beta_first]
    images = []
    zero_row = jnp.zeros_like(beta_first)
    entries = [[zero_row for column in range(ITERS)] for line in range(ITERS + 1)]
    for column in range(ITERS):
        image = hss_apply(krylov[column], inverse_blocks, inverse_rows, inverse_columns, inverse_transfer, inverse_coupling)
        images.append(image)
        mixed = hss_apply(image, diag_blocks, row_bases, column_bases, transfer, coupling)
        correction = jnp.zeros_like(mixed)
        for earlier in range(column + 1):
            product = lax.optimization_barrier(jnp.sum(krylov[earlier] * mixed, axis=0))
            entries[earlier][column] = product
            correction = correction + product * krylov[earlier]
        update = mixed - correction
        norm_value = jnp.sqrt(lax.optimization_barrier(jnp.sum(update * update, axis=0)) + EPSILON)
        entries[column + 1][column] = norm_value
        krylov.append(update / norm_value)
    coefficients = least_squares(entries, beta_first)
    solution = jnp.zeros_like(right_side)
    for column in range(ITERS):
        solution = solution + coefficients[column] * images[column]
    hessenberg = jnp.stack([jnp.stack(line) for line in entries])
    return (solution, hessenberg)
```

```python
import jax
import jax.numpy as jnp
from jax import lax
from jax.experimental import pallas as pl
from jax.experimental.pallas import tpu as pltpu
from jax.sharding import PartitionSpec as P

F32 = jnp.float32
BF16 = jnp.bfloat16
MESH = pl.DeviceIdType.MESH

ITERS = 3
EPSILON = 1e-06
WIDTH = 1024
RANK = 200
LANES = 256
COLS = 128
GROUP = 8
DEEP = 8
OUTER = 4
SLICE = COLS // GROUP
LEVELS = 8
TILE = 256

NT = (((1,), (1,)), ((), ()))
NN = (((1,), (0,)), ((), ()))


def halves(x):
    high = x.astype(BF16)
    return high, (x - high.astype(F32)).astype(BF16)


def product_rows(x, weight, dims):
    rows = x.shape[0]
    high, low = halves(x)
    both = lax.dot_general(
        jnp.concatenate([high, low], axis=0), weight, dims, preferred_element_type=F32
    )
    return both[:rows] + both[rows:]


def pairs(x):
    count = x.shape[0] // 2
    split = x.reshape(count, 2, SLICE, LANES)
    left = split[:, 0].reshape(count * SLICE, LANES)
    right = split[:, 1].reshape(count * SLICE, LANES)
    return left, right


def least_squares(entries, beta_first):
    unknowns = len(entries[0])
    matrix = [list(line) for line in entries]
    target = [beta_first] + [jnp.zeros_like(beta_first) for column in range(unknowns)]
    for column in range(unknowns):
        upper_entry = matrix[column][column]
        lower_entry = matrix[column + 1][column]
        radius = jnp.sqrt(upper_entry * upper_entry + lower_entry * lower_entry)
        cosine = upper_entry / radius
        sine_value = lower_entry / radius
        for following in range(column, unknowns):
            top_value = matrix[column][following]
            bottom_value = matrix[column + 1][following]
            matrix[column][following] = cosine * top_value + sine_value * bottom_value
            matrix[column + 1][following] = cosine * bottom_value - sine_value * top_value
        top_value = target[column]
        bottom_value = target[column + 1]
        target[column] = cosine * top_value + sine_value * bottom_value
        target[column + 1] = cosine * bottom_value - sine_value * top_value
    coefficients = [None] * unknowns
    for current_row in reversed(range(unknowns)):
        remainder = target[current_row]
        for following in range(current_row + 1, unknowns):
            remainder = remainder - matrix[current_row][following] * coefficients[following]
        coefficients[current_row] = remainder / matrix[current_row][current_row]
    return coefficients


def kernel(
    rhs_hbm,
    ea_hbm,
    pa_hbm,
    qa_hbm,
    ta_hbm,
    ca_hbm,
    em_hbm,
    pm_hbm,
    qm_hbm,
    tm_hbm,
    cm_hbm,
    sol_ref,
    hess_ref,
    blocks,
    rows_raw,
    rows_t,
    cols_side,
    trans_raw,
    coup_raw,
    trans,
    coup,
    basis,
    images,
    mixed,
    direct,
    stacked,
    a_send,
    a_slot,
    z_send,
    z_slot,
    x_send,
    x_slot,
    d_send,
    d_slot,
    c1_ref,
    c2_ref,
    c4_ref,
    c5_ref,
    bridge0,
    bridge1,
    bridge2,
    r_send,
    ra_slot,
    rz_slot,
    rx_slot,
    hs,
    load_sem,
    a_ss,
    a_rs,
    z_ss,
    z_rs,
    x_ss,
    x_rs,
    d_ss,
    d_rs,
    ra_ss,
    ra_rs,
    rz_ss,
    rz_rs,
    rx_ss,
    rx_rs,
):
    me = lax.axis_index("leaf")
    g = me % GROUP
    zc = (me // GROUP) % DEEP
    xc = me // (GROUP * DEEP)

    def to_group(k):
        return (me // GROUP) * GROUP + (g + k) % GROUP

    def to_deep(k):
        return xc * (GROUP * DEEP) + ((zc + k) % DEEP) * GROUP + g

    def to_outer(k):
        return ((xc + k) % OUTER) * (GROUP * DEEP) + me % (GROUP * DEEP)

    def load(src, dst, which):
        return pltpu.make_async_copy(src, dst, load_sem.at[which])

    loads = {
        "rhs": load(rhs_hbm, basis.at[0], 0),
        "q0": load(qm_hbm.at[0], cols_side.at[0], 1),
        "t0": load(tm_hbm, trans_raw.at[0], 2),
        "e0": load(em_hbm.at[0], blocks.at[0], 3),
        "c0": load(cm_hbm, coup_raw.at[0], 4),
        "p0": load(pm_hbm.at[0], rows_raw.at[0], 5),
        "q1": load(qa_hbm.at[0], cols_side.at[1], 6),
        "t1": load(ta_hbm, trans_raw.at[1], 7),
        "e1": load(ea_hbm.at[0], blocks.at[1], 8),
        "c1": load(ca_hbm, coup_raw.at[1], 9),
        "p1": load(pa_hbm.at[0], rows_raw.at[1], 10),
    }
    for item in loads.values():
        item.start()

    barrier = pltpu.get_barrier_semaphore()
    peers = [to_group(k) for k in range(1, GROUP)]
    peers += [to_deep(k) for k in range(1, DEEP)]
    peers += [to_outer(k) for k in range(1, OUTER)]
    for peer in peers:
        pl.semaphore_signal(barrier, inc=1, device_id=(peer,), device_id_type=MESH)

    for i in range(1, ITERS + 1):
        basis[i] = jnp.zeros((WIDTH, COLS), F32)

    def pad_tree(op):
        loads["t%d" % op].wait()
        loads["c%d" % op].wait()
        edge = ((0, LANES - RANK), (0, LANES - RANK))

        def one(h, carry):
            for s in range(2):
                trans[op, h, s * LANES : (s + 1) * LANES, :] = jnp.pad(trans_raw[op, h, s], edge)
                coup[op, h, s] = jnp.pad(coup_raw[op, h, s], edge)
            return carry

        lax.fori_loop(0, LEVELS, one, 0)

    def turn_rows(op):
        loads["p%d" % op].wait()
        for t in range(WIDTH // TILE):
            part = rows_raw[op, :, t * TILE : (t + 1) * TILE].astype(F32)
            part = jnp.pad(part, ((0, LANES - RANK), (0, 0)))
            rows_t[op, t * TILE : (t + 1) * TILE, :] = part.T.astype(BF16)

    def copies(count, coord, target, source, slot, send_sem, recv_sem):
        out = []
        arrive = []
        for k in range(1, count):
            out.append(
                pltpu.make_async_remote_copy(
                    src_ref=source(k),
                    dst_ref=slot.at[coord],
                    send_sem=send_sem.at[k - 1],
                    recv_sem=recv_sem.at[k - 1],
                    device_id=(target(k),),
                    device_id_type=MESH,
                )
            )
            arrive.append(
                pltpu.make_async_remote_copy(
                    src_ref=source(k),
                    dst_ref=slot.at[(coord + count - k) % count],
                    send_sem=send_sem.at[k - 1],
                    recv_sem=recv_sem.at[k - 1],
                    device_id=(target(k),),
                    device_id_type=MESH,
                )
            )
        return out, arrive

    def start(group):
        for c in group[0]:
            c.start()

    def arrived(group):
        for c in group[1]:
            c.wait_recv()

    def left_device(group):
        for c in group[0]:
            c.wait_send()

    def upward(x, op, h):
        left, right = pairs(x)
        joined = product_rows(
            jnp.concatenate([left, right], axis=1), trans[op, h], NN
        )
        return joined.reshape(x.shape[0] // 2, SLICE, LANES)

    def bridges(x, op, h):
        left, right = pairs(x)
        count = x.shape[0] // 2
        first = product_rows(right, coup[op, h, 0], NT).reshape(count, 1, SLICE, LANES)
        second = product_rows(left, coup[op, h, 1], NT).reshape(count, 1, SLICE, LANES)
        return jnp.concatenate([first, second], axis=1).reshape(x.shape)

    def downward(bridge, above, op, h):
        count = above.shape[0]
        moved = product_rows(above.reshape(count * SLICE, LANES), trans[op, h], NT)
        first = moved[:, :LANES].reshape(count, 1, SLICE, LANES)
        second = moved[:, LANES:].reshape(count, 1, SLICE, LANES)
        return bridge + jnp.concatenate([first, second], axis=1).reshape(bridge.shape)

    def own_bridge(values, own, op, h):
        side = own % 2
        return product_rows(values(own + 1 - 2 * side), coup[op, h, side], NT)

    def own_down(above, own, op, h):
        side = own % 2
        weight = trans[op, h, pl.ds(pl.multiple_of(side * LANES, LANES), LANES), :]
        return product_rows(above, weight, NT)

    def tree_apply(op, j, source, target):
        if op == 0:

            @pl.when(j == 0)
            def _():
                loads["rhs"].wait()

        @pl.when(j == 0)
        def _():
            loads["q%d" % op].wait()

        high, low = halves(source())
        stacked[:, :COLS] = high
        stacked[:, COLS:] = low
        both = jnp.dot(cols_side[op], stacked[...], preferred_element_type=F32)
        leaf = both[:, :COLS] + both[:, COLS:]
        leaf = jnp.pad(leaf, ((0, LANES - RANK), (0, 0)))
        a_send[op] = leaf.T.reshape(GROUP, SLICE, LANES)
        if op == 0:

            @pl.when(j == 0)
            def _():
                pl.semaphore_wait(barrier, len(peers))

        a = copies(
            GROUP, g, to_group, lambda k: a_send.at[op, (g + k) % GROUP],
            a_slot.at[op], a_ss.at[op], a_rs.at[op],
        )
        start(a)
        a_slot[op, g] = a_send[op, g]

        @pl.when(j == 0)
        def _():
            pad_tree(op)
            loads["e%d" % op].wait()

        for t in range(WIDTH // TILE):
            both = jnp.dot(
                blocks[op, t * TILE : (t + 1) * TILE, :], stacked[...],
                preferred_element_type=F32,
            )
            direct[t * TILE : (t + 1) * TILE, :] = both[:, :COLS] + both[:, COLS:]

        arrived(a)
        c1 = upward(a_slot[op], op, 0)
        c1_ref[...] = c1
        c2 = upward(c1, op, 1)
        c2_ref[...] = c2
        c3 = upward(c2, op, 2)
        z_send[op] = c3[0]
        z = copies(
            DEEP, zc, to_deep, lambda k: z_send.at[op],
            z_slot.at[op], z_ss.at[op], z_rs.at[op],
        )
        start(z)
        z_slot[op, zc] = c3[0]
        bridge0[...] = bridges(a_slot[op], op, 0)
        bridge1[...] = bridges(c1_ref[...], op, 1)
        bridge2[...] = bridges(c2_ref[...], op, 2)

        @pl.when(j == 0)
        def _():
            turn_rows(op)

        arrived(z)
        c4 = upward(z_slot[op], op, 3)
        c4_ref[...] = c4
        c5 = upward(c4, op, 4)
        c5_ref[...] = c5
        c6 = upward(c5, op, 5)
        x_send[op] = c6[0]
        x = copies(
            OUTER, xc, to_outer, lambda k: x_send.at[op],
            x_slot.at[op], x_ss.at[op], x_rs.at[op],
        )
        start(x)
        x_slot[op, xc] = c6[0]
        near3 = own_bridge(lambda n: z_slot[op, n], zc, op, 3)
        near4 = own_bridge(lambda n: c4_ref[n], zc // 2, op, 4)
        near5 = own_bridge(lambda n: c5_ref[n], zc // 4, op, 5)
        arrived(x)
        c7 = upward(x_slot[op], op, 6)
        near6 = own_bridge(lambda n: x_slot[op, n], xc, op, 6)
        c4_ref[0:2] = c7
        d7 = own_bridge(lambda n: c4_ref[n], xc // 2, op, 7)
        d6 = near6 + own_down(d7, xc, op, 6)
        d5 = near5 + own_down(d6, zc // 4, op, 5)
        d4 = near4 + own_down(d5, zc // 2, op, 4)
        d3 = near3 + own_down(d4, zc, op, 3)
        d2 = downward(bridge2[...], d3.reshape(1, SLICE, LANES), op, 2)
        d1 = downward(bridge1[...], d2, op, 1)
        d0 = downward(bridge0[...], d1, op, 0)
        d_send[op] = d0
        d = copies(
            GROUP, g, to_group, lambda k: d_send.at[op, (g + k) % GROUP],
            d_slot.at[op], d_ss.at[op], d_rs.at[op],
        )
        start(d)
        d_slot[op, g] = d_send[op, g]
        left_device(a)
        left_device(z)
        left_device(x)
        arrived(d)
        high, low = halves(d_slot[op].reshape(COLS, LANES))
        spread = jnp.concatenate([high, low], axis=0)
        for t in range(WIDTH // TILE):
            part = slice(t * TILE, (t + 1) * TILE)
            both = lax.dot_general(rows_t[op, part, :], spread, NT, preferred_element_type=F32)
            target(part, direct[part, :] + both[:, :COLS] + both[:, COLS:])
        left_device(d)

    def total_of(which, rows):
        r_send[which, 0] = rows
        ra = copies(
            GROUP, g, to_group, lambda k: r_send.at[which, 0],
            ra_slot.at[which], ra_ss.at[which], ra_rs.at[which],
        )
        start(ra)
        ra_slot[which, g] = rows
        arrived(ra)
        one = jnp.sum(ra_slot[which], axis=0)
        r_send[which, 1] = one
        rz = copies(
            DEEP, zc, to_deep, lambda k: r_send.at[which, 1],
            rz_slot.at[which], rz_ss.at[which], rz_rs.at[which],
        )
        start(rz)
        rz_slot[which, zc] = one
        arrived(rz)
        two = jnp.sum(rz_slot[which], axis=0)
        r_send[which, 2] = two
        rx = copies(
            OUTER, xc, to_outer, lambda k: r_send.at[which, 2],
            rx_slot.at[which], rx_ss.at[which], rx_rs.at[which],
        )
        start(rx)
        rx_slot[which, xc] = two
        arrived(rx)
        left_device(ra)
        left_device(rz)
        left_device(rx)
        return jnp.sum(rx_slot[which], axis=0)

    def column_sum(x):
        return jnp.sum(x, axis=0, keepdims=True)

    def iteration(j, carry):
        def to_image(part, value):
            images[j, part, :] = value

        def to_mixed(part, value):
            mixed[part, :] = value

        tree_apply(0, j, lambda: basis[j], to_image)
        tree_apply(1, j, lambda: images[j], to_mixed)
        partial = [column_sum(basis[i] * mixed[...]) for i in range(ITERS)]
        partial.append(column_sum(basis[j] * basis[j]))
        partial.append(jnp.zeros((8 - len(partial), COLS), F32))
        totals = total_of(0, jnp.concatenate(partial, axis=0))
        norm = jnp.sqrt(totals[ITERS : ITERS + 1] + EPSILON)
        hs[j * (ITERS + 1)] = norm
        scale = 1.0 / norm
        basis[j] = basis[j] * scale
        images[j] = images[j] * scale
        update = mixed[...] * scale
        for i in range(ITERS):
            entry = totals[i : i + 1] / norm
            entry = jnp.where(i == j, entry / norm, entry)
            entry = jnp.where(i > j, jnp.zeros_like(entry), entry)
            hs[j * (ITERS + 1) + 1 + i] = entry
            update = update - entry * basis[i]
        basis[j + 1] = update
        return carry

    lax.fori_loop(0, ITERS, iteration, 0)

    last = column_sum(basis[ITERS] * basis[ITERS])
    totals = total_of(1, jnp.concatenate([last, jnp.zeros((7, COLS), F32)], axis=0))
    last_norm = jnp.sqrt(totals[0:1] + EPSILON)
    zero = jnp.zeros((1, COLS), F32)
    entries = [[zero for column in range(ITERS)] for line in range(ITERS + 1)]
    for column in range(ITERS):
        for line in range(column + 1):
            entries[line][column] = hs[column * (ITERS + 1) + 1 + line]
        if column + 1 < ITERS:
            entries[column + 1][column] = hs[(column + 1) * (ITERS + 1)]
        else:
            entries[column + 1][column] = last_norm
    weights = least_squares(entries, hs[0])
    sol_ref[...] = weights[0] * images[0] + weights[1] * images[1] + weights[2] * images[2]
    for line in range(ITERS + 1):
        hess_ref[line] = jnp.concatenate(entries[line], axis=0)


def solution(mesh):
    dma = pltpu.SemaphoreType.DMA
    tree = (2, GROUP, SLICE, LANES)
    scratch = [
        pltpu.VMEM((2, WIDTH, WIDTH), BF16),
        pltpu.VMEM((2, RANK, WIDTH), BF16),
        pltpu.VMEM((2, WIDTH, LANES), BF16),
        pltpu.VMEM((2, RANK, WIDTH), BF16),
        pltpu.VMEM((2, LEVELS, 2, RANK, RANK), BF16),
        pltpu.VMEM((2, LEVELS, 2, RANK, RANK), BF16),
        pltpu.VMEM((2, LEVELS, 2 * LANES, LANES), BF16),
        pltpu.VMEM((2, LEVELS, 2, LANES, LANES), BF16),
        pltpu.VMEM((ITERS + 1, WIDTH, COLS), F32),
        pltpu.VMEM((ITERS, WIDTH, COLS), F32),
        pltpu.VMEM((WIDTH, COLS), F32),
        pltpu.VMEM((WIDTH, COLS), F32),
        pltpu.VMEM((WIDTH, 2 * COLS), BF16),
        pltpu.VMEM(tree, F32),
        pltpu.VMEM(tree, F32),
        pltpu.VMEM((2, SLICE, LANES), F32),
        pltpu.VMEM((2, DEEP, SLICE, LANES), F32),
        pltpu.VMEM((2, SLICE, LANES), F32),
        pltpu.VMEM((2, OUTER, SLICE, LANES), F32),
        pltpu.VMEM(tree, F32),
        pltpu.VMEM(tree, F32),
        pltpu.VMEM((4, SLICE, LANES), F32),
        pltpu.VMEM((2, SLICE, LANES), F32),
        pltpu.VMEM((4, SLICE, LANES), F32),
        pltpu.VMEM((2, SLICE, LANES), F32),
        pltpu.VMEM((8, SLICE, LANES), F32),
        pltpu.VMEM((4, SLICE, LANES), F32),
        pltpu.VMEM((2, SLICE, LANES), F32),
        pltpu.VMEM((2, 3, 8, COLS), F32),
        pltpu.VMEM((2, GROUP, 8, COLS), F32),
        pltpu.VMEM((2, DEEP, 8, COLS), F32),
        pltpu.VMEM((2, OUTER, 8, COLS), F32),
        pltpu.VMEM((ITERS * (ITERS + 1), 1, COLS), F32),
        dma((11,)),
        dma((2, GROUP - 1)),
        dma((2, GROUP - 1)),
        dma((2, DEEP - 1)),
        dma((2, DEEP - 1)),
        dma((2, OUTER - 1)),
        dma((2, OUTER - 1)),
        dma((2, GROUP - 1)),
        dma((2, GROUP - 1)),
        dma((2, GROUP - 1)),
        dma((2, GROUP - 1)),
        dma((2, DEEP - 1)),
        dma((2, DEEP - 1)),
        dma((2, OUTER - 1)),
        dma((2, OUTER - 1)),
    ]

    def on_device(*args):
        return pl.pallas_call(
            kernel,
            out_shape=(
                jax.ShapeDtypeStruct((WIDTH, COLS), F32),
                jax.ShapeDtypeStruct((ITERS + 1, ITERS, COLS), F32),
            ),
            in_specs=[pl.BlockSpec(memory_space=pl.ANY)] * 11,
            out_specs=[pl.BlockSpec(memory_space=pltpu.VMEM)] * 2,
            scratch_shapes=scratch,
            compiler_params=pltpu.CompilerParams(
                collective_id=0, has_side_effects=True, vmem_limit_bytes=60 * 2**20
            ),
        )(*args)

    leaf = P("leaf", None)
    block = P("leaf", None, None)
    in_specs = (leaf, block, block, block, P(), P(), block, block, block, P(), P())
    return jax.shard_map(
        on_device, mesh=mesh, in_specs=in_specs, out_specs=(leaf, P()), check_vma=False
    )
```

```python
import jax
import jax.numpy as jnp
from jax import lax
from jax.experimental import pallas as pl
from jax.experimental.pallas import tpu as pltpu
from jax.sharding import PartitionSpec as P

F32 = jnp.float32
BF16 = jnp.bfloat16
MESH = pl.DeviceIdType.MESH

ITERS = 3
EPSILON = 1e-06
WIDTH = 1024
RANK = 200
LANES = 256
COLS = 128
GROUP = 8
DEEP = 8
OUTER = 4
SLICE = COLS // GROUP
LEVELS = 8
TILE = 256

NT = (((1,), (1,)), ((), ()))
NN = (((1,), (0,)), ((), ()))


def halves(x):
    high = x.astype(BF16)
    return high, (x - high.astype(F32)).astype(BF16)


def product_rows(x, weight, dims):
    rows = x.shape[0]
    high, low = halves(x)
    both = lax.dot_general(
        jnp.concatenate([high, low], axis=0), weight, dims, preferred_element_type=F32
    )
    return both[:rows] + both[rows:]


def pairs(x):
    count = x.shape[0] // 2
    split = x.reshape(count, 2, SLICE, LANES)
    left = split[:, 0].reshape(count * SLICE, LANES)
    right = split[:, 1].reshape(count * SLICE, LANES)
    return left, right


def least_squares(entries, beta_first):
    unknowns = len(entries[0])
    matrix = [list(line) for line in entries]
    target = [beta_first] + [jnp.zeros_like(beta_first) for column in range(unknowns)]
    for column in range(unknowns):
        upper_entry = matrix[column][column]
        lower_entry = matrix[column + 1][column]
        radius = jnp.sqrt(upper_entry * upper_entry + lower_entry * lower_entry)
        cosine = upper_entry / radius
        sine_value = lower_entry / radius
        for following in range(column, unknowns):
            top_value = matrix[column][following]
            bottom_value = matrix[column + 1][following]
            matrix[column][following] = cosine * top_value + sine_value * bottom_value
            matrix[column + 1][following] = cosine * bottom_value - sine_value * top_value
        top_value = target[column]
        bottom_value = target[column + 1]
        target[column] = cosine * top_value + sine_value * bottom_value
        target[column + 1] = cosine * bottom_value - sine_value * top_value
    coefficients = [None] * unknowns
    for current_row in reversed(range(unknowns)):
        remainder = target[current_row]
        for following in range(current_row + 1, unknowns):
            remainder = remainder - matrix[current_row][following] * coefficients[following]
        coefficients[current_row] = remainder / matrix[current_row][current_row]
    return coefficients


def kernel(
    rhs_hbm,
    ea_hbm,
    pa_hbm,
    qa_hbm,
    ta_hbm,
    ca_hbm,
    em_hbm,
    pm_hbm,
    qm_hbm,
    tm_hbm,
    cm_hbm,
    sol_ref,
    hess_ref,
    blocks,
    rows_raw,
    rows_t,
    cols_side,
    trans_raw,
    coup_raw,
    trans,
    coup,
    basis,
    images,
    mixed,
    direct,
    stacked,
    a_send,
    a_slot,
    z_send,
    z_slot,
    x_send,
    x_slot,
    d_send,
    d_slot,
    c1_ref,
    c2_ref,
    c4_ref,
    c5_ref,
    bridge0,
    bridge1,
    bridge2,
    r_send,
    ra_slot,
    rz_slot,
    rx_slot,
    hs,
    load_sem,
    a_ss,
    a_rs,
    z_ss,
    z_rs,
    x_ss,
    x_rs,
    d_ss,
    d_rs,
    ra_ss,
    ra_rs,
    rz_ss,
    rz_rs,
    rx_ss,
    rx_rs,
):
    me = lax.axis_index("leaf")
    g = me % GROUP
    zc = (me // GROUP) % DEEP
    xc = me // (GROUP * DEEP)

    def to_group(k):
        return (me // GROUP) * GROUP + (g + k) % GROUP

    def to_deep(k):
        return xc * (GROUP * DEEP) + ((zc + k) % DEEP) * GROUP + g

    def to_outer(k):
        return ((xc + k) % OUTER) * (GROUP * DEEP) + me % (GROUP * DEEP)

    def load(src, dst, which):
        return pltpu.make_async_copy(src, dst, load_sem.at[which])

    loads = {
        "rhs": load(rhs_hbm, mixed, 0),
        "q0": load(qm_hbm.at[0], cols_side.at[0], 1),
        "t0": load(tm_hbm, trans_raw.at[0], 2),
        "e0": load(em_hbm.at[0], blocks.at[0], 3),
        "c0": load(cm_hbm, coup_raw.at[0], 4),
        "p0": load(pm_hbm.at[0], rows_raw.at[0], 5),
        "q1": load(qa_hbm.at[0], cols_side.at[1], 6),
        "t1": load(ta_hbm, trans_raw.at[1], 7),
        "e1": load(ea_hbm.at[0], blocks.at[1], 8),
        "c1": load(ca_hbm, coup_raw.at[1], 9),
        "p1": load(pa_hbm.at[0], rows_raw.at[1], 10),
    }
    for item in loads.values():
        item.start()

    barrier = pltpu.get_barrier_semaphore()
    peers = [to_group(k) for k in range(1, GROUP)]
    peers += [to_deep(k) for k in range(1, DEEP)]
    peers += [to_outer(k) for k in range(1, OUTER)]
    for peer in peers:
        pl.semaphore_signal(barrier, inc=1, device_id=(peer,), device_id_type=MESH)

    for i in range(1, ITERS):
        basis[i] = jnp.zeros((WIDTH, COLS), F32)
        images[i] = jnp.zeros((WIDTH, COLS), F32)

    def pad_tree(op):
        loads["t%d" % op].wait()
        loads["c%d" % op].wait()
        edge = ((0, LANES - RANK), (0, LANES - RANK))

        def one(h, carry):
            for s in range(2):
                trans[op, h, s * LANES : (s + 1) * LANES, :] = jnp.pad(trans_raw[op, h, s], edge)
                coup[op, h, s] = jnp.pad(coup_raw[op, h, s], edge)
            return carry

        lax.fori_loop(0, LEVELS, one, 0)

    def turn_rows(op):
        loads["p%d" % op].wait()
        for t in range(WIDTH // TILE):
            part = rows_raw[op, :, t * TILE : (t + 1) * TILE].astype(F32)
            part = jnp.pad(part, ((0, LANES - RANK), (0, 0)))
            rows_t[op, t * TILE : (t + 1) * TILE, :] = part.T.astype(BF16)

    def copies(count, coord, target, source, slot, send_sem, recv_sem):
        out = []
        arrive = []
        for k in range(1, count):
            out.append(
                pltpu.make_async_remote_copy(
                    src_ref=source(k),
                    dst_ref=slot.at[coord],
                    send_sem=send_sem.at[k - 1],
                    recv_sem=recv_sem.at[k - 1],
                    device_id=(target(k),),
                    device_id_type=MESH,
                )
            )
            arrive.append(
                pltpu.make_async_remote_copy(
                    src_ref=source(k),
                    dst_ref=slot.at[(coord + count - k) % count],
                    send_sem=send_sem.at[k - 1],
                    recv_sem=recv_sem.at[k - 1],
                    device_id=(target(k),),
                    device_id_type=MESH,
                )
            )
        return out, arrive

    def start(group):
        for c in group[0]:
            c.start()

    def arrived(group):
        for c in group[1]:
            c.wait_recv()

    def left_device(group):
        for c in group[0]:
            c.wait_send()

    def upward(x, op, h):
        left, right = pairs(x)
        joined = product_rows(
            jnp.concatenate([left, right], axis=1), trans[op, h], NN
        )
        return joined.reshape(x.shape[0] // 2, SLICE, LANES)

    def bridges(x, op, h):
        left, right = pairs(x)
        count = x.shape[0] // 2
        first = product_rows(right, coup[op, h, 0], NT).reshape(count, 1, SLICE, LANES)
        second = product_rows(left, coup[op, h, 1], NT).reshape(count, 1, SLICE, LANES)
        return jnp.concatenate([first, second], axis=1).reshape(x.shape)

    def downward(bridge, above, op, h):
        count = above.shape[0]
        moved = product_rows(above.reshape(count * SLICE, LANES), trans[op, h], NT)
        first = moved[:, :LANES].reshape(count, 1, SLICE, LANES)
        second = moved[:, LANES:].reshape(count, 1, SLICE, LANES)
        return bridge + jnp.concatenate([first, second], axis=1).reshape(bridge.shape)

    def own_bridge(values, own, op, h):
        side = own % 2
        return product_rows(values(own + 1 - 2 * side), coup[op, h, side], NT)

    def own_down(above, own, op, h):
        side = own % 2
        weight = trans[op, h, pl.ds(pl.multiple_of(side * LANES, LANES), LANES), :]
        return product_rows(above, weight, NT)

    def riding(x):
        lane = lax.broadcasted_iota(jnp.int32, (SLICE, LANES - COLS), 1)
        total = jnp.sum(x[:, :, COLS:], axis=0)
        total = jnp.where(lane >= RANK - COLS, total, jnp.zeros_like(total))
        return jnp.concatenate([jnp.zeros((SLICE, COLS), F32), total], axis=1)

    def tree_apply(op, j, source, target, sums=None):
        if op == 0:

            @pl.when(j == 0)
            def _():
                loads["rhs"].wait()
                basis[0] = mixed[...]

        @pl.when(j == 0)
        def _():
            loads["q%d" % op].wait()

        high, low = halves(source())
        stacked[:, :COLS] = high
        stacked[:, COLS:] = low
        both = jnp.dot(cols_side[op], stacked[...], preferred_element_type=F32)
        leaf = both[:, :COLS] + both[:, COLS:]
        rest = LANES - RANK
        if sums is None:
            leaf = jnp.pad(leaf, ((0, rest), (0, 0)))
        else:
            pad = jnp.zeros((rest - 8, COLS), F32)
            leaf = jnp.concatenate([leaf, sums(), pad], axis=0)
        a_send[op] = leaf.T.reshape(GROUP, SLICE, LANES)
        if op == 0:

            @pl.when(j == 0)
            def _():
                pl.semaphore_wait(barrier, len(peers))

        a = copies(
            GROUP, g, to_group, lambda k: a_send.at[op, (g + k) % GROUP],
            a_slot.at[op], a_ss.at[op], a_rs.at[op],
        )
        start(a)
        a_slot[op, g] = a_send[op, g]

        @pl.when(j == 0)
        def _():
            pad_tree(op)
            loads["e%d" % op].wait()

        for t in range(WIDTH // TILE):
            both = jnp.dot(
                blocks[op, t * TILE : (t + 1) * TILE, :], stacked[...],
                preferred_element_type=F32,
            )
            direct[t * TILE : (t + 1) * TILE, :] = both[:, :COLS] + both[:, COLS:]

        arrived(a)
        c1 = upward(a_slot[op], op, 0)
        c1_ref[...] = c1
        c2 = upward(c1, op, 1)
        c2_ref[...] = c2
        c3 = upward(c2, op, 2)
        c3 = c3[0] if sums is None else c3[0] + riding(a_slot[op])
        z_send[op] = c3
        z = copies(
            DEEP, zc, to_deep, lambda k: z_send.at[op],
            z_slot.at[op], z_ss.at[op], z_rs.at[op],
        )
        start(z)
        z_slot[op, zc] = c3
        bridge0[...] = bridges(a_slot[op], op, 0)
        bridge1[...] = bridges(c1_ref[...], op, 1)
        bridge2[...] = bridges(c2_ref[...], op, 2)

        @pl.when(j == 0)
        def _():
            turn_rows(op)

        arrived(z)
        c4 = upward(z_slot[op], op, 3)
        c4_ref[...] = c4
        c5 = upward(c4, op, 4)
        c5_ref[...] = c5
        c6 = upward(c5, op, 5)
        c6 = c6[0] if sums is None else c6[0] + riding(z_slot[op])
        x_send[op] = c6
        x = copies(
            OUTER, xc, to_outer, lambda k: x_send.at[op],
            x_slot.at[op], x_ss.at[op], x_rs.at[op],
        )
        start(x)
        x_slot[op, xc] = c6
        near3 = own_bridge(lambda n: z_slot[op, n], zc, op, 3)
        near4 = own_bridge(lambda n: c4_ref[n], zc // 2, op, 4)
        near5 = own_bridge(lambda n: c5_ref[n], zc // 4, op, 5)
        arrived(x)
        c7 = upward(x_slot[op], op, 6)
        near6 = own_bridge(lambda n: x_slot[op, n], xc, op, 6)
        c4_ref[0:2] = c7
        d7 = own_bridge(lambda n: c4_ref[n], xc // 2, op, 7)
        d6 = near6 + own_down(d7, xc, op, 6)
        d5 = near5 + own_down(d6, zc // 4, op, 5)
        d4 = near4 + own_down(d5, zc // 2, op, 4)
        d3 = near3 + own_down(d4, zc, op, 3)
        d2 = downward(bridge2[...], d3.reshape(1, SLICE, LANES), op, 2)
        d1 = downward(bridge1[...], d2, op, 1)
        d0 = downward(bridge0[...], d1, op, 0)
        d_send[op] = d0 if sums is None else d0 + riding(x_slot[op])[None]
        d = copies(
            GROUP, g, to_group, lambda k: d_send.at[op, (g + k) % GROUP],
            d_slot.at[op], d_ss.at[op], d_rs.at[op],
        )
        start(d)
        d_slot[op, g] = d_send[op, g]
        left_device(a)
        left_device(z)
        left_device(x)
        arrived(d)
        high, low = halves(d_slot[op].reshape(COLS, LANES))
        spread = jnp.concatenate([high, low], axis=0)
        totals = None
        if sums is not None:
            totals = d_slot[op].reshape(COLS, LANES)[:, COLS:].T[RANK - COLS : RANK - COLS + 8]
        for t in range(WIDTH // TILE):
            part = slice(t * TILE, (t + 1) * TILE)
            both = lax.dot_general(rows_t[op, part, :], spread, NT, preferred_element_type=F32)
            target(part, direct[part, :] + both[:, :COLS] + both[:, COLS:])
        left_device(d)
        return totals

    def total_of(which, rows):
        r_send[which, 0] = rows
        ra = copies(
            GROUP, g, to_group, lambda k: r_send.at[which, 0],
            ra_slot.at[which], ra_ss.at[which], ra_rs.at[which],
        )
        start(ra)
        ra_slot[which, g] = rows
        arrived(ra)
        one = jnp.sum(ra_slot[which], axis=0)
        r_send[which, 1] = one
        rz = copies(
            DEEP, zc, to_deep, lambda k: r_send.at[which, 1],
            rz_slot.at[which], rz_ss.at[which], rz_rs.at[which],
        )
        start(rz)
        rz_slot[which, zc] = one
        arrived(rz)
        two = jnp.sum(rz_slot[which], axis=0)
        r_send[which, 2] = two
        rx = copies(
            OUTER, xc, to_outer, lambda k: r_send.at[which, 2],
            rx_slot.at[which], rx_ss.at[which], rx_rs.at[which],
        )
        start(rx)
        rx_slot[which, xc] = two
        arrived(rx)
        left_device(ra)
        left_device(rz)
        left_device(rx)
        return jnp.sum(rx_slot[which], axis=0)

    def column_sum(x):
        return jnp.sum(x, axis=0, keepdims=True)

    def partial_sums(j):
        rows = [column_sum(basis[i] * mixed[...]) for i in range(ITERS)]
        rows.append(column_sum(basis[j] * basis[j]))
        rows.append(jnp.zeros((8 - len(rows), COLS), F32))
        return jnp.concatenate(rows, axis=0)

    def arnoldi_column(totals, j):
        norm = jnp.sqrt(totals[ITERS : ITERS + 1] + EPSILON)
        hs[j * (ITERS + 1)] = norm
        entries = []
        for i in range(ITERS):
            entry = totals[i : i + 1] / norm
            entry = jnp.where(i == j, entry / norm, entry)
            entry = jnp.where(i > j, jnp.zeros_like(entry), entry)
            hs[j * (ITERS + 1) + 1 + i] = entry
            entries.append(entry)
        return 1.0 / norm, entries

    def iteration(j, carry):
        def to_image(part, value):
            images[j, part, :] = value

        def to_mixed(part, value):
            mixed[part, :] = value

        before = jnp.maximum(j - 1, 0)
        totals = tree_apply(0, j, lambda: mixed[...], to_image, lambda: partial_sums(before))

        @pl.when(j > 0)
        def _():
            scale, entries = arnoldi_column(totals, before)
            for t in range(WIDTH // TILE):
                part = slice(t * TILE, (t + 1) * TILE)
                basis[before, part, :] = basis[before, part, :] * scale
                images[before, part, :] = images[before, part, :] * scale
                image = images[j, part, :] * scale
                update = mixed[part, :] * scale
                for i in range(ITERS - 1):
                    image = image - entries[i] * images[i, part, :]
                    update = update - entries[i] * basis[i, part, :]
                images[j, part, :] = image
                basis[j, part, :] = update

        tree_apply(1, j, lambda: images[j], to_mixed)
        return carry

    lax.fori_loop(0, ITERS, iteration, 0)

    totals = total_of(0, partial_sums(ITERS - 1))
    scale, entries = arnoldi_column(totals, ITERS - 1)
    basis[ITERS - 1] = basis[ITERS - 1] * scale
    images[ITERS - 1] = images[ITERS - 1] * scale
    update = mixed[...] * scale
    for i in range(ITERS):
        update = update - entries[i] * basis[i]
    last = column_sum(update * update)
    totals = total_of(1, jnp.concatenate([last, jnp.zeros((7, COLS), F32)], axis=0))
    last_norm = jnp.sqrt(totals[0:1] + EPSILON)
    zero = jnp.zeros((1, COLS), F32)
    entries = [[zero for column in range(ITERS)] for line in range(ITERS + 1)]
    for column in range(ITERS):
        for line in range(column + 1):
            entries[line][column] = hs[column * (ITERS + 1) + 1 + line]
        if column + 1 < ITERS:
            entries[column + 1][column] = hs[(column + 1) * (ITERS + 1)]
        else:
            entries[column + 1][column] = last_norm
    weights = least_squares(entries, hs[0])
    sol_ref[...] = weights[0] * images[0] + weights[1] * images[1] + weights[2] * images[2]
    for line in range(ITERS + 1):
        hess_ref[line] = jnp.concatenate(entries[line], axis=0)


def solution(mesh):
    dma = pltpu.SemaphoreType.DMA
    tree = (2, GROUP, SLICE, LANES)
    scratch = [
        pltpu.VMEM((2, WIDTH, WIDTH), BF16),
        pltpu.VMEM((2, RANK, WIDTH), BF16),
        pltpu.VMEM((2, WIDTH, LANES), BF16),
        pltpu.VMEM((2, RANK, WIDTH), BF16),
        pltpu.VMEM((2, LEVELS, 2, RANK, RANK), BF16),
        pltpu.VMEM((2, LEVELS, 2, RANK, RANK), BF16),
        pltpu.VMEM((2, LEVELS, 2 * LANES, LANES), BF16),
        pltpu.VMEM((2, LEVELS, 2, LANES, LANES), BF16),
        pltpu.VMEM((ITERS, WIDTH, COLS), F32),
        pltpu.VMEM((ITERS, WIDTH, COLS), F32),
        pltpu.VMEM((WIDTH, COLS), F32),
        pltpu.VMEM((WIDTH, COLS), F32),
        pltpu.VMEM((WIDTH, 2 * COLS), BF16),
        pltpu.VMEM(tree, F32),
        pltpu.VMEM(tree, F32),
        pltpu.VMEM((2, SLICE, LANES), F32),
        pltpu.VMEM((2, DEEP, SLICE, LANES), F32),
        pltpu.VMEM((2, SLICE, LANES), F32),
        pltpu.VMEM((2, OUTER, SLICE, LANES), F32),
        pltpu.VMEM(tree, F32),
        pltpu.VMEM(tree, F32),
        pltpu.VMEM((4, SLICE, LANES), F32),
        pltpu.VMEM((2, SLICE, LANES), F32),
        pltpu.VMEM((4, SLICE, LANES), F32),
        pltpu.VMEM((2, SLICE, LANES), F32),
        pltpu.VMEM((8, SLICE, LANES), F32),
        pltpu.VMEM((4, SLICE, LANES), F32),
        pltpu.VMEM((2, SLICE, LANES), F32),
        pltpu.VMEM((2, 3, 8, COLS), F32),
        pltpu.VMEM((2, GROUP, 8, COLS), F32),
        pltpu.VMEM((2, DEEP, 8, COLS), F32),
        pltpu.VMEM((2, OUTER, 8, COLS), F32),
        pltpu.VMEM((ITERS * (ITERS + 1), 1, COLS), F32),
        dma((11,)),
        dma((2, GROUP - 1)),
        dma((2, GROUP - 1)),
        dma((2, DEEP - 1)),
        dma((2, DEEP - 1)),
        dma((2, OUTER - 1)),
        dma((2, OUTER - 1)),
        dma((2, GROUP - 1)),
        dma((2, GROUP - 1)),
        dma((2, GROUP - 1)),
        dma((2, GROUP - 1)),
        dma((2, DEEP - 1)),
        dma((2, DEEP - 1)),
        dma((2, OUTER - 1)),
        dma((2, OUTER - 1)),
    ]

    def on_device(*args):
        return pl.pallas_call(
            kernel,
            out_shape=(
                jax.ShapeDtypeStruct((WIDTH, COLS), F32),
                jax.ShapeDtypeStruct((ITERS + 1, ITERS, COLS), F32),
            ),
            in_specs=[pl.BlockSpec(memory_space=pl.ANY)] * 11,
            out_specs=[pl.BlockSpec(memory_space=pltpu.VMEM)] * 2,
            scratch_shapes=scratch,
            compiler_params=pltpu.CompilerParams(
                collective_id=0, has_side_effects=True, vmem_limit_bytes=60 * 2**20
            ),
        )(*args)

    leaf = P("leaf", None)
    block = P("leaf", None, None)
    in_specs = (leaf, block, block, block, P(), P(), block, block, block, P(), P())
    return jax.shard_map(
        on_device, mesh=mesh, in_specs=in_specs, out_specs=(leaf, P()), check_vma=False
    )
```

```python
import jax
import jax.numpy as jnp
from jax import lax
from jax.experimental import pallas as pl
from jax.experimental.pallas import tpu as pltpu
from jax.sharding import PartitionSpec as P

F32 = jnp.float32
BF16 = jnp.bfloat16
MESH = pl.DeviceIdType.MESH

ITERS = 3
EPSILON = 1e-06
WIDTH = 1024
RANK = 200
LANES = 256
COLS = 128
GROUP = 8
DEEP = 8
OUTER = 4
SLICE = COLS // GROUP
LEVELS = 8
TILE = 256

NT = (((1,), (1,)), ((), ()))
NN = (((1,), (0,)), ((), ()))


def halves(x):
    high = x.astype(BF16)
    return high, (x - high.astype(F32)).astype(BF16)


def product_rows(x, weight, dims):
    rows = x.shape[0]
    high, low = halves(x)
    both = lax.dot_general(
        jnp.concatenate([high, low], axis=0), weight, dims, preferred_element_type=F32
    )
    return both[:rows] + both[rows:]


def pairs(x):
    count = x.shape[0] // 2
    split = x.reshape(count, 2, SLICE, LANES)
    left = split[:, 0].reshape(count * SLICE, LANES)
    right = split[:, 1].reshape(count * SLICE, LANES)
    return left, right


def least_squares(entries, beta_first):
    unknowns = len(entries[0])
    matrix = [list(line) for line in entries]
    target = [beta_first] + [jnp.zeros_like(beta_first) for column in range(unknowns)]
    for column in range(unknowns):
        upper_entry = matrix[column][column]
        lower_entry = matrix[column + 1][column]
        radius = jnp.sqrt(upper_entry * upper_entry + lower_entry * lower_entry)
        cosine = upper_entry / radius
        sine_value = lower_entry / radius
        for following in range(column, unknowns):
            top_value = matrix[column][following]
            bottom_value = matrix[column + 1][following]
            matrix[column][following] = cosine * top_value + sine_value * bottom_value
            matrix[column + 1][following] = cosine * bottom_value - sine_value * top_value
        top_value = target[column]
        bottom_value = target[column + 1]
        target[column] = cosine * top_value + sine_value * bottom_value
        target[column + 1] = cosine * bottom_value - sine_value * top_value
    coefficients = [None] * unknowns
    for current_row in reversed(range(unknowns)):
        remainder = target[current_row]
        for following in range(current_row + 1, unknowns):
            remainder = remainder - matrix[current_row][following] * coefficients[following]
        coefficients[current_row] = remainder / matrix[current_row][current_row]
    return coefficients


def kernel(
    rhs_hbm,
    ea_hbm,
    pa_hbm,
    qa_hbm,
    ta_hbm,
    ca_hbm,
    em_hbm,
    pm_hbm,
    qm_hbm,
    tm_hbm,
    cm_hbm,
    sol_ref,
    hess_ref,
    blocks,
    rows_raw,
    rows_t,
    cols_side,
    trans_raw,
    coup_raw,
    trans,
    coup,
    basis,
    images,
    mixed,
    direct,
    stacked,
    a_send,
    a_slot,
    z_send,
    z_slot,
    x_send,
    x_slot,
    d_send,
    d_slot,
    c1_ref,
    c2_ref,
    c4_ref,
    c5_ref,
    bridge0,
    bridge1,
    bridge2,
    r_send,
    ra_slot,
    rz_slot,
    rx_slot,
    hs,
    joins,
    join_w,
    carried,
    fresh,
    load_sem,
    a_ss,
    a_rs,
    z_ss,
    z_rs,
    x_ss,
    x_rs,
    d_ss,
    d_rs,
    ra_ss,
    ra_rs,
    rz_ss,
    rz_rs,
    rx_ss,
    rx_rs,
    j_ss,
    j_rs,
):
    me = lax.axis_index("leaf")
    g = me % GROUP
    zc = (me // GROUP) % DEEP
    xc = me // (GROUP * DEEP)

    def to_group(k):
        return (me // GROUP) * GROUP + (g + k) % GROUP

    def to_deep(k):
        return xc * (GROUP * DEEP) + ((zc + k) % DEEP) * GROUP + g

    def to_outer(k):
        return ((xc + k) % OUTER) * (GROUP * DEEP) + me % (GROUP * DEEP)

    def load(src, dst, which):
        return pltpu.make_async_copy(src, dst, load_sem.at[which])

    loads = {
        "rhs": load(rhs_hbm, mixed, 0),
        "q0": load(qm_hbm.at[0], cols_side.at[0], 1),
        "t0": load(tm_hbm, trans_raw.at[0], 2),
        "e0": load(em_hbm.at[0], blocks.at[0], 3),
        "c0": load(cm_hbm, coup_raw.at[0], 4),
        "p0": load(pm_hbm.at[0], rows_raw.at[0], 5),
        "q1": load(qa_hbm.at[0], cols_side.at[1], 6),
        "t1": load(ta_hbm, trans_raw.at[1], 7),
        "e1": load(ea_hbm.at[0], blocks.at[1], 8),
        "c1": load(ca_hbm, coup_raw.at[1], 9),
        "p1": load(pa_hbm.at[0], rows_raw.at[1], 10),
    }
    for item in loads.values():
        item.start()

    barrier = pltpu.get_barrier_semaphore()
    peers = [to_group(k) for k in range(1, GROUP)]
    peers += [to_deep(k) for k in range(1, DEEP)]
    peers += [to_outer(k) for k in range(1, OUTER)]
    for peer in peers:
        pl.semaphore_signal(barrier, inc=1, device_id=(peer,), device_id_type=MESH)

    for i in range(1, ITERS):
        basis[i] = jnp.zeros((WIDTH, COLS), F32)
        images[i] = jnp.zeros((WIDTH, COLS), F32)
        carried[i] = jnp.zeros((GROUP, SLICE, LANES), F32)

    def pad_tree(op):
        loads["t%d" % op].wait()
        loads["c%d" % op].wait()
        edge = ((0, LANES - RANK), (0, LANES - RANK))

        def one(h, carry):
            for s in range(2):
                trans[op, h, s * LANES : (s + 1) * LANES, :] = jnp.pad(trans_raw[op, h, s], edge)
                coup[op, h, s] = jnp.pad(coup_raw[op, h, s], edge)
            return carry

        lax.fori_loop(0, LEVELS, one, 0)

    def turn_rows(op):
        for t in range(WIDTH // TILE):
            part = rows_raw[op, :, t * TILE : (t + 1) * TILE].astype(F32)
            part = jnp.pad(part, ((0, LANES - RANK), (0, 0)))
            rows_t[op, t * TILE : (t + 1) * TILE, :] = part.T.astype(BF16)

    def copies(count, coord, target, source, slot, send_sem, recv_sem):
        out = []
        arrive = []
        for k in range(1, count):
            out.append(
                pltpu.make_async_remote_copy(
                    src_ref=source(k),
                    dst_ref=slot.at[coord],
                    send_sem=send_sem.at[k - 1],
                    recv_sem=recv_sem.at[k - 1],
                    device_id=(target(k),),
                    device_id_type=MESH,
                )
            )
            arrive.append(
                pltpu.make_async_remote_copy(
                    src_ref=source(k),
                    dst_ref=slot.at[(coord + count - k) % count],
                    send_sem=send_sem.at[k - 1],
                    recv_sem=recv_sem.at[k - 1],
                    device_id=(target(k),),
                    device_id_type=MESH,
                )
            )
        return out, arrive

    def start(group):
        for c in group[0]:
            c.start()

    def arrived(group):
        for c in group[1]:
            c.wait_recv()

    def left_device(group):
        for c in group[0]:
            c.wait_send()

    def upward(x, op, h):
        left, right = pairs(x)
        joined = product_rows(
            jnp.concatenate([left, right], axis=1), trans[op, h], NN
        )
        return joined.reshape(x.shape[0] // 2, SLICE, LANES)

    def bridges(x, op, h):
        left, right = pairs(x)
        count = x.shape[0] // 2
        first = product_rows(right, coup[op, h, 0], NT).reshape(count, 1, SLICE, LANES)
        second = product_rows(left, coup[op, h, 1], NT).reshape(count, 1, SLICE, LANES)
        return jnp.concatenate([first, second], axis=1).reshape(x.shape)

    def downward(bridge, above, op, h):
        count = above.shape[0]
        moved = product_rows(above.reshape(count * SLICE, LANES), trans[op, h], NT)
        first = moved[:, :LANES].reshape(count, 1, SLICE, LANES)
        second = moved[:, LANES:].reshape(count, 1, SLICE, LANES)
        return bridge + jnp.concatenate([first, second], axis=1).reshape(bridge.shape)

    def own_bridge(values, own, op, h):
        side = own % 2
        return product_rows(values(own + 1 - 2 * side), coup[op, h, side], NT)

    def own_down(above, own, op, h):
        side = own % 2
        weight = trans[op, h, pl.ds(pl.multiple_of(side * LANES, LANES), LANES), :]
        return product_rows(above, weight, NT)

    def riding(x):
        lane = lax.broadcasted_iota(jnp.int32, (SLICE, LANES - COLS), 1)
        total = jnp.sum(x[:, :, COLS:], axis=0)
        total = jnp.where(lane >= RANK - COLS, total, jnp.zeros_like(total))
        return jnp.concatenate([jnp.zeros((SLICE, COLS), F32), total], axis=1)

    def leaf_terms(op, value, sums=None):
        high, low = halves(value)
        stacked[:, :COLS] = high
        stacked[:, COLS:] = low
        both = jnp.dot(cols_side[op], stacked[...], preferred_element_type=F32)
        leaf = both[:, :COLS] + both[:, COLS:]
        rest = LANES - RANK
        if sums is None:
            leaf = jnp.pad(leaf, ((0, rest), (0, 0)))
        else:
            pad = jnp.zeros((rest - 8, COLS), F32)
            leaf = jnp.concatenate([leaf, sums, pad], axis=0)
        a_send[op] = leaf.T.reshape(GROUP, SLICE, LANES)

    def send_leaf(op):
        a = copies(
            GROUP, g, to_group, lambda k: a_send.at[op, (g + k) % GROUP],
            a_slot.at[op], a_ss.at[op], a_rs.at[op],
        )
        start(a)
        a_slot[op, g] = a_send[op, g]
        return a

    def send_down(op, value):
        d_send[op] = value
        d = copies(
            GROUP, g, to_group, lambda k: d_send.at[op, (g + k) % GROUP],
            d_slot.at[op], d_ss.at[op], d_rs.at[op],
        )
        start(d)
        d_slot[op, g] = d_send[op, g]
        return d

    def block_product(op):
        for t in range(WIDTH // TILE):
            both = jnp.dot(
                blocks[op, t * TILE : (t + 1) * TILE, :], stacked[...],
                preferred_element_type=F32,
            )
            direct[t * TILE : (t + 1) * TILE, :] = both[:, :COLS] + both[:, COLS:]

    def spread_down(op, target):
        high, low = halves(d_slot[op].reshape(COLS, LANES))
        spread = jnp.concatenate([high, low], axis=0)
        for t in range(WIDTH // TILE):
            part = slice(t * TILE, (t + 1) * TILE)
            both = lax.dot_general(rows_t[op, part, :], spread, NT, preferred_element_type=F32)
            target(part, direct[part, :] + both[:, :COLS] + both[:, COLS:])

    def tree(op, leaves, sums, while_z=None, while_x=None):
        c1 = upward(leaves(), op, 0)
        c1_ref[...] = c1
        c2 = upward(c1, op, 1)
        c2_ref[...] = c2
        c3 = upward(c2, op, 2)
        c3 = c3[0] + riding(leaves()) if sums else c3[0]
        z_send[op] = c3
        z = copies(
            DEEP, zc, to_deep, lambda k: z_send.at[op],
            z_slot.at[op], z_ss.at[op], z_rs.at[op],
        )
        start(z)
        z_slot[op, zc] = c3
        bridge0[...] = bridges(leaves(), op, 0)
        bridge1[...] = bridges(c1_ref[...], op, 1)
        bridge2[...] = bridges(c2_ref[...], op, 2)
        if while_z is not None:
            while_z()
        arrived(z)
        c4 = upward(z_slot[op], op, 3)
        c4_ref[...] = c4
        c5 = upward(c4, op, 4)
        c5_ref[...] = c5
        c6 = upward(c5, op, 5)
        c6 = c6[0] + riding(z_slot[op]) if sums else c6[0]
        x_send[op] = c6
        x = copies(
            OUTER, xc, to_outer, lambda k: x_send.at[op],
            x_slot.at[op], x_ss.at[op], x_rs.at[op],
        )
        start(x)
        x_slot[op, xc] = c6
        near3 = own_bridge(lambda n: z_slot[op, n], zc, op, 3)
        near4 = own_bridge(lambda n: c4_ref[n], zc // 2, op, 4)
        near5 = own_bridge(lambda n: c5_ref[n], zc // 4, op, 5)
        if while_x is not None:
            while_x()
        arrived(x)
        c7 = upward(x_slot[op], op, 6)
        near6 = own_bridge(lambda n: x_slot[op, n], xc, op, 6)
        c4_ref[0:2] = c7
        d7 = own_bridge(lambda n: c4_ref[n], xc // 2, op, 7)
        d6 = near6 + own_down(d7, xc, op, 6)
        d5 = near5 + own_down(d6, zc // 4, op, 5)
        d4 = near4 + own_down(d5, zc // 2, op, 4)
        d3 = near3 + own_down(d4, zc, op, 3)
        d2 = downward(bridge2[...], d3.reshape(1, SLICE, LANES), op, 2)
        d1 = downward(bridge1[...], d2, op, 1)
        d0 = downward(bridge0[...], d1, op, 0)
        left_device(z)
        left_device(x)
        return d0

    partner = g + 1 - 2 * (g % 2)
    join_out = []
    join_in = []
    for k in range(4):
        to = to_group(2 * k) if k else (me // GROUP) * GROUP + partner
        source = (g + GROUP - 2 * k) % GROUP if k else partner
        for group, where in ((join_out, g), (join_in, source)):
            group.append(
                pltpu.make_async_remote_copy(
                    src_ref=joins.at[g], dst_ref=joins.at[where],
                    send_sem=j_ss.at[k], recv_sem=j_rs.at[k],
                    device_id=(to,), device_id_type=MESH,
                )
            )
    pass_out = []
    pass_in = []
    for k in range(1, 4):
        mine = (g + GROUP - 2 * k) % GROUP
        theirs = (partner + GROUP - 2 * k) % GROUP
        for group, where in ((pass_out, mine), (pass_in, theirs)):
            group.append(
                pltpu.make_async_remote_copy(
                    src_ref=joins.at[mine], dst_ref=joins.at[where],
                    send_sem=j_ss.at[3 + k], recv_sem=j_rs.at[3 + k],
                    device_id=((me // GROUP) * GROUP + partner,), device_id_type=MESH,
                )
            )

    def begin_joins():
        loads["p0"].wait()
        loads["q1"].wait()
        own = lax.dot_general(rows_raw[0], cols_side[1], NT, preferred_element_type=F32)
        joins[g] = jnp.pad(own, ((0, 0), (0, LANES - RANK)))
        for c in join_out:
            c.start()
        turn_rows(0)

    def pass_joins():
        loads["p1"].wait()
        turn_rows(1)
        for k in range(1, 4):
            join_in[k].wait_recv()
            pass_out[k - 1].start()

    def end_joins():
        join_in[0].wait_recv()
        for c in pass_in:
            c.wait_recv()

        def one(i, carry):
            high, low = halves(jnp.pad(joins[i], ((0, LANES - RANK), (0, 0))))
            join_w[i, 0] = high
            join_w[i, 1] = low
            return carry

        lax.fori_loop(0, GROUP, one, 0)
        for c in join_out + pass_out:
            c.wait_send()

    def joined_rows(x, i):
        high, low = halves(x)
        main = jnp.dot(
            jnp.concatenate([high, low], axis=0), join_w[i, 0], preferred_element_type=F32
        )
        return main[:SLICE] + main[SLICE:] + jnp.dot(
            high, join_w[i, 1], preferred_element_type=F32
        )

    def total_of(which, rows):
        r_send[which, 0] = rows
        ra = copies(
            GROUP, g, to_group, lambda k: r_send.at[which, 0],
            ra_slot.at[which], ra_ss.at[which], ra_rs.at[which],
        )
        start(ra)
        ra_slot[which, g] = rows
        arrived(ra)
        one = jnp.sum(ra_slot[which], axis=0)
        r_send[which, 1] = one
        rz = copies(
            DEEP, zc, to_deep, lambda k: r_send.at[which, 1],
            rz_slot.at[which], rz_ss.at[which], rz_rs.at[which],
        )
        start(rz)
        rz_slot[which, zc] = one
        arrived(rz)
        two = jnp.sum(rz_slot[which], axis=0)
        r_send[which, 2] = two
        rx = copies(
            OUTER, xc, to_outer, lambda k: r_send.at[which, 2],
            rx_slot.at[which], rx_ss.at[which], rx_rs.at[which],
        )
        start(rx)
        rx_slot[which, xc] = two
        arrived(rx)
        left_device(ra)
        left_device(rz)
        left_device(rx)
        return jnp.sum(rx_slot[which], axis=0)

    def column_sum(x):
        return jnp.sum(x, axis=0, keepdims=True)

    def partial_sums(j):
        rows = [column_sum(basis[i] * mixed[...]) for i in range(ITERS)]
        rows.append(column_sum(basis[j] * basis[j]))
        rows.append(jnp.zeros((8 - len(rows), COLS), F32))
        return jnp.concatenate(rows, axis=0)

    def column_entries(sums, j):
        norm = jnp.sqrt(sums(ITERS) + EPSILON)
        entries = []
        for i in range(ITERS):
            entry = sums(i) / norm
            entry = jnp.where(i == j, entry / norm, entry)
            entries.append(jnp.where(i > j, jnp.zeros_like(entry), entry))
        return norm, 1.0 / norm, entries

    def arnoldi_column(totals, j):
        norm, scale, entries = column_entries(lambda i: totals[i : i + 1], j)
        hs[j * (ITERS + 1)] = norm
        for i in range(ITERS):
            hs[j * (ITERS + 1) + 1 + i] = entries[i]
        return scale, entries

    def to_mixed(part, value):
        mixed[part, :] = value

    def first():
        loads["rhs"].wait()
        loads["q0"].wait()
        basis[0] = mixed[...]
        leaf_terms(0, mixed[...])
        pl.semaphore_wait(barrier, len(peers))
        a = send_leaf(0)
        pad_tree(0)
        loads["e0"].wait()
        block_product(0)
        arrived(a)
        low = tree(0, lambda: a_slot[0], False, while_z=begin_joins)
        d = send_down(0, low)
        left_device(a)
        pad_tree(1)
        arrived(d)

        def to_image(part, value):
            images[0, part, :] = value

        spread_down(0, to_image)
        left_device(d)
        leaf_terms(1, images[0])
        a = send_leaf(1)
        loads["e1"].wait()
        block_product(1)
        arrived(a)
        carried[0] = a_slot[1]
        low = tree(1, lambda: carried[0], False, while_z=pass_joins)
        d = send_down(1, low)
        left_device(a)
        arrived(d)
        spread_down(1, to_mixed)
        left_device(d)

    def iteration(j, carry):
        before = j - 1
        leaf_terms(0, mixed[...], partial_sums(before))
        a0 = send_leaf(0)
        block_product(0)
        leaf_terms(1, direct[...])
        a1 = send_leaf(1)
        arrived(a0)

        def weights_ready():
            @pl.when(j == 1)
            def _():
                end_joins()

        low = tree(0, lambda: a_slot[0], True, while_z=weights_ready)
        d = send_down(0, low + riding(x_slot[0])[None])

        arrived(a1)
        sums = jnp.sum(x_slot[0, :, :, COLS:], axis=0)
        norm, scale, entries = column_entries(
            lambda i: sums[:, RANK - COLS + i : RANK - COLS + i + 1], before
        )
        carried[before] = carried[before] * scale[None]
        for i in range(GROUP):
            value = (a_slot[1, i] + joined_rows(low[i], i)) * scale
            for earlier in range(ITERS - 1):
                value = value - entries[earlier] * carried[earlier, i]
            fresh[i] = value
        carried[j] = fresh[...]
        left_device(a0)
        left_device(a1)

        def orthogonalise():
            arrived(d)
            totals = d_slot[0].reshape(COLS, LANES)[:, COLS:].T[RANK - COLS : RANK - COLS + 8]
            scale, entries = arnoldi_column(totals, before)
            basis[before] = basis[before] * scale
            images[before] = images[before] * scale

            def finish(part, image):
                image = image * scale
                update = mixed[part, :] * scale
                for i in range(ITERS - 1):
                    image = image - entries[i] * images[i, part, :]
                    update = update - entries[i] * basis[i, part, :]
                images[j, part, :] = image
                basis[j, part, :] = update
                high, low = halves(image)
                stacked[part, :COLS] = high
                stacked[part, COLS:] = low

            spread_down(0, finish)

        low = tree(1, lambda: fresh[...], False, while_x=orthogonalise)
        e = send_down(1, low)
        block_product(1)
        left_device(d)
        arrived(e)
        spread_down(1, to_mixed)
        left_device(e)
        return carry

    first()
    lax.fori_loop(1, ITERS, iteration, 0)

    totals = total_of(0, partial_sums(ITERS - 1))
    scale, entries = arnoldi_column(totals, ITERS - 1)
    basis[ITERS - 1] = basis[ITERS - 1] * scale
    images[ITERS - 1] = images[ITERS - 1] * scale
    update = mixed[...] * scale
    for i in range(ITERS):
        update = update - entries[i] * basis[i]
    last = column_sum(update * update)
    totals = total_of(1, jnp.concatenate([last, jnp.zeros((7, COLS), F32)], axis=0))
    last_norm = jnp.sqrt(totals[0:1] + EPSILON)
    zero = jnp.zeros((1, COLS), F32)
    entries = [[zero for column in range(ITERS)] for line in range(ITERS + 1)]
    for column in range(ITERS):
        for line in range(column + 1):
            entries[line][column] = hs[column * (ITERS + 1) + 1 + line]
        if column + 1 < ITERS:
            entries[column + 1][column] = hs[(column + 1) * (ITERS + 1)]
        else:
            entries[column + 1][column] = last_norm
    weights = least_squares(entries, hs[0])
    sol_ref[...] = weights[0] * images[0] + weights[1] * images[1] + weights[2] * images[2]
    for line in range(ITERS + 1):
        hess_ref[line] = jnp.concatenate(entries[line], axis=0)


def solution(mesh):
    dma = pltpu.SemaphoreType.DMA
    tree = (2, GROUP, SLICE, LANES)
    scratch = [
        pltpu.VMEM((2, WIDTH, WIDTH), BF16),
        pltpu.VMEM((2, RANK, WIDTH), BF16),
        pltpu.VMEM((2, WIDTH, LANES), BF16),
        pltpu.VMEM((2, RANK, WIDTH), BF16),
        pltpu.VMEM((2, LEVELS, 2, RANK, RANK), BF16),
        pltpu.VMEM((2, LEVELS, 2, RANK, RANK), BF16),
        pltpu.VMEM((2, LEVELS, 2 * LANES, LANES), BF16),
        pltpu.VMEM((2, LEVELS, 2, LANES, LANES), BF16),
        pltpu.VMEM((ITERS, WIDTH, COLS), F32),
        pltpu.VMEM((ITERS, WIDTH, COLS), F32),
        pltpu.VMEM((WIDTH, COLS), F32),
        pltpu.VMEM((WIDTH, COLS), F32),
        pltpu.VMEM((WIDTH, 2 * COLS), BF16),
        pltpu.VMEM(tree, F32),
        pltpu.VMEM(tree, F32),
        pltpu.VMEM((2, SLICE, LANES), F32),
        pltpu.VMEM((2, DEEP, SLICE, LANES), F32),
        pltpu.VMEM((2, SLICE, LANES), F32),
        pltpu.VMEM((2, OUTER, SLICE, LANES), F32),
        pltpu.VMEM(tree, F32),
        pltpu.VMEM(tree, F32),
        pltpu.VMEM((4, SLICE, LANES), F32),
        pltpu.VMEM((2, SLICE, LANES), F32),
        pltpu.VMEM((4, SLICE, LANES), F32),
        pltpu.VMEM((2, SLICE, LANES), F32),
        pltpu.VMEM((8, SLICE, LANES), F32),
        pltpu.VMEM((4, SLICE, LANES), F32),
        pltpu.VMEM((2, SLICE, LANES), F32),
        pltpu.VMEM((2, 3, 8, COLS), F32),
        pltpu.VMEM((2, GROUP, 8, COLS), F32),
        pltpu.VMEM((2, DEEP, 8, COLS), F32),
        pltpu.VMEM((2, OUTER, 8, COLS), F32),
        pltpu.VMEM((ITERS * (ITERS + 1), 1, COLS), F32),
        pltpu.VMEM((GROUP, RANK, LANES), F32),
        pltpu.VMEM((GROUP, 2, LANES, LANES), BF16),
        pltpu.VMEM((ITERS,) + tree[1:], F32),
        pltpu.VMEM(tree[1:], F32),
        dma((11,)),
        dma((2, GROUP - 1)),
        dma((2, GROUP - 1)),
        dma((2, DEEP - 1)),
        dma((2, DEEP - 1)),
        dma((2, OUTER - 1)),
        dma((2, OUTER - 1)),
        dma((2, GROUP - 1)),
        dma((2, GROUP - 1)),
        dma((2, GROUP - 1)),
        dma((2, GROUP - 1)),
        dma((2, DEEP - 1)),
        dma((2, DEEP - 1)),
        dma((2, OUTER - 1)),
        dma((2, OUTER - 1)),
        dma((7,)),
        dma((7,)),
    ]

    def on_device(*args):
        return pl.pallas_call(
            kernel,
            out_shape=(
                jax.ShapeDtypeStruct((WIDTH, COLS), F32),
                jax.ShapeDtypeStruct((ITERS + 1, ITERS, COLS), F32),
            ),
            in_specs=[pl.BlockSpec(memory_space=pl.ANY)] * 11,
            out_specs=[pl.BlockSpec(memory_space=pltpu.VMEM)] * 2,
            scratch_shapes=scratch,
            compiler_params=pltpu.CompilerParams(
                collective_id=0, has_side_effects=True, vmem_limit_bytes=60 * 2**20
            ),
        )(*args)

    leaf = P("leaf", None)
    block = P("leaf", None, None)
    in_specs = (leaf, block, block, block, P(), P(), block, block, block, P(), P())
    return jax.shard_map(
        on_device, mesh=mesh, in_specs=in_specs, out_specs=(leaf, P()), check_vma=False
    )
```

```python
import jax
import jax.numpy as jnp
from jax import lax
from jax.experimental import pallas as pl
from jax.experimental.pallas import tpu as pltpu
from jax.sharding import PartitionSpec as P

F32 = jnp.float32
BF16 = jnp.bfloat16
MESH = pl.DeviceIdType.MESH

ITERS = 3
EPSILON = 1e-06
WIDTH = 1024
RANK = 200
LANES = 256
COLS = 128
GROUP = 8
DEEP = 8
OUTER = 4
SLICE = COLS // GROUP
LEVELS = 8
TILE = 256

NT = (((1,), (1,)), ((), ()))
NN = (((1,), (0,)), ((), ()))


def halves(x):
    high = x.astype(BF16)
    return high, (x - high.astype(F32)).astype(BF16)


def product_rows(x, weight, dims):
    rows = x.shape[0]
    high, low = halves(x)
    both = lax.dot_general(
        jnp.concatenate([high, low], axis=0), weight, dims, preferred_element_type=F32
    )
    return both[:rows] + both[rows:]


def pairs(x):
    count = x.shape[0] // 2
    split = x.reshape(count, 2, SLICE, LANES)
    left = split[:, 0].reshape(count * SLICE, LANES)
    right = split[:, 1].reshape(count * SLICE, LANES)
    return left, right


def least_squares(entries, beta_first):
    unknowns = len(entries[0])
    matrix = [list(line) for line in entries]
    target = [beta_first] + [jnp.zeros_like(beta_first) for column in range(unknowns)]
    for column in range(unknowns):
        upper_entry = matrix[column][column]
        lower_entry = matrix[column + 1][column]
        radius = jnp.sqrt(upper_entry * upper_entry + lower_entry * lower_entry)
        cosine = upper_entry / radius
        sine_value = lower_entry / radius
        for following in range(column, unknowns):
            top_value = matrix[column][following]
            bottom_value = matrix[column + 1][following]
            matrix[column][following] = cosine * top_value + sine_value * bottom_value
            matrix[column + 1][following] = cosine * bottom_value - sine_value * top_value
        top_value = target[column]
        bottom_value = target[column + 1]
        target[column] = cosine * top_value + sine_value * bottom_value
        target[column + 1] = cosine * bottom_value - sine_value * top_value
    coefficients = [None] * unknowns
    for current_row in reversed(range(unknowns)):
        remainder = target[current_row]
        for following in range(current_row + 1, unknowns):
            remainder = remainder - matrix[current_row][following] * coefficients[following]
        coefficients[current_row] = remainder / matrix[current_row][current_row]
    return coefficients


def kernel(
    rhs_hbm,
    ea_hbm,
    pa_hbm,
    qa_hbm,
    ta_hbm,
    ca_hbm,
    em_hbm,
    pm_hbm,
    qm_hbm,
    tm_hbm,
    cm_hbm,
    sol_ref,
    hess_ref,
    blocks,
    rows_raw,
    rows_t,
    cols_side,
    trans_raw,
    coup_raw,
    trans,
    coup,
    basis,
    images,
    mixed,
    direct,
    stacked,
    a_send,
    a_slot,
    z_send,
    z_slot,
    x_send,
    x_slot,
    d_send,
    d_slot,
    c1_ref,
    c2_ref,
    c4_ref,
    c5_ref,
    bridge0,
    bridge1,
    bridge2,
    r_send,
    ra_slot,
    rz_slot,
    rx_slot,
    hs,
    sums_ref,
    joins,
    join_w,
    carried,
    fresh,
    load_sem,
    a_ss,
    a_rs,
    z_ss,
    z_rs,
    x_ss,
    x_rs,
    d_ss,
    d_rs,
    ra_ss,
    ra_rs,
    rz_ss,
    rz_rs,
    rx_ss,
    rx_rs,
    j_ss,
    j_rs,
):
    me = lax.axis_index("leaf")
    g = me % GROUP
    zc = (me // GROUP) % DEEP
    xc = me // (GROUP * DEEP)

    def to_group(k):
        return (me // GROUP) * GROUP + (g + k) % GROUP

    def to_deep(k):
        return xc * (GROUP * DEEP) + ((zc + k) % DEEP) * GROUP + g

    def to_outer(k):
        return ((xc + k) % OUTER) * (GROUP * DEEP) + me % (GROUP * DEEP)

    def load(src, dst, which):
        return pltpu.make_async_copy(src, dst, load_sem.at[which])

    loads = {
        "rhs": load(rhs_hbm, mixed, 0),
        "q0": load(qm_hbm.at[0], cols_side.at[0], 1),
        "p0": load(pm_hbm.at[0], rows_raw.at[0], 5),
        "q1": load(qa_hbm.at[0], cols_side.at[1], 6),
        "t0": load(tm_hbm, trans_raw.at[0], 2),
        "e0": load(em_hbm.at[0], blocks.at[0], 3),
        "c0": load(cm_hbm, coup_raw.at[0], 4),
        "t1": load(ta_hbm, trans_raw.at[1], 7),
        "e1": load(ea_hbm.at[0], blocks.at[1], 8),
        "c1": load(ca_hbm, coup_raw.at[1], 9),
        "p1": load(pa_hbm.at[0], rows_raw.at[1], 10),
    }
    for item in loads.values():
        item.start()

    barrier = pltpu.get_barrier_semaphore()
    peers = [to_group(k) for k in range(1, GROUP)]
    peers += [to_deep(k) for k in range(1, DEEP)]
    peers += [to_outer(k) for k in range(1, OUTER)]
    for peer in peers:
        pl.semaphore_signal(barrier, inc=1, device_id=(peer,), device_id_type=MESH)

    sums_ref[...] = jnp.zeros((8, COLS), F32)
    for i in range(ITERS):
        basis[i] = jnp.zeros((WIDTH, COLS), F32)
        images[i] = jnp.zeros((WIDTH, COLS), F32)
        carried[i] = jnp.zeros((GROUP, SLICE, LANES), F32)

    def pad_tree(op):
        loads["t%d" % op].wait()
        loads["c%d" % op].wait()
        edge = ((0, LANES - RANK), (0, LANES - RANK))

        def one(h, carry):
            for s in range(2):
                trans[op, h, s * LANES : (s + 1) * LANES, :] = jnp.pad(trans_raw[op, h, s], edge)
                coup[op, h, s] = jnp.pad(coup_raw[op, h, s], edge)
            return carry

        lax.fori_loop(0, LEVELS, one, 0)

    def turn_rows(op):
        for t in range(WIDTH // TILE):
            part = rows_raw[op, :, t * TILE : (t + 1) * TILE].astype(F32)
            part = jnp.pad(part, ((0, LANES - RANK), (0, 0)))
            rows_t[op, t * TILE : (t + 1) * TILE, :] = part.T.astype(BF16)

    def copies(count, coord, target, source, slot, send_sem, recv_sem):
        out = []
        arrive = []
        for k in range(1, count):
            out.append(
                pltpu.make_async_remote_copy(
                    src_ref=source(k),
                    dst_ref=slot.at[coord],
                    send_sem=send_sem.at[k - 1],
                    recv_sem=recv_sem.at[k - 1],
                    device_id=(target(k),),
                    device_id_type=MESH,
                )
            )
            arrive.append(
                pltpu.make_async_remote_copy(
                    src_ref=source(k),
                    dst_ref=slot.at[(coord + count - k) % count],
                    send_sem=send_sem.at[k - 1],
                    recv_sem=recv_sem.at[k - 1],
                    device_id=(target(k),),
                    device_id_type=MESH,
                )
            )
        return out, arrive

    def start(group):
        count = len(group[0]) + 1
        for k in sorted(range(1, count), key=lambda k: -min(k, count - k)):
            group[0][k - 1].start()

    def arrived(group):
        for c in group[1]:
            c.wait_recv()

    def left_device(group):
        for c in group[0]:
            c.wait_send()

    def upward(x, op, h):
        left, right = pairs(x)
        joined = product_rows(
            jnp.concatenate([left, right], axis=1), trans[op, h], NN
        )
        return joined.reshape(x.shape[0] // 2, SLICE, LANES)

    def bridges(x, op, h):
        left, right = pairs(x)
        count = x.shape[0] // 2
        first = product_rows(right, coup[op, h, 0], NT).reshape(count, 1, SLICE, LANES)
        second = product_rows(left, coup[op, h, 1], NT).reshape(count, 1, SLICE, LANES)
        return jnp.concatenate([first, second], axis=1).reshape(x.shape)

    def downward(bridge, above, op, h):
        count = above.shape[0]
        moved = product_rows(above.reshape(count * SLICE, LANES), trans[op, h], NT)
        first = moved[:, :LANES].reshape(count, 1, SLICE, LANES)
        second = moved[:, LANES:].reshape(count, 1, SLICE, LANES)
        return bridge + jnp.concatenate([first, second], axis=1).reshape(bridge.shape)

    def own_bridge(values, own, op, h):
        side = own % 2
        return product_rows(values(own + 1 - 2 * side), coup[op, h, side], NT)

    def own_down(above, own, op, h):
        side = own % 2
        weight = trans[op, h, pl.ds(pl.multiple_of(side * LANES, LANES), LANES), :]
        return product_rows(above, weight, NT)

    def riding(x):
        lane = lax.broadcasted_iota(jnp.int32, (SLICE, LANES - COLS), 1)
        total = jnp.sum(x[:, :, COLS:], axis=0)
        total = jnp.where(lane >= RANK - COLS, total, jnp.zeros_like(total))
        return jnp.concatenate([jnp.zeros((SLICE, COLS), F32), total], axis=1)

    def leaf_terms(op, value, sums=None):
        high, low = halves(value)
        stacked[:, :COLS] = high
        stacked[:, COLS:] = low
        both = jnp.dot(cols_side[op], stacked[...], preferred_element_type=F32)
        leaf = both[:, :COLS] + both[:, COLS:]
        rest = LANES - RANK
        if sums is None:
            leaf = jnp.pad(leaf, ((0, rest), (0, 0)))
        else:
            pad = jnp.zeros((rest - 8, COLS), F32)
            leaf = jnp.concatenate([leaf, sums, pad], axis=0)
        a_send[op] = leaf.T.reshape(GROUP, SLICE, LANES)

    def send_leaf(op):
        a = copies(
            GROUP, g, to_group, lambda k: a_send.at[op, (g + k) % GROUP],
            a_slot.at[op], a_ss.at[op], a_rs.at[op],
        )
        start(a)
        a_slot[op, g] = a_send[op, g]
        return a

    def send_down(op, value):
        d_send[op] = value
        d = copies(
            GROUP, g, to_group, lambda k: d_send.at[op, (g + k) % GROUP],
            d_slot.at[op], d_ss.at[op], d_rs.at[op],
        )
        start(d)
        d_slot[op, g] = d_send[op, g]
        return d

    def block_product(op):
        for t in range(WIDTH // TILE):
            both = jnp.dot(
                blocks[op, t * TILE : (t + 1) * TILE, :], stacked[...],
                preferred_element_type=F32,
            )
            direct[t * TILE : (t + 1) * TILE, :] = both[:, :COLS] + both[:, COLS:]

    def spread_down(op, target):
        high, low = halves(d_slot[op].reshape(COLS, LANES))
        spread = jnp.concatenate([high, low], axis=0)
        for t in range(WIDTH // TILE):
            part = slice(t * TILE, (t + 1) * TILE)
            both = lax.dot_general(rows_t[op, part, :], spread, NT, preferred_element_type=F32)
            target(part, direct[part, :] + both[:, :COLS] + both[:, COLS:])

    def tree(op, leaves, sums, while_z=None, while_x=None):
        c1 = upward(leaves(), op, 0)
        c1_ref[...] = c1
        c2 = upward(c1, op, 1)
        c2_ref[...] = c2
        c3 = upward(c2, op, 2)
        c3 = c3[0] + riding(leaves()) if sums else c3[0]
        z_send[op] = c3
        z = copies(
            DEEP, zc, to_deep, lambda k: z_send.at[op],
            z_slot.at[op], z_ss.at[op], z_rs.at[op],
        )
        start(z)
        z_slot[op, zc] = c3
        bridge0[...] = bridges(leaves(), op, 0)
        bridge1[...] = bridges(c1_ref[...], op, 1)
        bridge2[...] = bridges(c2_ref[...], op, 2)
        if while_z is not None:
            while_z()
        arrived(z)
        c4 = upward(z_slot[op], op, 3)
        c4_ref[...] = c4
        c5 = upward(c4, op, 4)
        c5_ref[...] = c5
        c6 = upward(c5, op, 5)
        c6 = c6[0] + riding(z_slot[op]) if sums else c6[0]
        x_send[op] = c6
        x = copies(
            OUTER, xc, to_outer, lambda k: x_send.at[op],
            x_slot.at[op], x_ss.at[op], x_rs.at[op],
        )
        start(x)
        x_slot[op, xc] = c6
        near3 = own_bridge(lambda n: z_slot[op, n], zc, op, 3)
        near4 = own_bridge(lambda n: c4_ref[n], zc // 2, op, 4)
        near5 = own_bridge(lambda n: c5_ref[n], zc // 4, op, 5)
        if while_x is not None:
            while_x()
        arrived(x)
        c7 = upward(x_slot[op], op, 6)
        near6 = own_bridge(lambda n: x_slot[op, n], xc, op, 6)
        c4_ref[0:2] = c7
        d7 = own_bridge(lambda n: c4_ref[n], xc // 2, op, 7)
        d6 = near6 + own_down(d7, xc, op, 6)
        d5 = near5 + own_down(d6, zc // 4, op, 5)
        d4 = near4 + own_down(d5, zc // 2, op, 4)
        d3 = near3 + own_down(d4, zc, op, 3)
        d2 = downward(bridge2[...], d3.reshape(1, SLICE, LANES), op, 2)
        d1 = downward(bridge1[...], d2, op, 1)
        d0 = downward(bridge0[...], d1, op, 0)
        left_device(z)
        left_device(x)
        return d0

    partner = g + 1 - 2 * (g % 2)
    join_out = []
    join_in = []
    for k in range(4):
        to = to_group(2 * k) if k else (me // GROUP) * GROUP + partner
        source = (g + GROUP - 2 * k) % GROUP if k else partner
        for group, where in ((join_out, g), (join_in, source)):
            group.append(
                pltpu.make_async_remote_copy(
                    src_ref=joins.at[g], dst_ref=joins.at[where],
                    send_sem=j_ss.at[k], recv_sem=j_rs.at[k],
                    device_id=(to,), device_id_type=MESH,
                )
            )
    pass_out = []
    pass_in = []
    for k in range(1, 4):
        mine = (g + GROUP - 2 * k) % GROUP
        theirs = (partner + GROUP - 2 * k) % GROUP
        for group, where in ((pass_out, mine), (pass_in, theirs)):
            group.append(
                pltpu.make_async_remote_copy(
                    src_ref=joins.at[mine], dst_ref=joins.at[where],
                    send_sem=j_ss.at[3 + k], recv_sem=j_rs.at[3 + k],
                    device_id=((me // GROUP) * GROUP + partner,), device_id_type=MESH,
                )
            )

    def begin_joins():
        loads["p0"].wait()
        loads["q1"].wait()
        own = lax.dot_general(rows_raw[0], cols_side[1], NT, preferred_element_type=F32)
        joins[g] = jnp.pad(own, ((0, 0), (0, LANES - RANK)))
        for c in join_out:
            c.start()

    def pass_joins():
        for k in range(1, 4):
            join_in[k].wait_recv()
            pass_out[k - 1].start()

    def end_joins():
        join_in[0].wait_recv()
        for c in pass_in:
            c.wait_recv()

        def one(i, carry):
            high, low = halves(jnp.pad(joins[i], ((0, LANES - RANK), (0, 0))))
            join_w[i, 0] = high
            join_w[i, 1] = low
            return carry

        lax.fori_loop(0, GROUP, one, 0)
        for c in join_out + pass_out:
            c.wait_send()

    def joined_rows(x, i):
        high, low = halves(x)
        main = jnp.dot(
            jnp.concatenate([high, low], axis=0), join_w[i, 0], preferred_element_type=F32
        )
        return main[:SLICE] + main[SLICE:] + jnp.dot(
            high, join_w[i, 1], preferred_element_type=F32
        )

    def total_of(which, rows):
        r_send[which, 0] = rows
        ra = copies(
            GROUP, g, to_group, lambda k: r_send.at[which, 0],
            ra_slot.at[which], ra_ss.at[which], ra_rs.at[which],
        )
        start(ra)
        ra_slot[which, g] = rows
        arrived(ra)
        one = jnp.sum(ra_slot[which], axis=0)
        r_send[which, 1] = one
        rz = copies(
            DEEP, zc, to_deep, lambda k: r_send.at[which, 1],
            rz_slot.at[which], rz_ss.at[which], rz_rs.at[which],
        )
        start(rz)
        rz_slot[which, zc] = one
        arrived(rz)
        two = jnp.sum(rz_slot[which], axis=0)
        r_send[which, 2] = two
        rx = copies(
            OUTER, xc, to_outer, lambda k: r_send.at[which, 2],
            rx_slot.at[which], rx_ss.at[which], rx_rs.at[which],
        )
        start(rx)
        rx_slot[which, xc] = two
        arrived(rx)
        left_device(ra)
        left_device(rz)
        left_device(rx)
        return jnp.sum(rx_slot[which], axis=0)

    def column_sum(x):
        return jnp.sum(x, axis=0, keepdims=True)

    def partial_sums(j):
        rows = [column_sum(basis[i] * mixed[...]) for i in range(ITERS)]
        rows.append(column_sum(basis[j] * basis[j]))
        rows.append(jnp.zeros((8 - len(rows), COLS), F32))
        return jnp.concatenate(rows, axis=0)

    def column_entries(sums, j):
        norm = jnp.sqrt(sums(ITERS) + EPSILON)
        entries = []
        for i in range(ITERS):
            entry = sums(i) / norm
            entry = jnp.where(i == j, entry / norm, entry)
            entries.append(jnp.where(i > j, jnp.zeros_like(entry), entry))
        return norm, 1.0 / norm, entries

    def arnoldi_column(totals, j):
        norm, scale, entries = column_entries(lambda i: totals[i : i + 1], j)
        place = jnp.maximum(j, 0) * (ITERS + 1)
        hs[place] = norm
        for i in range(ITERS):
            hs[place + 1 + i] = entries[i]
        return scale, entries

    def to_mixed(part, value):
        mixed[part, :] = value

    def iteration(j, carry):
        before = jnp.maximum(j - 1, 0)

        def at_first(*steps):
            @pl.when(j == 0)
            def _():
                for step in steps:
                    step()

        @pl.when(j > 0)
        def _():
            sums_ref[...] = partial_sums(before)

        leaf_terms(0, mixed[...], sums_ref[...])
        at_first(lambda: pl.semaphore_wait(barrier, len(peers)))
        a0 = send_leaf(0)
        at_first(begin_joins, lambda: pad_tree(0), loads["e0"].wait)
        block_product(0)
        leaf_terms(1, direct[...])
        a1 = send_leaf(1)
        arrived(a0)

        low = tree(
            0, lambda: a_slot[0], True,
            while_z=lambda: at_first(lambda: pad_tree(1), lambda: turn_rows(0)),
            while_x=lambda: at_first(pass_joins),
        )
        d = send_down(0, low + riding(x_slot[0])[None])
        at_first(end_joins)

        arrived(a1)
        sums = jnp.sum(x_slot[0, :, :, COLS:], axis=0)
        norm, scale, entries = column_entries(
            lambda i: sums[:, RANK - COLS + i : RANK - COLS + i + 1], j - 1
        )
        scale = jnp.where(j == 0, jnp.ones_like(scale), scale)
        carried[before] = carried[before] * scale[None]
        for i in range(GROUP):
            value = (a_slot[1, i] + joined_rows(low[i], i)) * scale
            for earlier in range(ITERS - 1):
                value = value - entries[earlier] * carried[earlier, i]
            fresh[i] = value
        carried[j] = fresh[...]
        left_device(a0)
        left_device(a1)

        def orthogonalise():
            arrived(d)
            totals = d_slot[0].reshape(COLS, LANES)[:, COLS:].T[RANK - COLS : RANK - COLS + 8]
            scale, entries = arnoldi_column(totals, j - 1)
            scale = jnp.where(j == 0, jnp.ones_like(scale), scale)
            basis[before] = basis[before] * scale
            images[before] = images[before] * scale

            def finish(part, image):
                image = image * scale
                update = mixed[part, :] * scale
                for i in range(ITERS - 1):
                    image = image - entries[i] * images[i, part, :]
                    update = update - entries[i] * basis[i, part, :]
                images[j, part, :] = image
                basis[j, part, :] = update
                high, low = halves(image)
                stacked[part, :COLS] = high
                stacked[part, COLS:] = low

            spread_down(0, finish)

        low = tree(
            1, lambda: fresh[...], False,
            while_z=lambda: at_first(loads["p1"].wait, lambda: turn_rows(1)),
            while_x=orthogonalise,
        )
        e = send_down(1, low)
        at_first(loads["e1"].wait)
        block_product(1)
        left_device(d)
        arrived(e)
        spread_down(1, to_mixed)
        left_device(e)
        return carry

    loads["rhs"].wait()
    loads["q0"].wait()
    lax.fori_loop(0, ITERS, iteration, 0)

    totals = total_of(0, partial_sums(ITERS - 1))
    scale, entries = arnoldi_column(totals, ITERS - 1)
    basis[ITERS - 1] = basis[ITERS - 1] * scale
    images[ITERS - 1] = images[ITERS - 1] * scale
    update = mixed[...] * scale
    for i in range(ITERS):
        update = update - entries[i] * basis[i]
    last = column_sum(update * update)
    totals = total_of(1, jnp.concatenate([last, jnp.zeros((7, COLS), F32)], axis=0))
    last_norm = jnp.sqrt(totals[0:1] + EPSILON)
    zero = jnp.zeros((1, COLS), F32)
    entries = [[zero for column in range(ITERS)] for line in range(ITERS + 1)]
    for column in range(ITERS):
        for line in range(column + 1):
            entries[line][column] = hs[column * (ITERS + 1) + 1 + line]
        if column + 1 < ITERS:
            entries[column + 1][column] = hs[(column + 1) * (ITERS + 1)]
        else:
            entries[column + 1][column] = last_norm
    weights = least_squares(entries, hs[0])
    sol_ref[...] = weights[0] * images[0] + weights[1] * images[1] + weights[2] * images[2]
    for line in range(ITERS + 1):
        hess_ref[line] = jnp.concatenate(entries[line], axis=0)


def solution(mesh):
    dma = pltpu.SemaphoreType.DMA
    tree = (2, GROUP, SLICE, LANES)
    scratch = [
        pltpu.VMEM((2, WIDTH, WIDTH), BF16),
        pltpu.VMEM((2, RANK, WIDTH), BF16),
        pltpu.VMEM((2, WIDTH, LANES), BF16),
        pltpu.VMEM((2, RANK, WIDTH), BF16),
        pltpu.VMEM((2, LEVELS, 2, RANK, RANK), BF16),
        pltpu.VMEM((2, LEVELS, 2, RANK, RANK), BF16),
        pltpu.VMEM((2, LEVELS, 2 * LANES, LANES), BF16),
        pltpu.VMEM((2, LEVELS, 2, LANES, LANES), BF16),
        pltpu.VMEM((ITERS, WIDTH, COLS), F32),
        pltpu.VMEM((ITERS, WIDTH, COLS), F32),
        pltpu.VMEM((WIDTH, COLS), F32),
        pltpu.VMEM((WIDTH, COLS), F32),
        pltpu.VMEM((WIDTH, 2 * COLS), BF16),
        pltpu.VMEM(tree, F32),
        pltpu.VMEM(tree, F32),
        pltpu.VMEM((2, SLICE, LANES), F32),
        pltpu.VMEM((2, DEEP, SLICE, LANES), F32),
        pltpu.VMEM((2, SLICE, LANES), F32),
        pltpu.VMEM((2, OUTER, SLICE, LANES), F32),
        pltpu.VMEM(tree, F32),
        pltpu.VMEM(tree, F32),
        pltpu.VMEM((4, SLICE, LANES), F32),
        pltpu.VMEM((2, SLICE, LANES), F32),
        pltpu.VMEM((4, SLICE, LANES), F32),
        pltpu.VMEM((2, SLICE, LANES), F32),
        pltpu.VMEM((8, SLICE, LANES), F32),
        pltpu.VMEM((4, SLICE, LANES), F32),
        pltpu.VMEM((2, SLICE, LANES), F32),
        pltpu.VMEM((2, 3, 8, COLS), F32),
        pltpu.VMEM((2, GROUP, 8, COLS), F32),
        pltpu.VMEM((2, DEEP, 8, COLS), F32),
        pltpu.VMEM((2, OUTER, 8, COLS), F32),
        pltpu.VMEM((ITERS * (ITERS + 1), 1, COLS), F32),
        pltpu.VMEM((8, COLS), F32),
        pltpu.VMEM((GROUP, RANK, LANES), F32),
        pltpu.VMEM((GROUP, 2, LANES, LANES), BF16),
        pltpu.VMEM((ITERS,) + tree[1:], F32),
        pltpu.VMEM(tree[1:], F32),
        dma((11,)),
        dma((2, GROUP - 1)),
        dma((2, GROUP - 1)),
        dma((2, DEEP - 1)),
        dma((2, DEEP - 1)),
        dma((2, OUTER - 1)),
        dma((2, OUTER - 1)),
        dma((2, GROUP - 1)),
        dma((2, GROUP - 1)),
        dma((2, GROUP - 1)),
        dma((2, GROUP - 1)),
        dma((2, DEEP - 1)),
        dma((2, DEEP - 1)),
        dma((2, OUTER - 1)),
        dma((2, OUTER - 1)),
        dma((7,)),
        dma((7,)),
    ]

    def on_device(*args):
        return pl.pallas_call(
            kernel,
            out_shape=(
                jax.ShapeDtypeStruct((WIDTH, COLS), F32),
                jax.ShapeDtypeStruct((ITERS + 1, ITERS, COLS), F32),
            ),
            in_specs=[pl.BlockSpec(memory_space=pl.ANY)] * 11,
            out_specs=[pl.BlockSpec(memory_space=pltpu.VMEM)] * 2,
            scratch_shapes=scratch,
            compiler_params=pltpu.CompilerParams(
                collective_id=0, has_side_effects=True, vmem_limit_bytes=60 * 2**20
            ),
        )(*args)

    leaf = P("leaf", None)
    block = P("leaf", None, None)
    in_specs = (leaf, block, block, block, P(), P(), block, block, block, P(), P())
    return jax.shard_map(
        on_device, mesh=mesh, in_specs=in_specs, out_specs=(leaf, P()), check_vma=False
    )
```

```python
import jax
import jax.numpy as jnp
from jax import lax
from jax.experimental import pallas as pl
from jax.experimental.pallas import tpu as pltpu
from jax.sharding import PartitionSpec as P

F32 = jnp.float32
BF16 = jnp.bfloat16
MESH = pl.DeviceIdType.MESH

ITERS = 3
EPSILON = 1e-06
WIDTH = 1024
RANK = 200
LANES = 256
COLS = 128
GROUP = 8
DEEP = 8
OUTER = 4
SLICE = COLS // GROUP
LEVELS = 8
TILE = 256
SUMS = 16

NT = (((1,), (1,)), ((), ()))
NN = (((1,), (0,)), ((), ()))


def halves(x):
    high = x.astype(BF16)
    return high, (x - high.astype(F32)).astype(BF16)


def product_rows(x, weight, dims):
    rows = x.shape[0]
    high, low = halves(x)
    both = lax.dot_general(
        jnp.concatenate([high, low], axis=0), weight, dims, preferred_element_type=F32
    )
    return both[:rows] + both[rows:]


def pairs(x):
    count = x.shape[0] // 2
    split = x.reshape(count, 2, SLICE, LANES)
    left = split[:, 0].reshape(count * SLICE, LANES)
    right = split[:, 1].reshape(count * SLICE, LANES)
    return left, right


def two_sum(a, b):
    total = a + b
    shift = total - a
    return total, (a - (total - shift)) + (b - shift)


def add_exact(x, y):
    high, low = two_sum(x[0], y[0])
    low = low + (x[1] + y[1])
    total = high + low
    return total, low - (total - high)


def times_exact(x, y):
    a, b = x[0], y[0]
    a_top = a.astype(BF16).astype(F32)
    b_top = b.astype(BF16).astype(F32)
    a_rest, b_rest = a - a_top, b - b_top
    high = a * b
    low = ((a_top * b_top - high) + a_top * b_rest + a_rest * b_top) + a_rest * b_rest
    low = low + (a * y[1] + b * x[1])
    total = high + low
    return total, low - (total - high)


def least_squares(entries, beta_first):
    unknowns = len(entries[0])
    matrix = [list(line) for line in entries]
    target = [beta_first] + [jnp.zeros_like(beta_first) for column in range(unknowns)]
    for column in range(unknowns):
        upper_entry = matrix[column][column]
        lower_entry = matrix[column + 1][column]
        radius = jnp.sqrt(upper_entry * upper_entry + lower_entry * lower_entry)
        cosine = upper_entry / radius
        sine_value = lower_entry / radius
        for following in range(column, unknowns):
            top_value = matrix[column][following]
            bottom_value = matrix[column + 1][following]
            matrix[column][following] = cosine * top_value + sine_value * bottom_value
            matrix[column + 1][following] = cosine * bottom_value - sine_value * top_value
        top_value = target[column]
        bottom_value = target[column + 1]
        target[column] = cosine * top_value + sine_value * bottom_value
        target[column + 1] = cosine * bottom_value - sine_value * top_value
    coefficients = [None] * unknowns
    for current_row in reversed(range(unknowns)):
        remainder = target[current_row]
        for following in range(current_row + 1, unknowns):
            remainder = remainder - matrix[current_row][following] * coefficients[following]
        coefficients[current_row] = remainder / matrix[current_row][current_row]
    return coefficients


def kernel(
    rhs_hbm,
    ea_hbm,
    pa_hbm,
    qa_hbm,
    ta_hbm,
    ca_hbm,
    em_hbm,
    pm_hbm,
    qm_hbm,
    tm_hbm,
    cm_hbm,
    sol_ref,
    hess_ref,
    blocks,
    rows_raw,
    rows_t,
    cols_side,
    trans_raw,
    coup_raw,
    trans,
    coup,
    basis,
    images,
    mixed,
    direct,
    stacked,
    a_send,
    a_slot,
    z_send,
    z_slot,
    x_send,
    x_slot,
    d_send,
    d_slot,
    c1_ref,
    c2_ref,
    c4_ref,
    c5_ref,
    bridge0,
    bridge1,
    bridge2,
    r_send,
    ra_slot,
    rz_slot,
    rx_slot,
    hs,
    sums_ref,
    joins,
    join_w,
    carried,
    fresh,
    load_sem,
    a_ss,
    a_rs,
    z_ss,
    z_rs,
    x_ss,
    x_rs,
    d_ss,
    d_rs,
    ra_ss,
    ra_rs,
    rz_ss,
    rz_rs,
    rx_ss,
    rx_rs,
    j_ss,
    j_rs,
):
    me = lax.axis_index("leaf")
    g = me % GROUP
    zc = (me // GROUP) % DEEP
    xc = me // (GROUP * DEEP)

    def to_group(k):
        return (me // GROUP) * GROUP + (g + k) % GROUP

    def to_deep(k):
        return xc * (GROUP * DEEP) + ((zc + k) % DEEP) * GROUP + g

    def to_outer(k):
        return ((xc + k) % OUTER) * (GROUP * DEEP) + me % (GROUP * DEEP)

    def load(src, dst, which):
        return pltpu.make_async_copy(src, dst, load_sem.at[which])

    loads = {
        "rhs": load(rhs_hbm, mixed, 0),
        "q0": load(qm_hbm.at[0], cols_side.at[0], 1),
        "p0": load(pm_hbm.at[0], rows_raw.at[0], 5),
        "q1": load(qa_hbm.at[0], cols_side.at[1], 6),
        "t0": load(tm_hbm, trans_raw.at[0], 2),
        "e0": load(em_hbm.at[0], blocks.at[0], 3),
        "c0": load(cm_hbm, coup_raw.at[0], 4),
        "t1": load(ta_hbm, trans_raw.at[1], 7),
        "e1": load(ea_hbm.at[0], blocks.at[1], 8),
        "c1": load(ca_hbm, coup_raw.at[1], 9),
        "p1": load(pa_hbm.at[0], rows_raw.at[1], 10),
    }
    for item in loads.values():
        item.start()

    barrier = pltpu.get_barrier_semaphore()
    peers = [to_group(k) for k in range(1, GROUP)]
    peers += [to_deep(k) for k in range(1, DEEP)]
    peers += [to_outer(k) for k in range(1, OUTER)]
    for peer in peers:
        pl.semaphore_signal(barrier, inc=1, device_id=(peer,), device_id_type=MESH)

    sums_ref[...] = jnp.zeros((8, COLS), F32)
    for i in range(ITERS):
        basis[i] = jnp.zeros((WIDTH, COLS), F32)
        images[i] = jnp.zeros((WIDTH, COLS), F32)
        carried[i] = jnp.zeros((GROUP, SLICE, LANES), F32)

    def pad_tree(op):
        loads["t%d" % op].wait()
        loads["c%d" % op].wait()
        edge = ((0, LANES - RANK), (0, LANES - RANK))

        def one(h, carry):
            for s in range(2):
                trans[op, h, s * LANES : (s + 1) * LANES, :] = jnp.pad(trans_raw[op, h, s], edge)
                coup[op, h, s] = jnp.pad(coup_raw[op, h, s], edge)
            return carry

        lax.fori_loop(0, LEVELS, one, 0)

    def turn_rows(op):
        for t in range(WIDTH // TILE):
            part = rows_raw[op, :, t * TILE : (t + 1) * TILE].astype(F32)
            part = jnp.pad(part, ((0, LANES - RANK), (0, 0)))
            rows_t[op, t * TILE : (t + 1) * TILE, :] = part.T.astype(BF16)

    def copies(count, coord, target, source, slot, send_sem, recv_sem):
        out = []
        arrive = []
        for k in range(1, count):
            out.append(
                pltpu.make_async_remote_copy(
                    src_ref=source(k),
                    dst_ref=slot.at[coord],
                    send_sem=send_sem.at[k - 1],
                    recv_sem=recv_sem.at[k - 1],
                    device_id=(target(k),),
                    device_id_type=MESH,
                )
            )
            arrive.append(
                pltpu.make_async_remote_copy(
                    src_ref=source(k),
                    dst_ref=slot.at[(coord + count - k) % count],
                    send_sem=send_sem.at[k - 1],
                    recv_sem=recv_sem.at[k - 1],
                    device_id=(target(k),),
                    device_id_type=MESH,
                )
            )
        return out, arrive

    def start(group):
        count = len(group[0]) + 1
        for k in sorted(range(1, count), key=lambda k: -min(k, count - k)):
            group[0][k - 1].start()

    def arrived(group):
        for c in group[1]:
            c.wait_recv()

    def left_device(group):
        for c in group[0]:
            c.wait_send()

    def upward(x, op, h):
        left, right = pairs(x)
        joined = product_rows(
            jnp.concatenate([left, right], axis=1), trans[op, h], NN
        )
        return joined.reshape(x.shape[0] // 2, SLICE, LANES)

    def bridges(x, op, h):
        left, right = pairs(x)
        count = x.shape[0] // 2
        first = product_rows(right, coup[op, h, 0], NT).reshape(count, 1, SLICE, LANES)
        second = product_rows(left, coup[op, h, 1], NT).reshape(count, 1, SLICE, LANES)
        return jnp.concatenate([first, second], axis=1).reshape(x.shape)

    def downward(bridge, above, op, h):
        count = above.shape[0]
        moved = product_rows(above.reshape(count * SLICE, LANES), trans[op, h], NT)
        first = moved[:, :LANES].reshape(count, 1, SLICE, LANES)
        second = moved[:, LANES:].reshape(count, 1, SLICE, LANES)
        return bridge + jnp.concatenate([first, second], axis=1).reshape(bridge.shape)

    def own_bridge(values, own, op, h):
        side = own % 2
        return product_rows(values(own + 1 - 2 * side), coup[op, h, side], NT)

    def own_down(above, own, op, h):
        side = own % 2
        weight = trans[op, h, pl.ds(pl.multiple_of(side * LANES, LANES), LANES), :]
        return product_rows(above, weight, NT)

    def riding(x):
        lane = lax.broadcasted_iota(jnp.int32, (SLICE, LANES - COLS), 1)
        total = jnp.sum(x[:, :, COLS:], axis=0)
        total = jnp.where(lane >= RANK - COLS, total, jnp.zeros_like(total))
        return jnp.concatenate([jnp.zeros((SLICE, COLS), F32), total], axis=1)

    def leaf_terms(op, value, sums=None):
        high, low = halves(value)
        stacked[:, :COLS] = high
        stacked[:, COLS:] = low
        both = jnp.dot(cols_side[op], stacked[...], preferred_element_type=F32)
        leaf = both[:, :COLS] + both[:, COLS:]
        rest = LANES - RANK
        if sums is None:
            leaf = jnp.pad(leaf, ((0, rest), (0, 0)))
        else:
            pad = jnp.zeros((rest - 8, COLS), F32)
            leaf = jnp.concatenate([leaf, sums, pad], axis=0)
        a_send[op] = leaf.T.reshape(GROUP, SLICE, LANES)

    def send_leaf(op):
        a = copies(
            GROUP, g, to_group, lambda k: a_send.at[op, (g + k) % GROUP],
            a_slot.at[op], a_ss.at[op], a_rs.at[op],
        )
        start(a)
        a_slot[op, g] = a_send[op, g]
        return a

    def send_down(op, value):
        d_send[op] = value
        d = copies(
            GROUP, g, to_group, lambda k: d_send.at[op, (g + k) % GROUP],
            d_slot.at[op], d_ss.at[op], d_rs.at[op],
        )
        start(d)
        d_slot[op, g] = d_send[op, g]
        return d

    def block_product(op):
        for t in range(WIDTH // TILE):
            both = jnp.dot(
                blocks[op, t * TILE : (t + 1) * TILE, :], stacked[...],
                preferred_element_type=F32,
            )
            direct[t * TILE : (t + 1) * TILE, :] = both[:, :COLS] + both[:, COLS:]

    def spread_down(op, target):
        high, low = halves(d_slot[op].reshape(COLS, LANES))
        spread = jnp.concatenate([high, low], axis=0)
        for t in range(WIDTH // TILE):
            part = slice(t * TILE, (t + 1) * TILE)
            both = lax.dot_general(rows_t[op, part, :], spread, NT, preferred_element_type=F32)
            target(part, direct[part, :] + both[:, :COLS] + both[:, COLS:])

    def tree(op, leaves, sums, while_z=None, while_x=None):
        c1 = upward(leaves(), op, 0)
        c1_ref[...] = c1
        c2 = upward(c1, op, 1)
        c2_ref[...] = c2
        c3 = upward(c2, op, 2)
        c3 = c3[0] + riding(leaves()) if sums else c3[0]
        z_send[op] = c3
        z = copies(
            DEEP, zc, to_deep, lambda k: z_send.at[op],
            z_slot.at[op], z_ss.at[op], z_rs.at[op],
        )
        start(z)
        z_slot[op, zc] = c3
        bridge0[...] = bridges(leaves(), op, 0)
        bridge1[...] = bridges(c1_ref[...], op, 1)
        bridge2[...] = bridges(c2_ref[...], op, 2)
        if while_z is not None:
            while_z()
        arrived(z)
        c4 = upward(z_slot[op], op, 3)
        c4_ref[...] = c4
        c5 = upward(c4, op, 4)
        c5_ref[...] = c5
        c6 = upward(c5, op, 5)
        c6 = c6[0] + riding(z_slot[op]) if sums else c6[0]
        x_send[op] = c6
        x = copies(
            OUTER, xc, to_outer, lambda k: x_send.at[op],
            x_slot.at[op], x_ss.at[op], x_rs.at[op],
        )
        start(x)
        x_slot[op, xc] = c6
        near3 = own_bridge(lambda n: z_slot[op, n], zc, op, 3)
        near4 = own_bridge(lambda n: c4_ref[n], zc // 2, op, 4)
        near5 = own_bridge(lambda n: c5_ref[n], zc // 4, op, 5)
        if while_x is not None:
            while_x()
        arrived(x)
        c7 = upward(x_slot[op], op, 6)
        near6 = own_bridge(lambda n: x_slot[op, n], xc, op, 6)
        c4_ref[0:2] = c7
        d7 = own_bridge(lambda n: c4_ref[n], xc // 2, op, 7)
        d6 = near6 + own_down(d7, xc, op, 6)
        d5 = near5 + own_down(d6, zc // 4, op, 5)
        d4 = near4 + own_down(d5, zc // 2, op, 4)
        d3 = near3 + own_down(d4, zc, op, 3)
        d2 = downward(bridge2[...], d3.reshape(1, SLICE, LANES), op, 2)
        d1 = downward(bridge1[...], d2, op, 1)
        d0 = downward(bridge0[...], d1, op, 0)
        left_device(z)
        left_device(x)
        return d0

    partner = g + 1 - 2 * (g % 2)
    join_out = []
    join_in = []
    for k in range(4):
        to = to_group(2 * k) if k else (me // GROUP) * GROUP + partner
        source = (g + GROUP - 2 * k) % GROUP if k else partner
        for group, where in ((join_out, g), (join_in, source)):
            group.append(
                pltpu.make_async_remote_copy(
                    src_ref=joins.at[g], dst_ref=joins.at[where],
                    send_sem=j_ss.at[k], recv_sem=j_rs.at[k],
                    device_id=(to,), device_id_type=MESH,
                )
            )
    pass_out = []
    pass_in = []
    for k in range(1, 4):
        mine = (g + GROUP - 2 * k) % GROUP
        theirs = (partner + GROUP - 2 * k) % GROUP
        for group, where in ((pass_out, mine), (pass_in, theirs)):
            group.append(
                pltpu.make_async_remote_copy(
                    src_ref=joins.at[mine], dst_ref=joins.at[where],
                    send_sem=j_ss.at[3 + k], recv_sem=j_rs.at[3 + k],
                    device_id=((me // GROUP) * GROUP + partner,), device_id_type=MESH,
                )
            )

    def begin_joins():
        loads["p0"].wait()
        loads["q1"].wait()
        own = lax.dot_general(rows_raw[0], cols_side[1], NT, preferred_element_type=F32)
        joins[g] = jnp.pad(own, ((0, 0), (0, LANES - RANK)))
        for c in join_out:
            c.start()

    def pass_joins():
        for k in range(1, 4):
            join_in[k].wait_recv()
            pass_out[k - 1].start()

    def end_joins():
        join_in[0].wait_recv()
        for c in pass_in:
            c.wait_recv()

        def one(i, carry):
            high, low = halves(jnp.pad(joins[i], ((0, LANES - RANK), (0, 0))))
            join_w[i, 0] = high
            join_w[i, 1] = low
            return carry

        lax.fori_loop(0, GROUP, one, 0)
        for c in join_out + pass_out:
            c.wait_send()

    def joined_rows(x, i):
        high, low = halves(x)
        main = jnp.dot(
            jnp.concatenate([high, low], axis=0), join_w[i, 0], preferred_element_type=F32
        )
        return main[:SLICE] + main[SLICE:] + jnp.dot(
            high, join_w[i, 1], preferred_element_type=F32
        )

    def total_of(high, low):
        def gather(stage, rows, count, coord, target, slot, send_sem, recv_sem):
            r_send[stage] = rows
            group = copies(
                count, coord, target, lambda k: r_send.at[stage], slot, send_sem, recv_sem
            )
            start(group)
            slot[coord] = rows
            arrived(group)
            half = SUMS
            pairs_in = [(slot[i, :half], slot[i, half:]) for i in range(count)]
            while len(pairs_in) > 1:
                pairs_in = [
                    add_exact(pairs_in[i], pairs_in[i + 1]) for i in range(0, len(pairs_in), 2)
                ]
            return group, jnp.concatenate(pairs_in[0], axis=0)

        rows = jnp.concatenate([high, low], axis=0)
        ra, rows = gather(0, rows, GROUP, g, to_group, ra_slot, ra_ss, ra_rs)
        rz, rows = gather(1, rows, DEEP, zc, to_deep, rz_slot, rz_ss, rz_rs)
        rx, rows = gather(2, rows, OUTER, xc, to_outer, rx_slot, rx_ss, rx_rs)
        for group in (ra, rz, rx):
            left_device(group)
        return rows

    def column_sum(x):
        return jnp.sum(x, axis=0, keepdims=True)

    def partial_sums(j):
        rows = [column_sum(basis[i] * mixed[...]) for i in range(ITERS)]
        rows.append(column_sum(basis[j] * basis[j]))
        rows.append(jnp.zeros((8 - len(rows), COLS), F32))
        return jnp.concatenate(rows, axis=0)

    def column_entries(sums, j):
        norm = jnp.sqrt(sums(ITERS) + EPSILON)
        entries = []
        for i in range(ITERS):
            entry = sums(i) / norm
            entry = jnp.where(i == j, entry / norm, entry)
            entries.append(jnp.where(i > j, jnp.zeros_like(entry), entry))
        return norm, 1.0 / norm, entries

    def arnoldi_column(totals, j):
        norm, scale, entries = column_entries(lambda i: totals[i : i + 1], j)
        place = jnp.maximum(j, 0) * (ITERS + 1)
        hs[place] = norm
        for i in range(ITERS):
            hs[place + 1 + i] = entries[i]
        return scale, entries

    def to_mixed(part, value):
        mixed[part, :] = value

    def iteration(j, carry):
        before = jnp.maximum(j - 1, 0)

        def at_first(*steps):
            @pl.when(j == 0)
            def _():
                for step in steps:
                    step()

        @pl.when(j > 0)
        def _():
            sums_ref[...] = partial_sums(before)

        leaf_terms(0, mixed[...], sums_ref[...])
        at_first(lambda: pl.semaphore_wait(barrier, len(peers)))
        a0 = send_leaf(0)
        at_first(begin_joins, lambda: pad_tree(0), loads["e0"].wait)
        block_product(0)
        leaf_terms(1, direct[...])
        a1 = send_leaf(1)
        arrived(a0)

        low = tree(
            0, lambda: a_slot[0], True,
            while_z=lambda: at_first(lambda: pad_tree(1), lambda: turn_rows(0)),
            while_x=lambda: at_first(pass_joins),
        )
        d = send_down(0, low + riding(x_slot[0])[None])
        at_first(end_joins)

        arrived(a1)
        sums = jnp.sum(x_slot[0, :, :, COLS:], axis=0)
        norm, scale, entries = column_entries(
            lambda i: sums[:, RANK - COLS + i : RANK - COLS + i + 1], j - 1
        )
        scale = jnp.where(j == 0, jnp.ones_like(scale), scale)
        carried[before] = carried[before] * scale[None]
        for i in range(GROUP):
            value = (a_slot[1, i] + joined_rows(low[i], i)) * scale
            for earlier in range(ITERS - 1):
                value = value - entries[earlier] * carried[earlier, i]
            fresh[i] = value
        carried[j] = fresh[...]
        left_device(a0)
        left_device(a1)

        def orthogonalise():
            arrived(d)
            totals = d_slot[0].reshape(COLS, LANES)[:, COLS:].T[RANK - COLS : RANK - COLS + 8]
            scale, entries = arnoldi_column(totals, j - 1)
            scale = jnp.where(j == 0, jnp.ones_like(scale), scale)
            basis[before] = basis[before] * scale
            images[before] = images[before] * scale

            def finish(part, image):
                image = image * scale
                update = mixed[part, :] * scale
                for i in range(ITERS - 1):
                    image = image - entries[i] * images[i, part, :]
                    update = update - entries[i] * basis[i, part, :]
                images[j, part, :] = image
                basis[j, part, :] = update
                high, low = halves(image)
                stacked[part, :COLS] = high
                stacked[part, COLS:] = low

            spread_down(0, finish)

        low = tree(
            1, lambda: fresh[...], False,
            while_z=lambda: at_first(loads["p1"].wait, lambda: turn_rows(1)),
            while_x=orthogonalise,
        )
        e = send_down(1, low)
        at_first(loads["e1"].wait)
        block_product(1)
        left_device(d)
        arrived(e)
        spread_down(1, to_mixed)
        left_device(e)
        return carry

    loads["rhs"].wait()
    loads["q0"].wait()
    lax.fori_loop(0, ITERS, iteration, 0)

    earlier_norm = hs[(ITERS - 2) * (ITERS + 1)]
    shrink = 1.0 / earlier_norm
    which = [(0, 3), (1, 3), (2, 3), (2, 2), (3, 3), (0, 0), (0, 1), (0, 2), (1, 1), (1, 2)]
    step = 64

    def one_step(t, carry):
        rows = pl.ds(pl.multiple_of(t * step, step), step)
        parts = [basis[i, rows, :] for i in range(ITERS)] + [mixed[rows, :] * shrink]
        out = []
        for (first, second), total in zip(which, carry):
            term = jnp.sum((parts[first] * parts[second]).reshape(step // 8, 8, COLS), axis=0)
            high, low = two_sum(total[0], term)
            out.append((high, total[1] + low))
        return tuple(out)

    nothing = jnp.zeros((8, COLS), F32)
    sums = lax.fori_loop(0, WIDTH // step, one_step, ((nothing, nothing),) * len(which))
    highs, lows = [], []
    for total in sums:
        for shift in (4, 2, 1):
            total = add_exact(total, tuple(pltpu.roll(x, shift, 0) for x in total))
        highs.append(total[0][0:1])
        lows.append(total[1][0:1])
    rest = [jnp.zeros((SUMS - len(which), COLS), F32)]
    totals = total_of(
        jnp.concatenate(highs + rest, axis=0), jnp.concatenate(lows + rest, axis=0)
    )
    inner = {
        pair: (totals[i : i + 1], totals[SUMS + i : SUMS + i + 1]) for i, pair in enumerate(which)
    }
    norm = jnp.sqrt(inner[2, 2][0] + EPSILON)
    hs[(ITERS - 1) * (ITERS + 1)] = norm
    lead = earlier_norm / norm
    weights_of = []
    for i in range(ITERS):
        entry = inner[i, ITERS][0] * lead
        if i == ITERS - 1:
            entry = entry / norm
        hs[(ITERS - 1) * (ITERS + 1) + 1 + i] = entry
        weights_of.append(-entry if i < ITERS - 1 else -(entry / norm))
    weights_of.append(lead)
    square = None
    for first, second in which:
        plain = (weights_of[first], jnp.zeros_like(norm))
        other = (weights_of[second], jnp.zeros_like(norm))
        term = times_exact(times_exact(plain, other), inner[first, second])
        if first != second:
            term = (2.0 * term[0], 2.0 * term[1])
        square = term if square is None else add_exact(square, term)
    last_norm = jnp.sqrt(jnp.maximum(square[0], jnp.zeros_like(norm)) + EPSILON)
    scale = 1.0 / norm
    zero = jnp.zeros((1, COLS), F32)
    entries = [[zero for column in range(ITERS)] for line in range(ITERS + 1)]
    for column in range(ITERS):
        for line in range(column + 1):
            entries[line][column] = hs[column * (ITERS + 1) + 1 + line]
        if column + 1 < ITERS:
            entries[column + 1][column] = hs[(column + 1) * (ITERS + 1)]
        else:
            entries[column + 1][column] = last_norm
    weights = least_squares(entries, hs[0])
    weights[ITERS - 1] = weights[ITERS - 1] * scale
    sol_ref[...] = weights[0] * images[0] + weights[1] * images[1] + weights[2] * images[2]
    for line in range(ITERS + 1):
        hess_ref[line] = jnp.concatenate(entries[line], axis=0)


def solution(mesh):
    dma = pltpu.SemaphoreType.DMA
    tree = (2, GROUP, SLICE, LANES)
    scratch = [
        pltpu.VMEM((2, WIDTH, WIDTH), BF16),
        pltpu.VMEM((2, RANK, WIDTH), BF16),
        pltpu.VMEM((2, WIDTH, LANES), BF16),
        pltpu.VMEM((2, RANK, WIDTH), BF16),
        pltpu.VMEM((2, LEVELS, 2, RANK, RANK), BF16),
        pltpu.VMEM((2, LEVELS, 2, RANK, RANK), BF16),
        pltpu.VMEM((2, LEVELS, 2 * LANES, LANES), BF16),
        pltpu.VMEM((2, LEVELS, 2, LANES, LANES), BF16),
        pltpu.VMEM((ITERS, WIDTH, COLS), F32),
        pltpu.VMEM((ITERS, WIDTH, COLS), F32),
        pltpu.VMEM((WIDTH, COLS), F32),
        pltpu.VMEM((WIDTH, COLS), F32),
        pltpu.VMEM((WIDTH, 2 * COLS), BF16),
        pltpu.VMEM(tree, F32),
        pltpu.VMEM(tree, F32),
        pltpu.VMEM((2, SLICE, LANES), F32),
        pltpu.VMEM((2, DEEP, SLICE, LANES), F32),
        pltpu.VMEM((2, SLICE, LANES), F32),
        pltpu.VMEM((2, OUTER, SLICE, LANES), F32),
        pltpu.VMEM(tree, F32),
        pltpu.VMEM(tree, F32),
        pltpu.VMEM((4, SLICE, LANES), F32),
        pltpu.VMEM((2, SLICE, LANES), F32),
        pltpu.VMEM((4, SLICE, LANES), F32),
        pltpu.VMEM((2, SLICE, LANES), F32),
        pltpu.VMEM((8, SLICE, LANES), F32),
        pltpu.VMEM((4, SLICE, LANES), F32),
        pltpu.VMEM((2, SLICE, LANES), F32),
        pltpu.VMEM((3, 2 * SUMS, COLS), F32),
        pltpu.VMEM((GROUP, 2 * SUMS, COLS), F32),
        pltpu.VMEM((DEEP, 2 * SUMS, COLS), F32),
        pltpu.VMEM((OUTER, 2 * SUMS, COLS), F32),
        pltpu.VMEM((ITERS * (ITERS + 1), 1, COLS), F32),
        pltpu.VMEM((8, COLS), F32),
        pltpu.VMEM((GROUP, RANK, LANES), F32),
        pltpu.VMEM((GROUP, 2, LANES, LANES), BF16),
        pltpu.VMEM((ITERS,) + tree[1:], F32),
        pltpu.VMEM(tree[1:], F32),
        dma((11,)),
        dma((2, GROUP - 1)),
        dma((2, GROUP - 1)),
        dma((2, DEEP - 1)),
        dma((2, DEEP - 1)),
        dma((2, OUTER - 1)),
        dma((2, OUTER - 1)),
        dma((2, GROUP - 1)),
        dma((2, GROUP - 1)),
        dma((GROUP - 1,)),
        dma((GROUP - 1,)),
        dma((DEEP - 1,)),
        dma((DEEP - 1,)),
        dma((OUTER - 1,)),
        dma((OUTER - 1,)),
        dma((7,)),
        dma((7,)),
    ]

    def on_device(*args):
        return pl.pallas_call(
            kernel,
            out_shape=(
                jax.ShapeDtypeStruct((WIDTH, COLS), F32),
                jax.ShapeDtypeStruct((ITERS + 1, ITERS, COLS), F32),
            ),
            in_specs=[pl.BlockSpec(memory_space=pl.ANY)] * 11,
            out_specs=[pl.BlockSpec(memory_space=pltpu.VMEM)] * 2,
            scratch_shapes=scratch,
            compiler_params=pltpu.CompilerParams(
                collective_id=0, has_side_effects=True, vmem_limit_bytes=60 * 2**20
            ),
        )(*args)

    leaf = P("leaf", None)
    block = P("leaf", None, None)
    in_specs = (leaf, block, block, block, P(), P(), block, block, block, P(), P())
    return jax.shard_map(
        on_device, mesh=mesh, in_specs=in_specs, out_specs=(leaf, P()), check_vma=False
    )
```

```python
import jax
import jax.numpy as jnp
from jax import lax
from jax.experimental import pallas as pl
from jax.experimental.pallas import tpu as pltpu
from jax.sharding import PartitionSpec as P

F32 = jnp.float32
BF16 = jnp.bfloat16
MESH = pl.DeviceIdType.MESH

ITERS = 3
EPSILON = 1e-06
WIDTH = 1024
RANK = 200
LANES = 256
COLS = 128
GROUP = 8
DEEP = 8
OUTER = 4
SLICE = COLS // GROUP
LEVELS = 8
TILE = 256
SUMS = 16

NT = (((1,), (1,)), ((), ()))
NN = (((1,), (0,)), ((), ()))


def halves(x):
    high = x.astype(BF16)
    return high, (x - high.astype(F32)).astype(BF16)


def product_rows(x, weight, dims):
    rows = x.shape[0]
    high, low = halves(x)
    both = lax.dot_general(
        jnp.concatenate([high, low], axis=0), weight, dims, preferred_element_type=F32
    )
    return both[:rows] + both[rows:]


def pairs(x):
    count = x.shape[0] // 2
    split = x.reshape(count, 2, SLICE, LANES)
    left = split[:, 0].reshape(count * SLICE, LANES)
    right = split[:, 1].reshape(count * SLICE, LANES)
    return left, right


def two_sum(a, b):
    total = a + b
    shift = total - a
    return total, (a - (total - shift)) + (b - shift)


def add_exact(x, y):
    high, low = two_sum(x[0], y[0])
    low = low + (x[1] + y[1])
    total = high + low
    return total, low - (total - high)


def times_exact(x, y):
    a, b = x[0], y[0]
    a_top = a.astype(BF16).astype(F32)
    b_top = b.astype(BF16).astype(F32)
    a_rest, b_rest = a - a_top, b - b_top
    high = a * b
    low = ((a_top * b_top - high) + a_top * b_rest + a_rest * b_top) + a_rest * b_rest
    low = low + (a * y[1] + b * x[1])
    total = high + low
    return total, low - (total - high)


def least_squares(entries, beta_first):
    unknowns = len(entries[0])
    matrix = [list(line) for line in entries]
    target = [beta_first] + [jnp.zeros_like(beta_first) for column in range(unknowns)]
    for column in range(unknowns):
        upper_entry = matrix[column][column]
        lower_entry = matrix[column + 1][column]
        radius = jnp.sqrt(upper_entry * upper_entry + lower_entry * lower_entry)
        cosine = upper_entry / radius
        sine_value = lower_entry / radius
        for following in range(column, unknowns):
            top_value = matrix[column][following]
            bottom_value = matrix[column + 1][following]
            matrix[column][following] = cosine * top_value + sine_value * bottom_value
            matrix[column + 1][following] = cosine * bottom_value - sine_value * top_value
        top_value = target[column]
        bottom_value = target[column + 1]
        target[column] = cosine * top_value + sine_value * bottom_value
        target[column + 1] = cosine * bottom_value - sine_value * top_value
    coefficients = [None] * unknowns
    for current_row in reversed(range(unknowns)):
        remainder = target[current_row]
        for following in range(current_row + 1, unknowns):
            remainder = remainder - matrix[current_row][following] * coefficients[following]
        coefficients[current_row] = remainder / matrix[current_row][current_row]
    return coefficients


def kernel(
    rhs_hbm,
    ea_hbm,
    pa_hbm,
    qa_hbm,
    ta_hbm,
    ca_hbm,
    em_hbm,
    pm_hbm,
    qm_hbm,
    tm_hbm,
    cm_hbm,
    sol_ref,
    hess_ref,
    blocks,
    rows_raw,
    rows_t,
    cols_side,
    trans_raw,
    coup_raw,
    trans,
    coup,
    basis,
    images,
    mixed,
    direct,
    stacked,
    a_send,
    a_slot,
    z_send,
    z_slot,
    x_send,
    x_slot,
    d_send,
    d_slot,
    c1_ref,
    c2_ref,
    c4_ref,
    c5_ref,
    bridge0,
    bridge1,
    bridge2,
    r_send,
    ra_slot,
    rz_slot,
    rx_slot,
    hs,
    sums_ref,
    joins,
    join_w,
    carried,
    fresh_m,
    fresh_a,
    applied,
    load_sem,
    a_ss,
    a_rs,
    z_ss,
    z_rs,
    x_ss,
    x_rs,
    d_ss,
    d_rs,
    ra_ss,
    ra_rs,
    rz_ss,
    rz_rs,
    rx_ss,
    rx_rs,
    j_ss,
    j_rs,
):
    me = lax.axis_index("leaf")
    g = me % GROUP
    zc = (me // GROUP) % DEEP
    xc = me // (GROUP * DEEP)

    def to_group(k):
        return (me // GROUP) * GROUP + (g + k) % GROUP

    def to_deep(k):
        return xc * (GROUP * DEEP) + ((zc + k) % DEEP) * GROUP + g

    def to_outer(k):
        return ((xc + k) % OUTER) * (GROUP * DEEP) + me % (GROUP * DEEP)

    def load(src, dst, which):
        return pltpu.make_async_copy(src, dst, load_sem.at[which])

    loads = {
        "rhs": load(rhs_hbm, mixed, 0),
        "q0": load(qm_hbm.at[0], cols_side.at[0], 1),
        "p0": load(pm_hbm.at[0], rows_raw.at[0], 5),
        "q1": load(qa_hbm.at[0], cols_side.at[1], 6),
        "p1": load(pa_hbm.at[0], rows_raw.at[1], 10),
        "t0": load(tm_hbm, trans_raw.at[0], 2),
        "e0": load(em_hbm.at[0], blocks.at[0], 3),
        "c0": load(cm_hbm, coup_raw.at[0], 4),
        "t1": load(ta_hbm, trans_raw.at[1], 7),
        "e1": load(ea_hbm.at[0], blocks.at[1], 8),
        "c1": load(ca_hbm, coup_raw.at[1], 9),
    }
    for item in loads.values():
        item.start()

    barrier = pltpu.get_barrier_semaphore()
    peers = [to_group(k) for k in range(1, GROUP)]
    peers += [to_deep(k) for k in range(1, DEEP)]
    peers += [to_outer(k) for k in range(1, OUTER)]
    for peer in peers:
        pl.semaphore_signal(barrier, inc=1, device_id=(peer,), device_id_type=MESH)

    sums_ref[...] = jnp.zeros((8, COLS), F32)
    for i in range(ITERS):
        basis[i] = jnp.zeros((WIDTH, COLS), F32)
        images[i] = jnp.zeros((WIDTH, COLS), F32)
        carried[i] = jnp.zeros((GROUP, SLICE, LANES), F32)
    for i in range(ITERS - 1):
        applied[i] = jnp.zeros((WIDTH, COLS), F32)

    def pad_tree(op):
        loads["t%d" % op].wait()
        loads["c%d" % op].wait()
        edge = ((0, LANES - RANK), (0, LANES - RANK))

        def one(h, carry):
            for s in range(2):
                trans[op, h, s * LANES : (s + 1) * LANES, :] = jnp.pad(trans_raw[op, h, s], edge)
                coup[op, h, s] = jnp.pad(coup_raw[op, h, s], edge)
            return carry

        lax.fori_loop(0, LEVELS, one, 0)

    def turn_rows(op):
        for t in range(WIDTH // TILE):
            part = rows_raw[op, :, t * TILE : (t + 1) * TILE].astype(F32)
            part = jnp.pad(part, ((0, LANES - RANK), (0, 0)))
            rows_t[op, t * TILE : (t + 1) * TILE, :] = part.T.astype(BF16)

    def copies(count, coord, target, source, slot, send_sem, recv_sem):
        out = []
        arrive = []
        for k in range(1, count):
            out.append(
                pltpu.make_async_remote_copy(
                    src_ref=source(k),
                    dst_ref=slot.at[coord],
                    send_sem=send_sem.at[k - 1],
                    recv_sem=recv_sem.at[k - 1],
                    device_id=(target(k),),
                    device_id_type=MESH,
                )
            )
            arrive.append(
                pltpu.make_async_remote_copy(
                    src_ref=source(k),
                    dst_ref=slot.at[(coord + count - k) % count],
                    send_sem=send_sem.at[k - 1],
                    recv_sem=recv_sem.at[k - 1],
                    device_id=(target(k),),
                    device_id_type=MESH,
                )
            )
        return out, arrive

    def start(group):
        count = len(group[0]) + 1
        for k in sorted(range(1, count), key=lambda k: -min(k, count - k)):
            group[0][k - 1].start()

    def arrived(group):
        for c in group[1]:
            c.wait_recv()

    def left_device(group):
        for c in group[0]:
            c.wait_send()

    def upward(x, op, h):
        left, right = pairs(x)
        joined = product_rows(
            jnp.concatenate([left, right], axis=1), trans[op, h], NN
        )
        return joined.reshape(x.shape[0] // 2, SLICE, LANES)

    def bridges(x, op, h):
        left, right = pairs(x)
        count = x.shape[0] // 2
        first = product_rows(right, coup[op, h, 0], NT).reshape(count, 1, SLICE, LANES)
        second = product_rows(left, coup[op, h, 1], NT).reshape(count, 1, SLICE, LANES)
        return jnp.concatenate([first, second], axis=1).reshape(x.shape)

    def downward(bridge, above, op, h):
        count = above.shape[0]
        moved = product_rows(above.reshape(count * SLICE, LANES), trans[op, h], NT)
        first = moved[:, :LANES].reshape(count, 1, SLICE, LANES)
        second = moved[:, LANES:].reshape(count, 1, SLICE, LANES)
        return bridge + jnp.concatenate([first, second], axis=1).reshape(bridge.shape)

    def own_bridge(values, own, op, h):
        side = own % 2
        return product_rows(values(own + 1 - 2 * side), coup[op, h, side], NT)

    def own_down(above, own, op, h):
        side = own % 2
        weight = trans[op, h, pl.ds(pl.multiple_of(side * LANES, LANES), LANES), :]
        return product_rows(above, weight, NT)

    def riding(x):
        lane = lax.broadcasted_iota(jnp.int32, (SLICE, LANES - COLS), 1)
        total = jnp.sum(x[:, :, COLS:], axis=0)
        total = jnp.where(lane >= RANK - COLS, total, jnp.zeros_like(total))
        return jnp.concatenate([jnp.zeros((SLICE, COLS), F32), total], axis=1)

    def leaf_terms(op, value, sums=None, only_stack=False):
        high, low = halves(value)
        stacked[:, :COLS] = high
        stacked[:, COLS:] = low
        if only_stack:
            return
        both = jnp.dot(cols_side[op], stacked[...], preferred_element_type=F32)
        leaf = both[:, :COLS] + both[:, COLS:]
        rest = LANES - RANK
        if sums is None:
            leaf = jnp.pad(leaf, ((0, rest), (0, 0)))
        else:
            pad = jnp.zeros((rest - 8, COLS), F32)
            leaf = jnp.concatenate([leaf, sums, pad], axis=0)
        a_send[op] = leaf.T.reshape(GROUP, SLICE, LANES)

    def leaf_copies(op):
        return copies(
            GROUP, g, to_group, lambda k: a_send.at[op, (g + k) % GROUP],
            a_slot.at[op], a_ss.at[op], a_rs.at[op],
        )

    def down_copies(op):
        return copies(
            GROUP, g, to_group, lambda k: d_send.at[op, (g + k) % GROUP],
            d_slot.at[op], d_ss.at[op], d_rs.at[op],
        )

    def send_leaf(op):
        start(leaf_copies(op))
        a_slot[op, g] = a_send[op, g]

    def send_down(op, value):
        d_send[op] = value
        start(down_copies(op))
        d_slot[op, g] = d_send[op, g]

    def finished(group):
        arrived(group)
        left_device(group)

    def block_product(op):
        for t in range(WIDTH // TILE):
            both = jnp.dot(
                blocks[op, t * TILE : (t + 1) * TILE, :], stacked[...],
                preferred_element_type=F32,
            )
            direct[t * TILE : (t + 1) * TILE, :] = both[:, :COLS] + both[:, COLS:]

    def spread_down(op, target):
        high, low = halves(d_slot[op].reshape(COLS, LANES))
        spread = jnp.concatenate([high, low], axis=0)
        for t in range(WIDTH // TILE):
            part = slice(t * TILE, (t + 1) * TILE)
            both = lax.dot_general(rows_t[op, part, :], spread, NT, preferred_element_type=F32)
            target(part, direct[part, :] + both[:, :COLS] + both[:, COLS:])

    def tree(op, leaves, sums, while_z=None, while_x=None):
        c1 = upward(leaves(), op, 0)
        c1_ref[...] = c1
        c2 = upward(c1, op, 1)
        c2_ref[...] = c2
        c3 = upward(c2, op, 2)
        c3 = c3[0] + riding(leaves()) if sums else c3[0]
        z_send[op] = c3
        z = copies(
            DEEP, zc, to_deep, lambda k: z_send.at[op],
            z_slot.at[op], z_ss.at[op], z_rs.at[op],
        )
        start(z)
        z_slot[op, zc] = c3
        bridge0[...] = bridges(leaves(), op, 0)
        bridge1[...] = bridges(c1_ref[...], op, 1)
        bridge2[...] = bridges(c2_ref[...], op, 2)
        if while_z is not None:
            while_z()
        arrived(z)
        c4 = upward(z_slot[op], op, 3)
        c4_ref[...] = c4
        c5 = upward(c4, op, 4)
        c5_ref[...] = c5
        c6 = upward(c5, op, 5)
        c6 = c6[0] + riding(z_slot[op]) if sums else c6[0]
        x_send[op] = c6
        x = copies(
            OUTER, xc, to_outer, lambda k: x_send.at[op],
            x_slot.at[op], x_ss.at[op], x_rs.at[op],
        )
        start(x)
        x_slot[op, xc] = c6
        near3 = own_bridge(lambda n: z_slot[op, n], zc, op, 3)
        near4 = own_bridge(lambda n: c4_ref[n], zc // 2, op, 4)
        near5 = own_bridge(lambda n: c5_ref[n], zc // 4, op, 5)
        if while_x is not None:
            while_x()
        arrived(x)
        c7 = upward(x_slot[op], op, 6)
        near6 = own_bridge(lambda n: x_slot[op, n], xc, op, 6)
        c4_ref[0:2] = c7
        d7 = own_bridge(lambda n: c4_ref[n], xc // 2, op, 7)
        d6 = near6 + own_down(d7, xc, op, 6)
        d5 = near5 + own_down(d6, zc // 4, op, 5)
        d4 = near4 + own_down(d5, zc // 2, op, 4)
        d3 = near3 + own_down(d4, zc, op, 3)
        d2 = downward(bridge2[...], d3.reshape(1, SLICE, LANES), op, 2)
        d1 = downward(bridge1[...], d2, op, 1)
        d0 = downward(bridge0[...], d1, op, 0)
        left_device(z)
        left_device(x)
        return d0

    partner = g + 1 - 2 * (g % 2)
    to_partner = (me // GROUP) * GROUP + partner

    def join_copy(op, source, where, k, to):
        return pltpu.make_async_remote_copy(
            src_ref=joins.at[op, source], dst_ref=joins.at[op, where],
            send_sem=j_ss.at[op, k], recv_sem=j_rs.at[op, k],
            device_id=(to,), device_id_type=MESH,
        )

    def join_copies(op):
        out = [join_copy(op, g, g, 0, to_partner)]
        into = [join_copy(op, g, partner, 0, to_partner)]
        for k in range(1, 4):
            out.append(join_copy(op, g, g, k, to_group(2 * k)))
            into.append(join_copy(op, g, (g + GROUP - 2 * k) % GROUP, k, to_group(2 * k)))
        return out, into

    def pass_copies(op):
        out, into = [], []
        for k in range(1, 4):
            mine = (g + GROUP - 2 * k) % GROUP
            theirs = (partner + GROUP - 2 * k) % GROUP
            out.append(join_copy(op, mine, mine, 3 + k, to_partner))
            into.append(join_copy(op, mine, theirs, 3 + k, to_partner))
        return out, into

    def begin_joins(op):
        own = lax.dot_general(rows_raw[op], cols_side[1 - op], NT, preferred_element_type=F32)
        joins[op, g] = jnp.pad(own, ((0, 0), (0, LANES - RANK)))
        for c in join_copies(op)[0]:
            c.start()

    def pass_joins(op):
        for came, further in zip(join_copies(op)[1][1:], pass_copies(op)[0]):
            came.wait_recv()
            further.start()

    def end_joins(op):
        join_copies(op)[1][0].wait_recv()
        for c in pass_copies(op)[1]:
            c.wait_recv()

        def one(i, carry):
            high, low = halves(jnp.pad(joins[op, i], ((0, LANES - RANK), (0, 0))))
            join_w[op, i, 0] = high
            join_w[op, i, 1] = low
            return carry

        lax.fori_loop(0, GROUP, one, 0)
        for c in join_copies(op)[0] + pass_copies(op)[0]:
            c.wait_send()

    def joined_rows(op, x, i):
        high, low = halves(x)
        main = jnp.dot(
            jnp.concatenate([high, low], axis=0), join_w[op, i, 0], preferred_element_type=F32
        )
        return main[:SLICE] + main[SLICE:] + jnp.dot(
            high, join_w[op, i, 1], preferred_element_type=F32
        )

    def total_of(high, low):
        def gather(stage, rows, count, coord, target, slot, send_sem, recv_sem):
            r_send[stage] = rows
            group = copies(
                count, coord, target, lambda k: r_send.at[stage], slot, send_sem, recv_sem
            )
            start(group)
            slot[coord] = rows
            arrived(group)
            half = SUMS
            pairs_in = [(slot[i, :half], slot[i, half:]) for i in range(count)]
            while len(pairs_in) > 1:
                pairs_in = [
                    add_exact(pairs_in[i], pairs_in[i + 1]) for i in range(0, len(pairs_in), 2)
                ]
            return group, jnp.concatenate(pairs_in[0], axis=0)

        rows = jnp.concatenate([high, low], axis=0)
        ra, rows = gather(0, rows, GROUP, g, to_group, ra_slot, ra_ss, ra_rs)
        rz, rows = gather(1, rows, DEEP, zc, to_deep, rz_slot, rz_ss, rz_rs)
        rx, rows = gather(2, rows, OUTER, xc, to_outer, rx_slot, rx_ss, rx_rs)
        for group in (ra, rz, rx):
            left_device(group)
        return rows

    def column_sum(x):
        return jnp.sum(x, axis=0, keepdims=True)

    def partial_sums(j):
        rows = [column_sum(basis[i] * mixed[...]) for i in range(ITERS)]
        rows.append(column_sum(basis[j] * basis[j]))
        rows.append(jnp.zeros((8 - len(rows), COLS), F32))
        return jnp.concatenate(rows, axis=0)

    def column_entries(sums, j):
        norm = jnp.sqrt(sums(ITERS) + EPSILON)
        entries = []
        for i in range(ITERS):
            entry = sums(i) / norm
            entry = jnp.where(i == j, entry / norm, entry)
            entries.append(jnp.where(i > j, jnp.zeros_like(entry), entry))
        return norm, 1.0 / norm, entries

    def arnoldi_column(totals, j):
        norm, scale, entries = column_entries(lambda i: totals[i : i + 1], j)
        place = jnp.maximum(j, 0) * (ITERS + 1)
        hs[place] = norm
        for i in range(ITERS):
            hs[place + 1 + i] = entries[i]
        return scale, entries

    def settle(j):
        d = down_copies(1)
        finished(d)
        totals = d_slot[1].reshape(COLS, LANES)[:, COLS:].T[RANK - COLS : RANK - COLS + 8]
        scale, entries = arnoldi_column(totals, j - 1)
        scale = jnp.where(j == 0, jnp.ones_like(scale), scale)
        before = jnp.maximum(j - 1, 0)
        basis[before] = basis[before] * scale
        images[before] = images[before] * scale
        applied[before] = mixed[...] * scale

        def finish(part, value):
            value = value * scale
            update = mixed[part, :] * scale
            image = images[j, part, :] * scale
            for i in range(ITERS - 1):
                value = value - entries[i] * applied[i, part, :]
                update = update - entries[i] * basis[i, part, :]
                image = image - entries[i] * images[i, part, :]
            basis[j, part, :] = update
            images[j, part, :] = image
            mixed[part, :] = value

        spread_down(1, finish)

    def iteration(j, carry):
        before = jnp.maximum(j - 1, 0)

        def at_first(*steps):
            @pl.when(j == 0)
            def _():
                for step in steps:
                    step()

        def in_m_tree():
            at_first(lambda: pad_tree(1), lambda: turn_rows(0))

            @pl.when(j > 0)
            def _():
                settle(before)
                sums_ref[...] = partial_sums(before)
                leaf_terms(0, mixed[...], only_stack=True)
                block_product(0)
                leaf_terms(1, direct[...], sums_ref[...])
                send_leaf(1)

        low = tree(
            0, lambda: fresh_m[...], False,
            while_z=in_m_tree, while_x=lambda: at_first(lambda: pass_joins(0)),
        )
        send_down(0, low)
        at_first(lambda: end_joins(0))
        finished(leaf_copies(1))
        for i in range(GROUP):
            fresh_a[i] = a_slot[1, i] + joined_rows(0, low[i], i)

        def in_a_tree():
            at_first(lambda: turn_rows(1))
            d = down_copies(0)
            finished(d)

            def to_image(part, value):
                images[j, part, :] = value
                high, low = halves(value)
                stacked[part, :COLS] = high
                stacked[part, COLS:] = low

            spread_down(0, to_image)
            at_first(loads["e1"].wait)
            block_product(1)

            @pl.when(j < ITERS - 1)
            def _():
                leaf_terms(0, direct[...])
                send_leaf(0)

        low = tree(
            1, lambda: fresh_a[...], True,
            while_z=in_a_tree, while_x=lambda: at_first(lambda: pass_joins(1)),
        )
        send_down(1, low + riding(x_slot[1])[None])
        at_first(lambda: end_joins(1))

        @pl.when(j < ITERS - 1)
        def _():
            finished(leaf_copies(0))
            sums = jnp.sum(x_slot[1, :, :, COLS:], axis=0)
            norm, scale, entries = column_entries(
                lambda i: sums[:, RANK - COLS + i : RANK - COLS + i + 1], j - 1
            )
            scale = jnp.where(j == 0, jnp.ones_like(scale), scale)
            carried[before] = carried[before] * scale[None]
            for i in range(GROUP):
                value = (a_slot[0, i] + joined_rows(1, low[i], i)) * scale
                for earlier in range(ITERS - 2):
                    value = value - entries[earlier] * carried[earlier, i]
                fresh_m[i] = value
            carried[j] = fresh_m[...]

        return carry

    loads["rhs"].wait()
    loads["q0"].wait()
    leaf_terms(0, mixed[...])
    pl.semaphore_wait(barrier, len(peers))
    send_leaf(0)
    loads["p0"].wait()
    loads["q1"].wait()
    begin_joins(0)
    pad_tree(0)
    loads["e0"].wait()
    block_product(0)
    leaf_terms(1, direct[...], sums_ref[...])
    send_leaf(1)
    loads["p1"].wait()
    begin_joins(1)
    finished(leaf_copies(0))
    fresh_m[...] = a_slot[0]
    lax.fori_loop(0, ITERS, iteration, 0)
    settle(ITERS - 1)

    earlier_norm = hs[(ITERS - 2) * (ITERS + 1)]
    shrink = 1.0 / earlier_norm
    which = [(0, 3), (1, 3), (2, 3), (2, 2), (3, 3), (0, 0), (0, 1), (0, 2), (1, 1), (1, 2)]
    step = 64

    def one_step(t, carry):
        rows = pl.ds(pl.multiple_of(t * step, step), step)
        parts = [basis[i, rows, :] for i in range(ITERS)] + [mixed[rows, :] * shrink]
        out = []
        for (first, second), total in zip(which, carry):
            term = jnp.sum((parts[first] * parts[second]).reshape(step // 8, 8, COLS), axis=0)
            high, low = two_sum(total[0], term)
            out.append((high, total[1] + low))
        return tuple(out)

    nothing = jnp.zeros((8, COLS), F32)
    sums = lax.fori_loop(0, WIDTH // step, one_step, ((nothing, nothing),) * len(which))
    highs, lows = [], []
    for total in sums:
        for shift in (4, 2, 1):
            total = add_exact(total, tuple(pltpu.roll(x, shift, 0) for x in total))
        highs.append(total[0][0:1])
        lows.append(total[1][0:1])
    rest = [jnp.zeros((SUMS - len(which), COLS), F32)]
    totals = total_of(
        jnp.concatenate(highs + rest, axis=0), jnp.concatenate(lows + rest, axis=0)
    )
    inner = {
        pair: (totals[i : i + 1], totals[SUMS + i : SUMS + i + 1]) for i, pair in enumerate(which)
    }
    norm = jnp.sqrt(inner[2, 2][0] + EPSILON)
    hs[(ITERS - 1) * (ITERS + 1)] = norm
    lead = earlier_norm / norm
    weights_of = []
    for i in range(ITERS):
        entry = inner[i, ITERS][0] * lead
        if i == ITERS - 1:
            entry = entry / norm
        hs[(ITERS - 1) * (ITERS + 1) + 1 + i] = entry
        weights_of.append(-entry if i < ITERS - 1 else -(entry / norm))
    weights_of.append(lead)
    square = None
    for first, second in which:
        plain = (weights_of[first], jnp.zeros_like(norm))
        other = (weights_of[second], jnp.zeros_like(norm))
        term = times_exact(times_exact(plain, other), inner[first, second])
        if first != second:
            term = (2.0 * term[0], 2.0 * term[1])
        square = term if square is None else add_exact(square, term)
    last_norm = jnp.sqrt(jnp.maximum(square[0], jnp.zeros_like(norm)) + EPSILON)
    scale = 1.0 / norm
    zero = jnp.zeros((1, COLS), F32)
    entries = [[zero for column in range(ITERS)] for line in range(ITERS + 1)]
    for column in range(ITERS):
        for line in range(column + 1):
            entries[line][column] = hs[column * (ITERS + 1) + 1 + line]
        if column + 1 < ITERS:
            entries[column + 1][column] = hs[(column + 1) * (ITERS + 1)]
        else:
            entries[column + 1][column] = last_norm
    weights = least_squares(entries, hs[0])
    weights[ITERS - 1] = weights[ITERS - 1] * scale
    sol_ref[...] = weights[0] * images[0] + weights[1] * images[1] + weights[2] * images[2]
    for line in range(ITERS + 1):
        hess_ref[line] = jnp.concatenate(entries[line], axis=0)


def solution(mesh):
    dma = pltpu.SemaphoreType.DMA
    tree = (2, GROUP, SLICE, LANES)
    scratch = [
        pltpu.VMEM((2, WIDTH, WIDTH), BF16),
        pltpu.VMEM((2, RANK, WIDTH), BF16),
        pltpu.VMEM((2, WIDTH, LANES), BF16),
        pltpu.VMEM((2, RANK, WIDTH), BF16),
        pltpu.VMEM((2, LEVELS, 2, RANK, RANK), BF16),
        pltpu.VMEM((2, LEVELS, 2, RANK, RANK), BF16),
        pltpu.VMEM((2, LEVELS, 2 * LANES, LANES), BF16),
        pltpu.VMEM((2, LEVELS, 2, LANES, LANES), BF16),
        pltpu.VMEM((ITERS, WIDTH, COLS), F32),
        pltpu.VMEM((ITERS, WIDTH, COLS), F32),
        pltpu.VMEM((WIDTH, COLS), F32),
        pltpu.VMEM((WIDTH, COLS), F32),
        pltpu.VMEM((WIDTH, 2 * COLS), BF16),
        pltpu.VMEM(tree, F32),
        pltpu.VMEM(tree, F32),
        pltpu.VMEM((2, SLICE, LANES), F32),
        pltpu.VMEM((2, DEEP, SLICE, LANES), F32),
        pltpu.VMEM((2, SLICE, LANES), F32),
        pltpu.VMEM((2, OUTER, SLICE, LANES), F32),
        pltpu.VMEM(tree, F32),
        pltpu.VMEM(tree, F32),
        pltpu.VMEM((4, SLICE, LANES), F32),
        pltpu.VMEM((2, SLICE, LANES), F32),
        pltpu.VMEM((4, SLICE, LANES), F32),
        pltpu.VMEM((2, SLICE, LANES), F32),
        pltpu.VMEM((8, SLICE, LANES), F32),
        pltpu.VMEM((4, SLICE, LANES), F32),
        pltpu.VMEM((2, SLICE, LANES), F32),
        pltpu.VMEM((3, 2 * SUMS, COLS), F32),
        pltpu.VMEM((GROUP, 2 * SUMS, COLS), F32),
        pltpu.VMEM((DEEP, 2 * SUMS, COLS), F32),
        pltpu.VMEM((OUTER, 2 * SUMS, COLS), F32),
        pltpu.VMEM((ITERS * (ITERS + 1), 1, COLS), F32),
        pltpu.VMEM((8, COLS), F32),
        pltpu.VMEM((2, GROUP, RANK, LANES), F32),
        pltpu.VMEM((2, GROUP, 2, LANES, LANES), BF16),
        pltpu.VMEM((ITERS,) + tree[1:], F32),
        pltpu.VMEM(tree[1:], F32),
        pltpu.VMEM(tree[1:], F32),
        pltpu.VMEM((ITERS - 1, WIDTH, COLS), F32),
        dma((11,)),
        dma((2, GROUP - 1)),
        dma((2, GROUP - 1)),
        dma((2, DEEP - 1)),
        dma((2, DEEP - 1)),
        dma((2, OUTER - 1)),
        dma((2, OUTER - 1)),
        dma((2, GROUP - 1)),
        dma((2, GROUP - 1)),
        dma((GROUP - 1,)),
        dma((GROUP - 1,)),
        dma((DEEP - 1,)),
        dma((DEEP - 1,)),
        dma((OUTER - 1,)),
        dma((OUTER - 1,)),
        dma((2, 7)),
        dma((2, 7)),
    ]

    def on_device(*args):
        return pl.pallas_call(
            kernel,
            out_shape=(
                jax.ShapeDtypeStruct((WIDTH, COLS), F32),
                jax.ShapeDtypeStruct((ITERS + 1, ITERS, COLS), F32),
            ),
            in_specs=[pl.BlockSpec(memory_space=pl.ANY)] * 11,
            out_specs=[pl.BlockSpec(memory_space=pltpu.VMEM)] * 2,
            scratch_shapes=scratch,
            compiler_params=pltpu.CompilerParams(
                collective_id=0, has_side_effects=True, vmem_limit_bytes=60 * 2**20
            ),
        )(*args)

    leaf = P("leaf", None)
    block = P("leaf", None, None)
    in_specs = (leaf, block, block, block, P(), P(), block, block, block, P(), P())
    return jax.shard_map(
        on_device, mesh=mesh, in_specs=in_specs, out_specs=(leaf, P()), check_vma=False
    )
```

```python
import jax
import jax.numpy as jnp
from jax import lax
from jax.experimental import pallas as pl
from jax.experimental.pallas import tpu as pltpu
from jax.sharding import PartitionSpec as P

F32 = jnp.float32
BF16 = jnp.bfloat16
MESH = pl.DeviceIdType.MESH

ITERS = 3
EPSILON = 1e-06
WIDTH = 1024
RANK = 200
LANES = 256
COLS = 128
GROUP = 8
DEEP = 8
OUTER = 4
SLICE = COLS // GROUP
LEVELS = 8
TILE = 256
SUMS = 12

NT = (((1,), (1,)), ((), ()))
NN = (((1,), (0,)), ((), ()))


def halves(x):
    high = x.astype(BF16)
    return high, (x - high.astype(F32)).astype(BF16)


def product_rows(x, weight, dims):
    rows = x.shape[0]
    high, low = halves(x)
    both = lax.dot_general(
        jnp.concatenate([high, low], axis=0), weight, dims, preferred_element_type=F32
    )
    return both[:rows] + both[rows:]


def pairs(x):
    count = x.shape[0] // 2
    split = x.reshape(count, 2, SLICE, LANES)
    left = split[:, 0].reshape(count * SLICE, LANES)
    right = split[:, 1].reshape(count * SLICE, LANES)
    return left, right


def two_sum(a, b):
    total = a + b
    shift = total - a
    return total, (a - (total - shift)) + (b - shift)


def add_exact(x, y):
    high, low = two_sum(x[0], y[0])
    low = low + (x[1] + y[1])
    total = high + low
    return total, low - (total - high)


def times_exact(x, y):
    a, b = x[0], y[0]
    a_top = a.astype(BF16).astype(F32)
    b_top = b.astype(BF16).astype(F32)
    a_rest, b_rest = a - a_top, b - b_top
    high = a * b
    low = ((a_top * b_top - high) + a_top * b_rest + a_rest * b_top) + a_rest * b_rest
    low = low + (a * y[1] + b * x[1])
    total = high + low
    return total, low - (total - high)


def least_squares(entries, beta_first):
    unknowns = len(entries[0])
    matrix = [list(line) for line in entries]
    target = [beta_first] + [jnp.zeros_like(beta_first) for column in range(unknowns)]
    for column in range(unknowns):
        upper_entry = matrix[column][column]
        lower_entry = matrix[column + 1][column]
        radius = jnp.sqrt(upper_entry * upper_entry + lower_entry * lower_entry)
        cosine = upper_entry / radius
        sine_value = lower_entry / radius
        for following in range(column, unknowns):
            top_value = matrix[column][following]
            bottom_value = matrix[column + 1][following]
            matrix[column][following] = cosine * top_value + sine_value * bottom_value
            matrix[column + 1][following] = cosine * bottom_value - sine_value * top_value
        top_value = target[column]
        bottom_value = target[column + 1]
        target[column] = cosine * top_value + sine_value * bottom_value
        target[column + 1] = cosine * bottom_value - sine_value * top_value
    coefficients = [None] * unknowns
    for current_row in reversed(range(unknowns)):
        remainder = target[current_row]
        for following in range(current_row + 1, unknowns):
            remainder = remainder - matrix[current_row][following] * coefficients[following]
        coefficients[current_row] = remainder / matrix[current_row][current_row]
    return coefficients


def kernel(
    rhs_hbm,
    ea_hbm,
    pa_hbm,
    qa_hbm,
    ta_hbm,
    ca_hbm,
    em_hbm,
    pm_hbm,
    qm_hbm,
    tm_hbm,
    cm_hbm,
    sol_ref,
    hess_ref,
    blocks,
    rows_raw,
    rows_t,
    cols_side,
    trans_raw,
    coup_raw,
    trans,
    coup,
    basis,
    images,
    mixed,
    direct,
    stacked,
    a_send,
    a_slot,
    z_send,
    z_slot,
    x_send,
    x_slot,
    d_send,
    d_slot,
    c1_ref,
    c2_ref,
    c4_ref,
    c5_ref,
    bridge0,
    bridge1,
    bridge2,
    r_send,
    ra_slot,
    rz_slot,
    rx_slot,
    hs,
    sums_ref,
    joins,
    join_w,
    carried,
    fresh_m,
    fresh_a,
    applied,
    load_sem,
    a_ss,
    a_rs,
    z_ss,
    z_rs,
    x_ss,
    x_rs,
    d_ss,
    d_rs,
    ra_ss,
    ra_rs,
    rz_ss,
    rz_rs,
    rx_ss,
    rx_rs,
    j_ss,
    j_rs,
):
    me = lax.axis_index("leaf")
    g = me % GROUP
    zc = (me // GROUP) % DEEP
    xc = me // (GROUP * DEEP)

    def to_group(k):
        return (me // GROUP) * GROUP + (g + k) % GROUP

    def to_deep(k):
        return xc * (GROUP * DEEP) + ((zc + k) % DEEP) * GROUP + g

    def to_outer(k):
        return ((xc + k) % OUTER) * (GROUP * DEEP) + me % (GROUP * DEEP)

    def load(src, dst, which):
        return pltpu.make_async_copy(src, dst, load_sem.at[which])

    loads = {
        "rhs": load(rhs_hbm, mixed, 0),
        "q0": load(qm_hbm.at[0], cols_side.at[0], 1),
        "p0": load(pm_hbm.at[0], rows_raw.at[0], 5),
        "q1": load(qa_hbm.at[0], cols_side.at[1], 6),
        "p1": load(pa_hbm.at[0], rows_raw.at[1], 10),
        "t0": load(tm_hbm, trans_raw.at[0], 2),
        "e0": load(em_hbm.at[0], blocks.at[0], 3),
        "c0": load(cm_hbm, coup_raw.at[0], 4),
        "t1": load(ta_hbm, trans_raw.at[1], 7),
        "e1": load(ea_hbm.at[0], blocks.at[1], 8),
        "c1": load(ca_hbm, coup_raw.at[1], 9),
    }
    for item in loads.values():
        item.start()

    barrier = pltpu.get_barrier_semaphore()
    peers = [to_group(k) for k in range(1, GROUP)]
    peers += [to_deep(k) for k in range(1, DEEP)]
    peers += [to_outer(k) for k in range(1, OUTER)]
    for peer in peers:
        pl.semaphore_signal(barrier, inc=1, device_id=(peer,), device_id_type=MESH)

    sums_ref[...] = jnp.zeros((8, COLS), F32)
    for i in range(ITERS):
        basis[i] = jnp.zeros((WIDTH, COLS), F32)
        images[i] = jnp.zeros((WIDTH, COLS), F32)
        carried[i] = jnp.zeros((GROUP, SLICE, LANES), F32)
    for i in range(ITERS - 1):
        applied[i] = jnp.zeros((WIDTH, COLS), F32)

    def pad_tree(op, low, high):
        if low == 0:
            loads["t%d" % op].wait()
            loads["c%d" % op].wait()
        edge = ((0, LANES - RANK), (0, LANES - RANK))

        def one(h, carry):
            for s in range(2):
                trans[op, h, s * LANES : (s + 1) * LANES, :] = jnp.pad(trans_raw[op, h, s], edge)
                coup[op, h, s] = jnp.pad(coup_raw[op, h, s], edge)
            return carry

        lax.fori_loop(low, high, one, 0)

    def turn_rows(op):
        for t in range(WIDTH // TILE):
            part = rows_raw[op, :, t * TILE : (t + 1) * TILE].astype(F32)
            part = jnp.pad(part, ((0, LANES - RANK), (0, 0)))
            rows_t[op, t * TILE : (t + 1) * TILE, :] = part.T.astype(BF16)

    def copies(count, coord, target, source, slot, send_sem, recv_sem):
        out = []
        arrive = []
        for k in range(1, count):
            out.append(
                pltpu.make_async_remote_copy(
                    src_ref=source(k),
                    dst_ref=slot.at[coord],
                    send_sem=send_sem.at[k - 1],
                    recv_sem=recv_sem.at[k - 1],
                    device_id=(target(k),),
                    device_id_type=MESH,
                )
            )
            arrive.append(
                pltpu.make_async_remote_copy(
                    src_ref=source(k),
                    dst_ref=slot.at[(coord + count - k) % count],
                    send_sem=send_sem.at[k - 1],
                    recv_sem=recv_sem.at[k - 1],
                    device_id=(target(k),),
                    device_id_type=MESH,
                )
            )
        return out, arrive

    def start(group):
        count = len(group[0]) + 1
        for k in sorted(range(1, count), key=lambda k: -min(k, count - k)):
            group[0][k - 1].start()

    def arrived(group):
        for c in group[1]:
            c.wait_recv()

    def left_device(group):
        for c in group[0]:
            c.wait_send()

    def upward(x, op, h):
        left, right = pairs(x)
        joined = product_rows(
            jnp.concatenate([left, right], axis=1), trans[op, h], NN
        )
        return joined.reshape(x.shape[0] // 2, SLICE, LANES)

    def bridges(x, op, h):
        left, right = pairs(x)
        count = x.shape[0] // 2
        first = product_rows(right, coup[op, h, 0], NT).reshape(count, 1, SLICE, LANES)
        second = product_rows(left, coup[op, h, 1], NT).reshape(count, 1, SLICE, LANES)
        return jnp.concatenate([first, second], axis=1).reshape(x.shape)

    def downward(bridge, above, op, h):
        count = above.shape[0]
        moved = product_rows(above.reshape(count * SLICE, LANES), trans[op, h], NT)
        first = moved[:, :LANES].reshape(count, 1, SLICE, LANES)
        second = moved[:, LANES:].reshape(count, 1, SLICE, LANES)
        return bridge + jnp.concatenate([first, second], axis=1).reshape(bridge.shape)

    def own_bridge(values, own, op, h):
        side = own % 2
        return product_rows(values(own + 1 - 2 * side), coup[op, h, side], NT)

    def own_down(above, own, op, h):
        side = own % 2
        weight = trans[op, h, pl.ds(pl.multiple_of(side * LANES, LANES), LANES), :]
        return product_rows(above, weight, NT)

    def riding(x):
        lane = lax.broadcasted_iota(jnp.int32, (SLICE, LANES - COLS), 1)
        total = jnp.sum(x[:, :, COLS:], axis=0)
        total = jnp.where(lane >= RANK - COLS, total, jnp.zeros_like(total))
        return jnp.concatenate([jnp.zeros((SLICE, COLS), F32), total], axis=1)

    def leaf_terms(op, value, sums=None, only_stack=False):
        high, low = halves(value)
        stacked[:, :COLS] = high
        stacked[:, COLS:] = low
        if only_stack:
            return
        both = jnp.dot(cols_side[op], stacked[...], preferred_element_type=F32)
        leaf = both[:, :COLS] + both[:, COLS:]
        rest = LANES - RANK
        if sums is None:
            leaf = jnp.pad(leaf, ((0, rest), (0, 0)))
        else:
            pad = jnp.zeros((rest - 8, COLS), F32)
            leaf = jnp.concatenate([leaf, sums, pad], axis=0)
        a_send[op] = leaf.T.reshape(GROUP, SLICE, LANES)

    def leaf_copies(op):
        return copies(
            GROUP, g, to_group, lambda k: a_send.at[op, (g + k) % GROUP],
            a_slot.at[op], a_ss.at[op], a_rs.at[op],
        )

    def down_copies(op):
        return copies(
            GROUP, g, to_group, lambda k: d_send.at[op, (g + k) % GROUP],
            d_slot.at[op], d_ss.at[op], d_rs.at[op],
        )

    def send_leaf(op):
        start(leaf_copies(op))
        a_slot[op, g] = a_send[op, g]

    def send_down(op, value):
        d_send[op] = value
        start(down_copies(op))
        d_slot[op, g] = d_send[op, g]

    def finished(group):
        arrived(group)
        left_device(group)

    def block_product(op):
        for t in range(WIDTH // TILE):
            both = jnp.dot(
                blocks[op, t * TILE : (t + 1) * TILE, :], stacked[...],
                preferred_element_type=F32,
            )
            direct[t * TILE : (t + 1) * TILE, :] = both[:, :COLS] + both[:, COLS:]

    def spread_down(op, target):
        high, low = halves(d_slot[op].reshape(COLS, LANES))
        spread = jnp.concatenate([high, low], axis=0)
        for t in range(WIDTH // TILE):
            part = slice(t * TILE, (t + 1) * TILE)
            both = lax.dot_general(rows_t[op, part, :], spread, NT, preferred_element_type=F32)
            target(part, direct[part, :] + both[:, :COLS] + both[:, COLS:])

    def tree(op, leaves, sums, while_z=None, while_x=None):
        c1 = upward(leaves(), op, 0)
        c1_ref[...] = c1
        c2 = upward(c1, op, 1)
        c2_ref[...] = c2
        c3 = upward(c2, op, 2)
        c3 = c3[0] + riding(leaves()) if sums else c3[0]
        z_send[op] = c3
        z = copies(
            DEEP, zc, to_deep, lambda k: z_send.at[op],
            z_slot.at[op], z_ss.at[op], z_rs.at[op],
        )
        start(z)
        z_slot[op, zc] = c3
        bridge0[...] = bridges(leaves(), op, 0)
        bridge1[...] = bridges(c1_ref[...], op, 1)
        bridge2[...] = bridges(c2_ref[...], op, 2)
        if while_z is not None:
            while_z()
        arrived(z)
        c4 = upward(z_slot[op], op, 3)
        c4_ref[...] = c4
        c5 = upward(c4, op, 4)
        c5_ref[...] = c5
        c6 = upward(c5, op, 5)
        c6 = c6[0] + riding(z_slot[op]) if sums else c6[0]
        x_send[op] = c6
        x = copies(
            OUTER, xc, to_outer, lambda k: x_send.at[op],
            x_slot.at[op], x_ss.at[op], x_rs.at[op],
        )
        start(x)
        x_slot[op, xc] = c6
        near3 = own_bridge(lambda n: z_slot[op, n], zc, op, 3)
        near4 = own_bridge(lambda n: c4_ref[n], zc // 2, op, 4)
        near5 = own_bridge(lambda n: c5_ref[n], zc // 4, op, 5)
        if while_x is not None:
            while_x()
        arrived(x)
        c7 = upward(x_slot[op], op, 6)
        near6 = own_bridge(lambda n: x_slot[op, n], xc, op, 6)
        c4_ref[0:2] = c7
        d7 = own_bridge(lambda n: c4_ref[n], xc // 2, op, 7)
        d6 = near6 + own_down(d7, xc, op, 6)
        d5 = near5 + own_down(d6, zc // 4, op, 5)
        d4 = near4 + own_down(d5, zc // 2, op, 4)
        d3 = near3 + own_down(d4, zc, op, 3)
        d2 = downward(bridge2[...], d3.reshape(1, SLICE, LANES), op, 2)
        d1 = downward(bridge1[...], d2, op, 1)
        d0 = downward(bridge0[...], d1, op, 0)
        left_device(z)
        left_device(x)
        return d0

    partner = g + 1 - 2 * (g % 2)
    to_partner = (me // GROUP) * GROUP + partner

    def join_copy(op, source, where, k, to):
        return pltpu.make_async_remote_copy(
            src_ref=joins.at[op, source], dst_ref=joins.at[op, where],
            send_sem=j_ss.at[op, k], recv_sem=j_rs.at[op, k],
            device_id=(to,), device_id_type=MESH,
        )

    def join_copies(op):
        out = [join_copy(op, g, g, 0, to_partner)]
        into = [join_copy(op, g, partner, 0, to_partner)]
        for k in range(1, 4):
            out.append(join_copy(op, g, g, k, to_group(2 * k)))
            into.append(join_copy(op, g, (g + GROUP - 2 * k) % GROUP, k, to_group(2 * k)))
        return out, into

    def pass_copies(op):
        out, into = [], []
        for k in range(1, 4):
            mine = (g + GROUP - 2 * k) % GROUP
            theirs = (partner + GROUP - 2 * k) % GROUP
            out.append(join_copy(op, mine, mine, 3 + k, to_partner))
            into.append(join_copy(op, mine, theirs, 3 + k, to_partner))
        return out, into

    def begin_joins(op):
        own = lax.dot_general(rows_raw[op], cols_side[1 - op], NT, preferred_element_type=F32)
        joins[op, g] = jnp.pad(own, ((0, 0), (0, LANES - RANK)))
        for c in join_copies(op)[0]:
            c.start()

    def pass_joins(op):
        for came, further in zip(join_copies(op)[1][1:], pass_copies(op)[0]):
            came.wait_recv()
            further.start()

    def end_joins(op):
        join_copies(op)[1][0].wait_recv()
        for c in pass_copies(op)[1]:
            c.wait_recv()

        def one(i, carry):
            high, low = halves(jnp.pad(joins[op, i], ((0, LANES - RANK), (0, 0))))
            join_w[op, i, 0] = high
            join_w[op, i, 1] = low
            return carry

        lax.fori_loop(0, GROUP, one, 0)
        for c in join_copies(op)[0] + pass_copies(op)[0]:
            c.wait_send()

    def joined_rows(op, x, i):
        high, low = halves(x)
        main = jnp.dot(
            jnp.concatenate([high, low], axis=0), join_w[op, i, 0], preferred_element_type=F32
        )
        return main[:SLICE] + main[SLICE:] + jnp.dot(
            high, join_w[op, i, 1], preferred_element_type=F32
        )

    def total_of(high, low, meanwhile):
        def gather(stage, rows, count, coord, target, slot, send_sem, recv_sem):
            r_send[stage] = rows
            group = copies(
                count, coord, target, lambda k: r_send.at[stage], slot, send_sem, recv_sem
            )
            start(group)
            slot[coord] = rows
            if stage == 0:
                meanwhile()
            arrived(group)
            half = SUMS
            pairs_in = [(slot[i, :half], slot[i, half:]) for i in range(count)]
            while len(pairs_in) > 1:
                pairs_in = [
                    add_exact(pairs_in[i], pairs_in[i + 1]) for i in range(0, len(pairs_in), 2)
                ]
            return group, jnp.concatenate(pairs_in[0], axis=0)

        rows = jnp.concatenate([high, low], axis=0)
        ra, rows = gather(0, rows, GROUP, g, to_group, ra_slot, ra_ss, ra_rs)
        rz, rows = gather(1, rows, DEEP, zc, to_deep, rz_slot, rz_ss, rz_rs)
        rx, rows = gather(2, rows, OUTER, xc, to_outer, rx_slot, rx_ss, rx_rs)
        for group in (ra, rz, rx):
            left_device(group)
        return rows

    def column_sum(x):
        return jnp.sum(x, axis=0, keepdims=True)

    def partial_sums(j):
        rows = [column_sum(basis[i] * mixed[...]) for i in range(ITERS)]
        rows.append(column_sum(basis[j] * basis[j]))
        rows.append(jnp.zeros((8 - len(rows), COLS), F32))
        return jnp.concatenate(rows, axis=0)

    def column_entries(sums, j):
        norm = jnp.sqrt(sums(ITERS) + EPSILON)
        entries = []
        for i in range(ITERS):
            entry = sums(i) / norm
            entry = jnp.where(i == j, entry / norm, entry)
            entries.append(jnp.where(i > j, jnp.zeros_like(entry), entry))
        return norm, 1.0 / norm, entries

    def arnoldi_column(totals, j):
        norm, scale, entries = column_entries(lambda i: totals[i : i + 1], j)
        place = jnp.maximum(j, 0) * (ITERS + 1)
        hs[place] = norm
        for i in range(ITERS):
            hs[place + 1 + i] = entries[i]
        return scale, entries

    def settle(j, last=False):
        d = down_copies(1)
        finished(d)
        totals = d_slot[1].reshape(COLS, LANES)[:, COLS:].T[RANK - COLS : RANK - COLS + 8]
        scale, entries = arnoldi_column(totals, j - 1)
        scale = jnp.where(j == 0, jnp.ones_like(scale), scale)
        before = jnp.maximum(j - 1, 0)
        basis[before] = basis[before] * scale
        if not last:
            applied[before] = mixed[...] * scale

        def finish(part, value):
            value = value * scale
            update = mixed[part, :] * scale
            for i in range(ITERS - 1):
                held = update if last and i == ITERS - 2 else applied[i, part, :]
                value = value - entries[i] * held
            for i in range(ITERS - 1):
                update = update - entries[i] * basis[i, part, :]
            basis[j, part, :] = update
            mixed[part, :] = value
            if not last:
                high, low = halves(value)
                stacked[part, :COLS] = high
                stacked[part, COLS:] = low

        def finish_images():
            images[before] = images[before] * scale
            image = images[j] * scale
            for i in range(ITERS - 1):
                image = image - entries[i] * images[i]
            images[j] = image

        spread_down(1, finish)
        return finish_images

    def iteration(j, carry):
        before = jnp.maximum(j - 1, 0)

        def at_first(*steps):
            @pl.when(j == 0)
            def _():
                for step in steps:
                    step()

        def in_m_tree():
            at_first(
                lambda: pad_tree(0, 3, LEVELS), lambda: pad_tree(1, 0, LEVELS), lambda: turn_rows(0)
            )

            @pl.when(j > 0)
            def _():
                finish_images = settle(before)
                sums_ref[...] = partial_sums(before)
                block_product(0)
                leaf_terms(1, direct[...], sums_ref[...])
                send_leaf(1)
                finish_images()

        low = tree(
            0, lambda: fresh_m[...], False,
            while_z=in_m_tree, while_x=lambda: at_first(lambda: pass_joins(0)),
        )
        send_down(0, low)
        at_first(lambda: end_joins(0))
        finished(leaf_copies(1))
        for i in range(GROUP):
            fresh_a[i] = a_slot[1, i] + joined_rows(0, low[i], i)

        def in_a_tree():
            at_first(lambda: turn_rows(1))
            d = down_copies(0)
            finished(d)

            def to_image(part, value):
                images[j, part, :] = value
                high, low = halves(value)
                stacked[part, :COLS] = high
                stacked[part, COLS:] = low

            spread_down(0, to_image)
            at_first(loads["e1"].wait)
            block_product(1)

            @pl.when(j < ITERS - 1)
            def _():
                leaf_terms(0, direct[...])
                send_leaf(0)

        low = tree(
            1, lambda: fresh_a[...], True,
            while_z=in_a_tree, while_x=lambda: at_first(lambda: pass_joins(1)),
        )
        send_down(1, low + riding(x_slot[1])[None])
        at_first(lambda: end_joins(1))

        @pl.when(j < ITERS - 1)
        def _():
            finished(leaf_copies(0))
            sums = jnp.sum(x_slot[1, :, :, COLS:], axis=0)
            norm, scale, entries = column_entries(
                lambda i: sums[:, RANK - COLS + i : RANK - COLS + i + 1], j - 1
            )
            scale = jnp.where(j == 0, jnp.ones_like(scale), scale)
            carried[before] = carried[before] * scale[None]
            for i in range(GROUP):
                value = (a_slot[0, i] + joined_rows(1, low[i], i)) * scale
                for earlier in range(ITERS - 2):
                    value = value - entries[earlier] * carried[earlier, i]
                fresh_m[i] = value
            carried[j] = fresh_m[...]

        return carry

    loads["rhs"].wait()
    loads["q0"].wait()
    leaf_terms(0, mixed[...])
    pl.semaphore_wait(barrier, len(peers))
    send_leaf(0)
    loads["p0"].wait()
    loads["q1"].wait()
    begin_joins(0)
    pad_tree(0, 0, 3)
    loads["e0"].wait()
    block_product(0)
    leaf_terms(1, direct[...], sums_ref[...])
    send_leaf(1)
    loads["p1"].wait()
    begin_joins(1)
    finished(leaf_copies(0))
    fresh_m[...] = a_slot[0]
    lax.fori_loop(0, ITERS, iteration, 0)
    finish_images = settle(ITERS - 1, last=True)

    earlier_norm = hs[(ITERS - 2) * (ITERS + 1)]
    shrink = 1.0 / earlier_norm
    which = [(0, 3), (1, 3), (2, 3), (2, 2), (3, 3), (0, 0), (0, 1), (0, 2), (1, 1), (1, 2)]
    step = 64

    def one_step(t, carry):
        rows = pl.ds(pl.multiple_of(t * step, step), step)
        parts = [basis[i, rows, :] for i in range(ITERS)] + [mixed[rows, :] * shrink]
        out = []
        for (first, second), total in zip(which, carry):
            term = jnp.sum((parts[first] * parts[second]).reshape(step // 8, 8, COLS), axis=0)
            high, low = two_sum(total[0], term)
            out.append((high, total[1] + low))
        return tuple(out)

    nothing = jnp.zeros((8, COLS), F32)
    sums = lax.fori_loop(0, WIDTH // step, one_step, ((nothing, nothing),) * len(which))
    highs, lows = [], []
    for total in sums:
        for shift in (4, 2, 1):
            total = add_exact(total, tuple(pltpu.roll(x, shift, 0) for x in total))
        highs.append(total[0][0:1])
        lows.append(total[1][0:1])
    rest = [jnp.zeros((SUMS - len(which), COLS), F32)]
    totals = total_of(
        jnp.concatenate(highs + rest, axis=0),
        jnp.concatenate(lows + rest, axis=0),
        finish_images,
    )
    inner = {
        pair: (totals[i : i + 1], totals[SUMS + i : SUMS + i + 1]) for i, pair in enumerate(which)
    }
    norm = jnp.sqrt(inner[2, 2][0] + EPSILON)
    hs[(ITERS - 1) * (ITERS + 1)] = norm
    lead = earlier_norm / norm
    weights_of = []
    for i in range(ITERS):
        entry = inner[i, ITERS][0] * lead
        if i == ITERS - 1:
            entry = entry / norm
        hs[(ITERS - 1) * (ITERS + 1) + 1 + i] = entry
        weights_of.append(-entry if i < ITERS - 1 else -(entry / norm))
    weights_of.append(lead)
    square = None
    for first, second in which:
        plain = (weights_of[first], jnp.zeros_like(norm))
        other = (weights_of[second], jnp.zeros_like(norm))
        term = times_exact(times_exact(plain, other), inner[first, second])
        if first != second:
            term = (2.0 * term[0], 2.0 * term[1])
        square = term if square is None else add_exact(square, term)
    last_norm = jnp.sqrt(jnp.maximum(square[0], jnp.zeros_like(norm)) + EPSILON)
    scale = 1.0 / norm
    zero = jnp.zeros((1, COLS), F32)
    entries = [[zero for column in range(ITERS)] for line in range(ITERS + 1)]
    for column in range(ITERS):
        for line in range(column + 1):
            entries[line][column] = hs[column * (ITERS + 1) + 1 + line]
        if column + 1 < ITERS:
            entries[column + 1][column] = hs[(column + 1) * (ITERS + 1)]
        else:
            entries[column + 1][column] = last_norm
    weights = least_squares(entries, hs[0])
    weights[ITERS - 1] = weights[ITERS - 1] * scale
    sol_ref[...] = weights[0] * images[0] + weights[1] * images[1] + weights[2] * images[2]
    for line in range(ITERS + 1):
        for column in range(ITERS):
            hess_ref[column, line : line + 1, :] = entries[line][column]


def solution(mesh):
    dma = pltpu.SemaphoreType.DMA
    tree = (2, GROUP, SLICE, LANES)
    scratch = [
        pltpu.VMEM((2, WIDTH, WIDTH), BF16),
        pltpu.VMEM((2, RANK, WIDTH), BF16),
        pltpu.VMEM((2, WIDTH, LANES), BF16),
        pltpu.VMEM((2, RANK, WIDTH), BF16),
        pltpu.VMEM((2, LEVELS, 2, RANK, RANK), BF16),
        pltpu.VMEM((2, LEVELS, 2, RANK, RANK), BF16),
        pltpu.VMEM((2, LEVELS, 2 * LANES, LANES), BF16),
        pltpu.VMEM((2, LEVELS, 2, LANES, LANES), BF16),
        pltpu.VMEM((ITERS, WIDTH, COLS), F32),
        pltpu.VMEM((ITERS, WIDTH, COLS), F32),
        pltpu.VMEM((WIDTH, COLS), F32),
        pltpu.VMEM((WIDTH, COLS), F32),
        pltpu.VMEM((WIDTH, 2 * COLS), BF16),
        pltpu.VMEM(tree, F32),
        pltpu.VMEM(tree, F32),
        pltpu.VMEM((2, SLICE, LANES), F32),
        pltpu.VMEM((2, DEEP, SLICE, LANES), F32),
        pltpu.VMEM((2, SLICE, LANES), F32),
        pltpu.VMEM((2, OUTER, SLICE, LANES), F32),
        pltpu.VMEM(tree, F32),
        pltpu.VMEM(tree, F32),
        pltpu.VMEM((4, SLICE, LANES), F32),
        pltpu.VMEM((2, SLICE, LANES), F32),
        pltpu.VMEM((4, SLICE, LANES), F32),
        pltpu.VMEM((2, SLICE, LANES), F32),
        pltpu.VMEM((8, SLICE, LANES), F32),
        pltpu.VMEM((4, SLICE, LANES), F32),
        pltpu.VMEM((2, SLICE, LANES), F32),
        pltpu.VMEM((3, 2 * SUMS, COLS), F32),
        pltpu.VMEM((GROUP, 2 * SUMS, COLS), F32),
        pltpu.VMEM((DEEP, 2 * SUMS, COLS), F32),
        pltpu.VMEM((OUTER, 2 * SUMS, COLS), F32),
        pltpu.VMEM((ITERS * (ITERS + 1), 1, COLS), F32),
        pltpu.VMEM((8, COLS), F32),
        pltpu.VMEM((2, GROUP, RANK, LANES), F32),
        pltpu.VMEM((2, GROUP, 2, LANES, LANES), BF16),
        pltpu.VMEM((ITERS,) + tree[1:], F32),
        pltpu.VMEM(tree[1:], F32),
        pltpu.VMEM(tree[1:], F32),
        pltpu.VMEM((ITERS - 1, WIDTH, COLS), F32),
        dma((11,)),
        dma((2, GROUP - 1)),
        dma((2, GROUP - 1)),
        dma((2, DEEP - 1)),
        dma((2, DEEP - 1)),
        dma((2, OUTER - 1)),
        dma((2, OUTER - 1)),
        dma((2, GROUP - 1)),
        dma((2, GROUP - 1)),
        dma((GROUP - 1,)),
        dma((GROUP - 1,)),
        dma((DEEP - 1,)),
        dma((DEEP - 1,)),
        dma((OUTER - 1,)),
        dma((OUTER - 1,)),
        dma((2, 7)),
        dma((2, 7)),
    ]

    def hand_over(sol_in, hess_in, sol_out, hess_out):
        sol_out[...] = sol_in[...]
        hess_out[...] = hess_in[...]

    def on_device(*args):
        both = pl.pallas_call(
            kernel,
            out_shape=(
                jax.ShapeDtypeStruct((WIDTH, COLS), F32),
                jax.ShapeDtypeStruct((ITERS, ITERS + 1, COLS), F32),
            ),
            in_specs=[pl.BlockSpec(memory_space=pl.ANY)] * 11,
            out_specs=[pl.BlockSpec(memory_space=pltpu.VMEM)] * 2,
            scratch_shapes=scratch,
            compiler_params=pltpu.CompilerParams(
                collective_id=0, has_side_effects=True, vmem_limit_bytes=60 * 2**20
            ),
        )(*args)
        sol, hess = pl.pallas_call(
            hand_over,
            out_shape=tuple(jax.ShapeDtypeStruct(x.shape, x.dtype) for x in both),
            in_specs=[pl.BlockSpec(memory_space=pltpu.VMEM)] * 2,
            out_specs=[pl.BlockSpec(memory_space=pltpu.VMEM)] * 2,
        )(*both)
        return sol, jnp.swapaxes(hess, 0, 1)

    leaf = P("leaf", None)
    block = P("leaf", None, None)
    in_specs = (leaf, block, block, block, P(), P(), block, block, block, P(), P())
    return jax.shard_map(
        on_device, mesh=mesh, in_specs=in_specs, out_specs=(leaf, P()), check_vma=False
    )
```

```python
import jax
import jax.numpy as jnp
from jax import lax
from jax.experimental import pallas as pl
from jax.experimental.pallas import tpu as pltpu
from jax.sharding import PartitionSpec as P

F32 = jnp.float32
BF16 = jnp.bfloat16
MESH = pl.DeviceIdType.MESH

ITERS = 3
EPSILON = 1e-06
WIDTH = 1024
RANK = 200
LANES = 256
COLS = 128
GROUP = 8
DEEP = 8
OUTER = 4
SLICE = COLS // GROUP
LEVELS = 8
TILE = 256
SUMS = 12

NT = (((1,), (1,)), ((), ()))
NN = (((1,), (0,)), ((), ()))


def halves(x):
    high = x.astype(BF16)
    return high, (x - high.astype(F32)).astype(BF16)


def product_rows(x, weight, dims):
    rows = x.shape[0]
    high, low = halves(x)
    both = lax.dot_general(
        jnp.concatenate([high, low], axis=0), weight, dims, preferred_element_type=F32
    )
    return both[:rows] + both[rows:]


def pairs(x):
    count = x.shape[0] // 2
    split = x.reshape(count, 2, SLICE, LANES)
    left = split[:, 0].reshape(count * SLICE, LANES)
    right = split[:, 1].reshape(count * SLICE, LANES)
    return left, right


def two_sum(a, b):
    total = a + b
    shift = total - a
    return total, (a - (total - shift)) + (b - shift)


def add_exact(x, y):
    high, low = two_sum(x[0], y[0])
    low = low + (x[1] + y[1])
    total = high + low
    return total, low - (total - high)


def times_exact(x, y):
    a, b = x[0], y[0]
    a_top = a.astype(BF16).astype(F32)
    b_top = b.astype(BF16).astype(F32)
    a_rest, b_rest = a - a_top, b - b_top
    high = a * b
    low = ((a_top * b_top - high) + a_top * b_rest + a_rest * b_top) + a_rest * b_rest
    low = low + (a * y[1] + b * x[1])
    total = high + low
    return total, low - (total - high)


def least_squares(entries, beta_first):
    unknowns = len(entries[0])
    matrix = [list(line) for line in entries]
    target = [beta_first] + [jnp.zeros_like(beta_first) for column in range(unknowns)]
    for column in range(unknowns):
        upper_entry = matrix[column][column]
        lower_entry = matrix[column + 1][column]
        radius = jnp.sqrt(upper_entry * upper_entry + lower_entry * lower_entry)
        cosine = upper_entry / radius
        sine_value = lower_entry / radius
        for following in range(column, unknowns):
            top_value = matrix[column][following]
            bottom_value = matrix[column + 1][following]
            matrix[column][following] = cosine * top_value + sine_value * bottom_value
            matrix[column + 1][following] = cosine * bottom_value - sine_value * top_value
        top_value = target[column]
        bottom_value = target[column + 1]
        target[column] = cosine * top_value + sine_value * bottom_value
        target[column + 1] = cosine * bottom_value - sine_value * top_value
    coefficients = [None] * unknowns
    for current_row in reversed(range(unknowns)):
        remainder = target[current_row]
        for following in range(current_row + 1, unknowns):
            remainder = remainder - matrix[current_row][following] * coefficients[following]
        coefficients[current_row] = remainder / matrix[current_row][current_row]
    return coefficients


def kernel(
    rhs_hbm,
    ea_hbm,
    pa_hbm,
    qa_hbm,
    ta_hbm,
    ca_hbm,
    em_hbm,
    pm_hbm,
    qm_hbm,
    tm_hbm,
    cm_hbm,
    sol_ref,
    hess_ref,
    blocks,
    rows_raw,
    rows_t,
    cols_side,
    trans_raw,
    coup_raw,
    trans,
    coup,
    basis,
    images,
    mixed,
    direct,
    stacked,
    a_send,
    a_slot,
    z_send,
    z_slot,
    x_send,
    x_slot,
    d_send,
    d_slot,
    c1_ref,
    c2_ref,
    c4_ref,
    c5_ref,
    bridge0,
    bridge1,
    bridge2,
    r_send,
    ra_slot,
    rz_slot,
    rx_slot,
    hs,
    sums_ref,
    joins,
    join_w,
    carried,
    fresh_m,
    fresh_a,
    applied,
    root_w,
    load_sem,
    a_ss,
    a_rs,
    z_ss,
    z_rs,
    x_ss,
    x_rs,
    d_ss,
    d_rs,
    ra_ss,
    ra_rs,
    rz_ss,
    rz_rs,
    rx_ss,
    rx_rs,
    j_ss,
    j_rs,
):
    me = lax.axis_index("leaf")
    g = me % GROUP
    zc = (me // GROUP) % DEEP
    xc = me // (GROUP * DEEP)

    def to_group(k):
        return (me // GROUP) * GROUP + (g + k) % GROUP

    def to_deep(k):
        return xc * (GROUP * DEEP) + ((zc + k) % DEEP) * GROUP + g

    def to_outer(k):
        return ((xc + k) % OUTER) * (GROUP * DEEP) + me % (GROUP * DEEP)

    def load(src, dst, which):
        return pltpu.make_async_copy(src, dst, load_sem.at[which])

    loads = {
        "rhs": load(rhs_hbm, mixed, 0),
        "q0": load(qm_hbm.at[0], cols_side.at[0], 1),
        "p0": load(pm_hbm.at[0], rows_raw.at[0], 5),
        "q1": load(qa_hbm.at[0], cols_side.at[1], 6),
        "p1": load(pa_hbm.at[0], rows_raw.at[1], 10),
        "t0": load(tm_hbm, trans_raw.at[0], 2),
        "e0": load(em_hbm.at[0], blocks.at[0], 3),
        "c0": load(cm_hbm, coup_raw.at[0], 4),
        "t1": load(ta_hbm, trans_raw.at[1], 7),
        "e1": load(ea_hbm.at[0], blocks.at[1], 8),
        "c1": load(ca_hbm, coup_raw.at[1], 9),
    }
    for item in loads.values():
        item.start()

    barrier = pltpu.get_barrier_semaphore()
    peers = [to_group(k) for k in range(1, GROUP)]
    peers += [to_deep(k) for k in range(1, DEEP)]
    peers += [to_outer(k) for k in range(1, OUTER)]
    for peer in peers:
        pl.semaphore_signal(barrier, inc=1, device_id=(peer,), device_id_type=MESH)

    sums_ref[...] = jnp.zeros((8, COLS), F32)
    for i in range(ITERS):
        basis[i] = jnp.zeros((WIDTH, COLS), F32)
        images[i] = jnp.zeros((WIDTH, COLS), F32)
        carried[i] = jnp.zeros((GROUP, SLICE, LANES), F32)
    for i in range(ITERS - 1):
        applied[i] = jnp.zeros((WIDTH, COLS), F32)

    def pad_tree(op, low, high):
        if low == 0:
            loads["t%d" % op].wait()
            loads["c%d" % op].wait()
        edge = ((0, LANES - RANK), (0, LANES - RANK))

        def one(h, carry):
            for s in range(2):
                trans[op, h, s * LANES : (s + 1) * LANES, :] = jnp.pad(trans_raw[op, h, s], edge)
                coup[op, h, s] = jnp.pad(coup_raw[op, h, s], edge)
            return carry

        lax.fori_loop(low, high, one, 0)

    def turn_rows(op):
        for t in range(WIDTH // TILE):
            part = rows_raw[op, :, t * TILE : (t + 1) * TILE].astype(F32)
            part = jnp.pad(part, ((0, LANES - RANK), (0, 0)))
            rows_t[op, t * TILE : (t + 1) * TILE, :] = part.T.astype(BF16)

    def copies(count, coord, target, source, slot, send_sem, recv_sem):
        out = []
        arrive = []
        for k in range(1, count):
            out.append(
                pltpu.make_async_remote_copy(
                    src_ref=source(k),
                    dst_ref=slot.at[coord],
                    send_sem=send_sem.at[k - 1],
                    recv_sem=recv_sem.at[k - 1],
                    device_id=(target(k),),
                    device_id_type=MESH,
                )
            )
            arrive.append(
                pltpu.make_async_remote_copy(
                    src_ref=source(k),
                    dst_ref=slot.at[(coord + count - k) % count],
                    send_sem=send_sem.at[k - 1],
                    recv_sem=recv_sem.at[k - 1],
                    device_id=(target(k),),
                    device_id_type=MESH,
                )
            )
        return out, arrive

    def start(group):
        count = len(group[0]) + 1
        for k in sorted(range(1, count), key=lambda k: -min(k, count - k)):
            group[0][k - 1].start()

    def arrived(group):
        for c in group[1]:
            c.wait_recv()

    def left_device(group):
        for c in group[0]:
            c.wait_send()

    def upward(x, op, h):
        left, right = pairs(x)
        joined = product_rows(
            jnp.concatenate([left, right], axis=1), trans[op, h], NN
        )
        return joined.reshape(x.shape[0] // 2, SLICE, LANES)

    def bridges(x, op, h):
        left, right = pairs(x)
        count = x.shape[0] // 2
        first = product_rows(right, coup[op, h, 0], NT).reshape(count, 1, SLICE, LANES)
        second = product_rows(left, coup[op, h, 1], NT).reshape(count, 1, SLICE, LANES)
        return jnp.concatenate([first, second], axis=1).reshape(x.shape)

    def downward(bridge, above, op, h):
        count = above.shape[0]
        moved = product_rows(above.reshape(count * SLICE, LANES), trans[op, h], NT)
        first = moved[:, :LANES].reshape(count, 1, SLICE, LANES)
        second = moved[:, LANES:].reshape(count, 1, SLICE, LANES)
        return bridge + jnp.concatenate([first, second], axis=1).reshape(bridge.shape)

    def own_bridge(values, own, op, h):
        side = own % 2
        return product_rows(values(own + 1 - 2 * side), coup[op, h, side], NT)

    def own_down(above, own, op, h):
        side = own % 2
        weight = trans[op, h, pl.ds(pl.multiple_of(side * LANES, LANES), LANES), :]
        return product_rows(above, weight, NT)

    def riding(x):
        lane = lax.broadcasted_iota(jnp.int32, (SLICE, LANES - COLS), 1)
        total = jnp.sum(x[:, :, COLS:], axis=0)
        total = jnp.where(lane >= RANK - COLS, total, jnp.zeros_like(total))
        return jnp.concatenate([jnp.zeros((SLICE, COLS), F32), total], axis=1)

    def compose(op):
        def step(h, own):
            side = pl.multiple_of(own % 2 * LANES, LANES)
            return trans[op, h, pl.ds(side, LANES), :]

        path = jnp.dot(step(3, zc), step(4, zc // 2), preferred_element_type=F32)
        path = product_rows(path, step(5, zc // 4), NN)
        near = product_rows(path, coup[op, 6, xc % 2], NN)
        far = product_rows(path, step(6, xc), NN)
        far = product_rows(far, coup[op, 7, xc // 2], NN)
        pieces = [near]
        for s in range(2):
            pieces.append(product_rows(far, trans[op, 6, s * LANES : (s + 1) * LANES, :], NT))
        for i, piece in enumerate(pieces):
            high, low = halves(piece.T)
            root_w[op, 0, i * LANES : (i + 1) * LANES, :] = high
            root_w[op, 1, i * LANES : (i + 1) * LANES, :] = low

    def leaf_terms(op, value, sums=None, only_stack=False):
        high, low = halves(value)
        stacked[:, :COLS] = high
        stacked[:, COLS:] = low
        if only_stack:
            return
        both = jnp.dot(cols_side[op], stacked[...], preferred_element_type=F32)
        leaf = both[:, :COLS] + both[:, COLS:]
        rest = LANES - RANK
        if sums is None:
            leaf = jnp.pad(leaf, ((0, rest), (0, 0)))
        else:
            pad = jnp.zeros((rest - 8, COLS), F32)
            leaf = jnp.concatenate([leaf, sums, pad], axis=0)
        a_send[op] = leaf.T.reshape(GROUP, SLICE, LANES)

    def leaf_copies(op):
        return copies(
            GROUP, g, to_group, lambda k: a_send.at[op, (g + k) % GROUP],
            a_slot.at[op], a_ss.at[op], a_rs.at[op],
        )

    def down_copies(op):
        return copies(
            GROUP, g, to_group, lambda k: d_send.at[op, (g + k) % GROUP],
            d_slot.at[op], d_ss.at[op], d_rs.at[op],
        )

    def send_leaf(op):
        start(leaf_copies(op))
        a_slot[op, g] = a_send[op, g]

    def send_down(op, value):
        d_send[op] = value
        start(down_copies(op))
        d_slot[op, g] = d_send[op, g]

    def finished(group):
        arrived(group)
        left_device(group)

    def block_product(op):
        for t in range(WIDTH // TILE):
            both = jnp.dot(
                blocks[op, t * TILE : (t + 1) * TILE, :], stacked[...],
                preferred_element_type=F32,
            )
            direct[t * TILE : (t + 1) * TILE, :] = both[:, :COLS] + both[:, COLS:]

    def spread_down(op, target):
        high, low = halves(d_slot[op].reshape(COLS, LANES))
        spread = jnp.concatenate([high, low], axis=0)
        for t in range(WIDTH // TILE):
            part = slice(t * TILE, (t + 1) * TILE)
            both = lax.dot_general(rows_t[op, part, :], spread, NT, preferred_element_type=F32)
            target(part, direct[part, :] + both[:, :COLS] + both[:, COLS:])

    def tree(op, leaves, sums, while_z=None, while_x=None):
        c1 = upward(leaves(), op, 0)
        c1_ref[...] = c1
        c2 = upward(c1, op, 1)
        c2_ref[...] = c2
        c3 = upward(c2, op, 2)
        c3 = c3[0] + riding(leaves()) if sums else c3[0]
        z_send[op] = c3
        z = copies(
            DEEP, zc, to_deep, lambda k: z_send.at[op],
            z_slot.at[op], z_ss.at[op], z_rs.at[op],
        )
        start(z)
        z_slot[op, zc] = c3
        bridge0[...] = bridges(leaves(), op, 0)
        bridge1[...] = bridges(c1_ref[...], op, 1)
        bridge2[...] = bridges(c2_ref[...], op, 2)
        if while_z is not None:
            while_z()
        arrived(z)
        c4 = upward(z_slot[op], op, 3)
        c4_ref[...] = c4
        c5 = upward(c4, op, 4)
        c5_ref[...] = c5
        c6 = upward(c5, op, 5)
        c6 = c6[0] + riding(z_slot[op]) if sums else c6[0]
        x_send[op] = c6
        x = copies(
            OUTER, xc, to_outer, lambda k: x_send.at[op],
            x_slot.at[op], x_ss.at[op], x_rs.at[op],
        )
        start(x)
        x_slot[op, xc] = c6
        near3 = own_bridge(lambda n: z_slot[op, n], zc, op, 3)
        near4 = own_bridge(lambda n: c4_ref[n], zc // 2, op, 4)
        near5 = own_bridge(lambda n: c5_ref[n], zc // 4, op, 5)
        near = near3 + own_down(near4 + own_down(near5, zc // 2, op, 4), zc, op, 3)
        if while_x is not None:
            while_x()
        arrived(x)
        other = 2 * (1 - xc // 2)
        above = jnp.concatenate(
            [x_slot[op, xc + 1 - 2 * (xc % 2)], x_slot[op, other], x_slot[op, other + 1]], axis=1
        )
        high, low = halves(above)
        main = jnp.dot(
            jnp.concatenate([high, low], axis=0), root_w[op, 0], preferred_element_type=F32
        )
        rest = jnp.dot(high, root_w[op, 1], preferred_element_type=F32)
        d3 = near + main[:SLICE] + main[SLICE:] + rest
        d2 = downward(bridge2[...], d3.reshape(1, SLICE, LANES), op, 2)
        d1 = downward(bridge1[...], d2, op, 1)
        d0 = downward(bridge0[...], d1, op, 0)
        left_device(z)
        left_device(x)
        return d0

    partner = g + 1 - 2 * (g % 2)
    to_partner = (me // GROUP) * GROUP + partner

    def join_copy(op, source, where, k, to):
        return pltpu.make_async_remote_copy(
            src_ref=joins.at[op, source], dst_ref=joins.at[op, where],
            send_sem=j_ss.at[op, k], recv_sem=j_rs.at[op, k],
            device_id=(to,), device_id_type=MESH,
        )

    def join_copies(op):
        out = [join_copy(op, g, g, 0, to_partner)]
        into = [join_copy(op, g, partner, 0, to_partner)]
        for k in range(1, 4):
            out.append(join_copy(op, g, g, k, to_group(2 * k)))
            into.append(join_copy(op, g, (g + GROUP - 2 * k) % GROUP, k, to_group(2 * k)))
        return out, into

    def pass_copies(op):
        out, into = [], []
        for k in range(1, 4):
            mine = (g + GROUP - 2 * k) % GROUP
            theirs = (partner + GROUP - 2 * k) % GROUP
            out.append(join_copy(op, mine, mine, 3 + k, to_partner))
            into.append(join_copy(op, mine, theirs, 3 + k, to_partner))
        return out, into

    def begin_joins(op):
        own = lax.dot_general(rows_raw[op], cols_side[1 - op], NT, preferred_element_type=F32)
        joins[op, g] = jnp.pad(own, ((0, 0), (0, LANES - RANK)))
        for c in join_copies(op)[0]:
            c.start()

    def pass_joins(op):
        for came, further in zip(join_copies(op)[1][1:], pass_copies(op)[0]):
            came.wait_recv()
            further.start()

    def end_joins(op):
        join_copies(op)[1][0].wait_recv()
        for c in pass_copies(op)[1]:
            c.wait_recv()

        def one(i, carry):
            high, low = halves(jnp.pad(joins[op, i], ((0, LANES - RANK), (0, 0))))
            join_w[op, i, 0] = high
            join_w[op, i, 1] = low
            return carry

        lax.fori_loop(0, GROUP, one, 0)
        for c in join_copies(op)[0] + pass_copies(op)[0]:
            c.wait_send()

    def joined_rows(op, x, i):
        high, low = halves(x)
        main = jnp.dot(
            jnp.concatenate([high, low], axis=0), join_w[op, i, 0], preferred_element_type=F32
        )
        return main[:SLICE] + main[SLICE:] + jnp.dot(
            high, join_w[op, i, 1], preferred_element_type=F32
        )

    def total_of(high, low, meanwhile):
        def gather(stage, rows, count, coord, target, slot, send_sem, recv_sem):
            r_send[stage] = rows
            group = copies(
                count, coord, target, lambda k: r_send.at[stage], slot, send_sem, recv_sem
            )
            start(group)
            slot[coord] = rows
            if stage == 0:
                meanwhile()
            arrived(group)
            half = SUMS
            pairs_in = [(slot[i, :half], slot[i, half:]) for i in range(count)]
            while len(pairs_in) > 1:
                pairs_in = [
                    add_exact(pairs_in[i], pairs_in[i + 1]) for i in range(0, len(pairs_in), 2)
                ]
            return group, jnp.concatenate(pairs_in[0], axis=0)

        rows = jnp.concatenate([high, low], axis=0)
        ra, rows = gather(0, rows, GROUP, g, to_group, ra_slot, ra_ss, ra_rs)
        rz, rows = gather(1, rows, DEEP, zc, to_deep, rz_slot, rz_ss, rz_rs)
        rx, rows = gather(2, rows, OUTER, xc, to_outer, rx_slot, rx_ss, rx_rs)
        for group in (ra, rz, rx):
            left_device(group)
        return rows

    def column_sum(x):
        return jnp.sum(x, axis=0, keepdims=True)

    def partial_sums(j):
        rows = [column_sum(basis[i] * mixed[...]) for i in range(ITERS)]
        rows.append(column_sum(basis[j] * basis[j]))
        rows.append(jnp.zeros((8 - len(rows), COLS), F32))
        return jnp.concatenate(rows, axis=0)

    def column_entries(sums, j):
        norm = jnp.sqrt(sums(ITERS) + EPSILON)
        entries = []
        for i in range(ITERS):
            entry = sums(i) / norm
            entry = jnp.where(i == j, entry / norm, entry)
            entries.append(jnp.where(i > j, jnp.zeros_like(entry), entry))
        return norm, 1.0 / norm, entries

    def arnoldi_column(totals, j):
        norm, scale, entries = column_entries(lambda i: totals[i : i + 1], j)
        place = jnp.maximum(j, 0) * (ITERS + 1)
        hs[place] = norm
        for i in range(ITERS):
            hs[place + 1 + i] = entries[i]
        return scale, entries

    def settle(j, last=False):
        d = down_copies(1)
        finished(d)
        totals = d_slot[1].reshape(COLS, LANES)[:, COLS:].T[RANK - COLS : RANK - COLS + 8]
        scale, entries = arnoldi_column(totals, j - 1)
        scale = jnp.where(j == 0, jnp.ones_like(scale), scale)
        before = jnp.maximum(j - 1, 0)
        basis[before] = basis[before] * scale
        if not last:
            applied[before] = mixed[...] * scale

        def finish(part, value):
            value = value * scale
            update = mixed[part, :] * scale
            for i in range(ITERS - 1):
                held = update if last and i == ITERS - 2 else applied[i, part, :]
                value = value - entries[i] * held
            for i in range(ITERS - 1):
                update = update - entries[i] * basis[i, part, :]
            basis[j, part, :] = update
            mixed[part, :] = value
            if not last:
                high, low = halves(value)
                stacked[part, :COLS] = high
                stacked[part, COLS:] = low

        def finish_images():
            images[before] = images[before] * scale
            image = images[j] * scale
            for i in range(ITERS - 1):
                image = image - entries[i] * images[i]
            images[j] = image

        spread_down(1, finish)
        return finish_images

    def iteration(j, carry):
        before = jnp.maximum(j - 1, 0)

        def at_first(*steps):
            @pl.when(j == 0)
            def _():
                for step in steps:
                    step()

        def in_m_tree():
            at_first(
                lambda: pad_tree(0, 3, LEVELS), lambda: compose(0),
                lambda: pad_tree(1, 0, LEVELS), lambda: turn_rows(0),
            )

            @pl.when(j > 0)
            def _():
                finish_images = settle(before)
                sums_ref[...] = partial_sums(before)
                block_product(0)
                leaf_terms(1, direct[...], sums_ref[...])
                send_leaf(1)
                finish_images()

        low = tree(
            0, lambda: fresh_m[...], False,
            while_z=in_m_tree, while_x=lambda: at_first(lambda: pass_joins(0)),
        )
        send_down(0, low)
        at_first(lambda: end_joins(0))
        finished(leaf_copies(1))
        for i in range(GROUP):
            fresh_a[i] = a_slot[1, i] + joined_rows(0, low[i], i)

        def in_a_tree():
            at_first(lambda: turn_rows(1), lambda: compose(1))
            d = down_copies(0)
            finished(d)

            def to_image(part, value):
                images[j, part, :] = value
                high, low = halves(value)
                stacked[part, :COLS] = high
                stacked[part, COLS:] = low

            spread_down(0, to_image)
            at_first(loads["e1"].wait)
            block_product(1)

            @pl.when(j < ITERS - 1)
            def _():
                leaf_terms(0, direct[...])
                send_leaf(0)

        low = tree(
            1, lambda: fresh_a[...], True,
            while_z=in_a_tree, while_x=lambda: at_first(lambda: pass_joins(1)),
        )
        send_down(1, low + riding(x_slot[1])[None])
        at_first(lambda: end_joins(1))

        @pl.when(j < ITERS - 1)
        def _():
            finished(leaf_copies(0))
            sums = jnp.sum(x_slot[1, :, :, COLS:], axis=0)
            norm, scale, entries = column_entries(
                lambda i: sums[:, RANK - COLS + i : RANK - COLS + i + 1], j - 1
            )
            scale = jnp.where(j == 0, jnp.ones_like(scale), scale)
            carried[before] = carried[before] * scale[None]
            for i in range(GROUP):
                value = (a_slot[0, i] + joined_rows(1, low[i], i)) * scale
                for earlier in range(ITERS - 2):
                    value = value - entries[earlier] * carried[earlier, i]
                fresh_m[i] = value
            carried[j] = fresh_m[...]

        return carry

    loads["rhs"].wait()
    loads["q0"].wait()
    leaf_terms(0, mixed[...])
    pl.semaphore_wait(barrier, len(peers))
    send_leaf(0)
    loads["p0"].wait()
    loads["q1"].wait()
    begin_joins(0)
    pad_tree(0, 0, 3)
    loads["e0"].wait()
    block_product(0)
    leaf_terms(1, direct[...], sums_ref[...])
    send_leaf(1)
    loads["p1"].wait()
    begin_joins(1)
    finished(leaf_copies(0))
    fresh_m[...] = a_slot[0]
    lax.fori_loop(0, ITERS, iteration, 0)
    finish_images = settle(ITERS - 1, last=True)

    earlier_norm = hs[(ITERS - 2) * (ITERS + 1)]
    shrink = 1.0 / earlier_norm
    which = [(0, 3), (1, 3), (2, 3), (2, 2), (3, 3), (0, 0), (0, 1), (0, 2), (1, 1), (1, 2)]
    step = 64

    def one_step(t, carry):
        rows = pl.ds(pl.multiple_of(t * step, step), step)
        parts = [basis[i, rows, :] for i in range(ITERS)] + [mixed[rows, :] * shrink]
        out = []
        for (first, second), total in zip(which, carry):
            term = jnp.sum((parts[first] * parts[second]).reshape(step // 8, 8, COLS), axis=0)
            high, low = two_sum(total[0], term)
            out.append((high, total[1] + low))
        return tuple(out)

    nothing = jnp.zeros((8, COLS), F32)
    sums = lax.fori_loop(0, WIDTH // step, one_step, ((nothing, nothing),) * len(which))
    highs, lows = [], []
    for total in sums:
        for shift in (4, 2, 1):
            total = add_exact(total, tuple(pltpu.roll(x, shift, 0) for x in total))
        highs.append(total[0][0:1])
        lows.append(total[1][0:1])
    rest = [jnp.zeros((SUMS - len(which), COLS), F32)]
    totals = total_of(
        jnp.concatenate(highs + rest, axis=0),
        jnp.concatenate(lows + rest, axis=0),
        finish_images,
    )
    inner = {
        pair: (totals[i : i + 1], totals[SUMS + i : SUMS + i + 1]) for i, pair in enumerate(which)
    }
    norm = jnp.sqrt(inner[2, 2][0] + EPSILON)
    hs[(ITERS - 1) * (ITERS + 1)] = norm
    lead = earlier_norm / norm
    weights_of = []
    for i in range(ITERS):
        entry = inner[i, ITERS][0] * lead
        if i == ITERS - 1:
            entry = entry / norm
        hs[(ITERS - 1) * (ITERS + 1) + 1 + i] = entry
        weights_of.append(-entry if i < ITERS - 1 else -(entry / norm))
    weights_of.append(lead)
    square = None
    for first, second in which:
        plain = (weights_of[first], jnp.zeros_like(norm))
        other = (weights_of[second], jnp.zeros_like(norm))
        term = times_exact(times_exact(plain, other), inner[first, second])
        if first != second:
            term = (2.0 * term[0], 2.0 * term[1])
        square = term if square is None else add_exact(square, term)
    last_norm = jnp.sqrt(jnp.maximum(square[0], jnp.zeros_like(norm)) + EPSILON)
    scale = 1.0 / norm
    zero = jnp.zeros((1, COLS), F32)
    entries = [[zero for column in range(ITERS)] for line in range(ITERS + 1)]
    for column in range(ITERS):
        for line in range(column + 1):
            entries[line][column] = hs[column * (ITERS + 1) + 1 + line]
        if column + 1 < ITERS:
            entries[column + 1][column] = hs[(column + 1) * (ITERS + 1)]
        else:
            entries[column + 1][column] = last_norm
    weights = least_squares(entries, hs[0])
    weights[ITERS - 1] = weights[ITERS - 1] * scale
    sol_ref[...] = weights[0] * images[0] + weights[1] * images[1] + weights[2] * images[2]
    for line in range(ITERS + 1):
        for column in range(ITERS):
            hess_ref[column, line : line + 1, :] = entries[line][column]


def solution(mesh):
    dma = pltpu.SemaphoreType.DMA
    tree = (2, GROUP, SLICE, LANES)
    scratch = [
        pltpu.VMEM((2, WIDTH, WIDTH), BF16),
        pltpu.VMEM((2, RANK, WIDTH), BF16),
        pltpu.VMEM((2, WIDTH, LANES), BF16),
        pltpu.VMEM((2, RANK, WIDTH), BF16),
        pltpu.VMEM((2, LEVELS, 2, RANK, RANK), BF16),
        pltpu.VMEM((2, LEVELS, 2, RANK, RANK), BF16),
        pltpu.VMEM((2, LEVELS, 2 * LANES, LANES), BF16),
        pltpu.VMEM((2, LEVELS, 2, LANES, LANES), BF16),
        pltpu.VMEM((ITERS, WIDTH, COLS), F32),
        pltpu.VMEM((ITERS, WIDTH, COLS), F32),
        pltpu.VMEM((WIDTH, COLS), F32),
        pltpu.VMEM((WIDTH, COLS), F32),
        pltpu.VMEM((WIDTH, 2 * COLS), BF16),
        pltpu.VMEM(tree, F32),
        pltpu.VMEM(tree, F32),
        pltpu.VMEM((2, SLICE, LANES), F32),
        pltpu.VMEM((2, DEEP, SLICE, LANES), F32),
        pltpu.VMEM((2, SLICE, LANES), F32),
        pltpu.VMEM((2, OUTER, SLICE, LANES), F32),
        pltpu.VMEM(tree, F32),
        pltpu.VMEM(tree, F32),
        pltpu.VMEM((4, SLICE, LANES), F32),
        pltpu.VMEM((2, SLICE, LANES), F32),
        pltpu.VMEM((4, SLICE, LANES), F32),
        pltpu.VMEM((2, SLICE, LANES), F32),
        pltpu.VMEM((8, SLICE, LANES), F32),
        pltpu.VMEM((4, SLICE, LANES), F32),
        pltpu.VMEM((2, SLICE, LANES), F32),
        pltpu.VMEM((3, 2 * SUMS, COLS), F32),
        pltpu.VMEM((GROUP, 2 * SUMS, COLS), F32),
        pltpu.VMEM((DEEP, 2 * SUMS, COLS), F32),
        pltpu.VMEM((OUTER, 2 * SUMS, COLS), F32),
        pltpu.VMEM((ITERS * (ITERS + 1), 1, COLS), F32),
        pltpu.VMEM((8, COLS), F32),
        pltpu.VMEM((2, GROUP, RANK, LANES), F32),
        pltpu.VMEM((2, GROUP, 2, LANES, LANES), BF16),
        pltpu.VMEM((ITERS,) + tree[1:], F32),
        pltpu.VMEM(tree[1:], F32),
        pltpu.VMEM(tree[1:], F32),
        pltpu.VMEM((ITERS - 1, WIDTH, COLS), F32),
        pltpu.VMEM((2, 2, 3 * LANES, LANES), BF16),
        dma((11,)),
        dma((2, GROUP - 1)),
        dma((2, GROUP - 1)),
        dma((2, DEEP - 1)),
        dma((2, DEEP - 1)),
        dma((2, OUTER - 1)),
        dma((2, OUTER - 1)),
        dma((2, GROUP - 1)),
        dma((2, GROUP - 1)),
        dma((GROUP - 1,)),
        dma((GROUP - 1,)),
        dma((DEEP - 1,)),
        dma((DEEP - 1,)),
        dma((OUTER - 1,)),
        dma((OUTER - 1,)),
        dma((2, 7)),
        dma((2, 7)),
    ]

    def hand_over(sol_in, hess_in, sol_out, hess_out):
        sol_out[...] = sol_in[...]
        hess_out[...] = hess_in[...]

    def on_device(*args):
        both = pl.pallas_call(
            kernel,
            out_shape=(
                jax.ShapeDtypeStruct((WIDTH, COLS), F32),
                jax.ShapeDtypeStruct((ITERS, ITERS + 1, COLS), F32),
            ),
            in_specs=[pl.BlockSpec(memory_space=pl.ANY)] * 11,
            out_specs=[pl.BlockSpec(memory_space=pltpu.VMEM)] * 2,
            scratch_shapes=scratch,
            compiler_params=pltpu.CompilerParams(
                collective_id=0, has_side_effects=True, vmem_limit_bytes=60 * 2**20
            ),
        )(*args)
        sol, hess = pl.pallas_call(
            hand_over,
            out_shape=tuple(jax.ShapeDtypeStruct(x.shape, x.dtype) for x in both),
            in_specs=[pl.BlockSpec(memory_space=pltpu.VMEM)] * 2,
            out_specs=[pl.BlockSpec(memory_space=pltpu.VMEM)] * 2,
        )(*both)
        return sol, jnp.swapaxes(hess, 0, 1)

    leaf = P("leaf", None)
    block = P("leaf", None, None)
    in_specs = (leaf, block, block, block, P(), P(), block, block, block, P(), P())
    return jax.shard_map(
        on_device, mesh=mesh, in_specs=in_specs, out_specs=(leaf, P()), check_vma=False
    )
```

```python
import jax
import jax.numpy as jnp
from jax import lax
from jax.experimental import pallas as pl
from jax.experimental.pallas import tpu as pltpu
from jax.sharding import PartitionSpec as P

F32 = jnp.float32
BF16 = jnp.bfloat16
MESH = pl.DeviceIdType.MESH

ITERS = 3
EPSILON = 1e-06
WIDTH = 1024
RANK = 200
LANES = 256
COLS = 128
GROUP = 8
DEEP = 8
OUTER = 4
SLICE = COLS // GROUP
LEVELS = 8
TILE = 256
SUMS = 12

NT = (((1,), (1,)), ((), ()))
NN = (((1,), (0,)), ((), ()))


def halves(x):
    high = x.astype(BF16)
    return high, (x - high.astype(F32)).astype(BF16)


def product_rows(x, weight, dims):
    rows = x.shape[0]
    high, low = halves(x)
    both = lax.dot_general(
        jnp.concatenate([high, low], axis=0), weight, dims, preferred_element_type=F32
    )
    return both[:rows] + both[rows:]


def pairs(x):
    count = x.shape[0] // 2
    split = x.reshape(count, 2, SLICE, LANES)
    left = split[:, 0].reshape(count * SLICE, LANES)
    right = split[:, 1].reshape(count * SLICE, LANES)
    return left, right


def two_sum(a, b):
    total = a + b
    shift = total - a
    return total, (a - (total - shift)) + (b - shift)


def add_exact(x, y):
    high, low = two_sum(x[0], y[0])
    low = low + (x[1] + y[1])
    total = high + low
    return total, low - (total - high)


def times_exact(x, y):
    a, b = x[0], y[0]
    a_top = a.astype(BF16).astype(F32)
    b_top = b.astype(BF16).astype(F32)
    a_rest, b_rest = a - a_top, b - b_top
    high = a * b
    low = ((a_top * b_top - high) + a_top * b_rest + a_rest * b_top) + a_rest * b_rest
    low = low + (a * y[1] + b * x[1])
    total = high + low
    return total, low - (total - high)


def least_squares(entries, beta_first):
    unknowns = len(entries[0])
    matrix = [list(line) for line in entries]
    target = [beta_first] + [jnp.zeros_like(beta_first) for column in range(unknowns)]
    for column in range(unknowns):
        upper_entry = matrix[column][column]
        lower_entry = matrix[column + 1][column]
        radius = jnp.sqrt(upper_entry * upper_entry + lower_entry * lower_entry)
        cosine = upper_entry / radius
        sine_value = lower_entry / radius
        for following in range(column, unknowns):
            top_value = matrix[column][following]
            bottom_value = matrix[column + 1][following]
            matrix[column][following] = cosine * top_value + sine_value * bottom_value
            matrix[column + 1][following] = cosine * bottom_value - sine_value * top_value
        top_value = target[column]
        bottom_value = target[column + 1]
        target[column] = cosine * top_value + sine_value * bottom_value
        target[column + 1] = cosine * bottom_value - sine_value * top_value
    coefficients = [None] * unknowns
    for current_row in reversed(range(unknowns)):
        remainder = target[current_row]
        for following in range(current_row + 1, unknowns):
            remainder = remainder - matrix[current_row][following] * coefficients[following]
        coefficients[current_row] = remainder / matrix[current_row][current_row]
    return coefficients


def kernel(
    rhs_hbm,
    ea_hbm,
    pa_hbm,
    qa_hbm,
    ta_hbm,
    ca_hbm,
    em_hbm,
    pm_hbm,
    qm_hbm,
    tm_hbm,
    cm_hbm,
    sol_ref,
    hess_ref,
    blocks,
    rows_raw,
    rows_t,
    cols_side,
    trans_raw,
    coup_raw,
    trans,
    coup,
    basis,
    images,
    mixed,
    direct,
    stacked,
    a_send,
    a_slot,
    z_send,
    z_slot,
    x_send,
    x_slot,
    d_send,
    d_slot,
    c1_ref,
    c2_ref,
    c4_ref,
    c5_ref,
    bridge0,
    bridge1,
    bridge2,
    r_send,
    ra_slot,
    rz_slot,
    rx_slot,
    hs,
    sums_ref,
    joins,
    join_w,
    carried,
    fresh_m,
    fresh_a,
    applied,
    root_w,
    load_sem,
    a_ss,
    a_rs,
    z_ss,
    z_rs,
    x_ss,
    x_rs,
    d_ss,
    d_rs,
    ra_ss,
    ra_rs,
    rz_ss,
    rz_rs,
    rx_ss,
    rx_rs,
    j_ss,
    j_rs,
):
    me = lax.axis_index("leaf")
    g = me % GROUP
    zc = (me // GROUP) % DEEP
    xc = me // (GROUP * DEEP)

    def to_group(k):
        return (me // GROUP) * GROUP + (g + k) % GROUP

    def to_deep(k):
        return xc * (GROUP * DEEP) + ((zc + k) % DEEP) * GROUP + g

    def to_outer(k):
        return ((xc + k) % OUTER) * (GROUP * DEEP) + me % (GROUP * DEEP)

    def load(src, dst, which):
        return pltpu.make_async_copy(src, dst, load_sem.at[which])

    loads = {
        "rhs": load(rhs_hbm, mixed, 0),
        "q0": load(qm_hbm.at[0], cols_side.at[0], 1),
        "p0": load(pm_hbm.at[0], rows_raw.at[0], 5),
        "q1": load(qa_hbm.at[0], cols_side.at[1], 6),
        "p1": load(pa_hbm.at[0], rows_raw.at[1], 10),
        "t0": load(tm_hbm, trans_raw.at[0], 2),
        "e0": load(em_hbm.at[0], blocks.at[0], 3),
        "c0": load(cm_hbm, coup_raw.at[0], 4),
        "t1": load(ta_hbm, trans_raw.at[1], 7),
        "e1": load(ea_hbm.at[0], blocks.at[1], 8),
        "c1": load(ca_hbm, coup_raw.at[1], 9),
    }
    for item in loads.values():
        item.start()

    barrier = pltpu.get_barrier_semaphore()
    peers = [to_group(k) for k in range(1, GROUP)]
    peers += [to_deep(k) for k in range(1, DEEP)]
    peers += [to_outer(k) for k in range(1, OUTER)]
    for peer in peers:
        pl.semaphore_signal(barrier, inc=1, device_id=(peer,), device_id_type=MESH)

    sums_ref[...] = jnp.zeros((8, COLS), F32)
    for i in range(ITERS):
        basis[i] = jnp.zeros((WIDTH, COLS), F32)
        images[i] = jnp.zeros((WIDTH, COLS), F32)
        carried[i] = jnp.zeros((GROUP, SLICE, LANES), F32)
    for i in range(ITERS - 1):
        applied[i] = jnp.zeros((WIDTH, COLS), F32)

    def pad_tree(op, low, high):
        if low == 0:
            loads["t%d" % op].wait()
            loads["c%d" % op].wait()
        edge = ((0, LANES - RANK), (0, LANES - RANK))

        def one(h, carry):
            for s in range(2):
                trans[op, h, s * LANES : (s + 1) * LANES, :] = jnp.pad(trans_raw[op, h, s], edge)
                coup[op, h, s] = jnp.pad(coup_raw[op, h, s], edge)
            return carry

        lax.fori_loop(low, high, one, 0)

    def turn_rows(op):
        for t in range(WIDTH // TILE):
            part = rows_raw[op, :, t * TILE : (t + 1) * TILE].astype(F32)
            part = jnp.pad(part, ((0, LANES - RANK), (0, 0)))
            rows_t[op, t * TILE : (t + 1) * TILE, :] = part.T.astype(BF16)

    def copies(count, coord, target, source, slot, send_sem, recv_sem):
        out = []
        arrive = []
        for k in range(1, count):
            out.append(
                pltpu.make_async_remote_copy(
                    src_ref=source(k),
                    dst_ref=slot.at[coord],
                    send_sem=send_sem.at[k - 1],
                    recv_sem=recv_sem.at[k - 1],
                    device_id=(target(k),),
                    device_id_type=MESH,
                )
            )
            arrive.append(
                pltpu.make_async_remote_copy(
                    src_ref=source(k),
                    dst_ref=slot.at[(coord + count - k) % count],
                    send_sem=send_sem.at[k - 1],
                    recv_sem=recv_sem.at[k - 1],
                    device_id=(target(k),),
                    device_id_type=MESH,
                )
            )
        return out, arrive

    def start(group):
        count = len(group[0]) + 1
        for k in sorted(range(1, count), key=lambda k: -min(k, count - k)):
            group[0][k - 1].start()

    def arrived(group):
        for c in group[1]:
            c.wait_recv()

    def left_device(group):
        for c in group[0]:
            c.wait_send()

    def upward(x, op, h):
        left, right = pairs(x)
        joined = product_rows(
            jnp.concatenate([left, right], axis=1), trans[op, h], NN
        )
        return joined.reshape(x.shape[0] // 2, SLICE, LANES)

    def bridges(x, op, h):
        left, right = pairs(x)
        count = x.shape[0] // 2
        first = product_rows(right, coup[op, h, 0], NT).reshape(count, 1, SLICE, LANES)
        second = product_rows(left, coup[op, h, 1], NT).reshape(count, 1, SLICE, LANES)
        return jnp.concatenate([first, second], axis=1).reshape(x.shape)

    def downward(bridge, above, op, h):
        count = above.shape[0]
        moved = product_rows(above.reshape(count * SLICE, LANES), trans[op, h], NT)
        first = moved[:, :LANES].reshape(count, 1, SLICE, LANES)
        second = moved[:, LANES:].reshape(count, 1, SLICE, LANES)
        return bridge + jnp.concatenate([first, second], axis=1).reshape(bridge.shape)

    def own_bridge(values, own, op, h):
        side = own % 2
        return product_rows(values(own + 1 - 2 * side), coup[op, h, side], NT)

    def own_down(above, own, op, h):
        side = own % 2
        weight = trans[op, h, pl.ds(pl.multiple_of(side * LANES, LANES), LANES), :]
        return product_rows(above, weight, NT)

    def riding(x):
        lane = lax.broadcasted_iota(jnp.int32, (SLICE, LANES - COLS), 1)
        total = jnp.sum(x[:, :, COLS:], axis=0)
        total = jnp.where(lane >= RANK - COLS, total, jnp.zeros_like(total))
        return jnp.concatenate([jnp.zeros((SLICE, COLS), F32), total], axis=1)

    def compose(op):
        def step(h, own):
            side = pl.multiple_of(own % 2 * LANES, LANES)
            return trans[op, h, pl.ds(side, LANES), :]

        path = jnp.dot(step(3, zc), step(4, zc // 2), preferred_element_type=F32)
        path = product_rows(path, step(5, zc // 4), NN)
        near = product_rows(path, coup[op, 6, xc % 2], NN)
        far = product_rows(path, step(6, xc), NN)
        far = product_rows(far, coup[op, 7, xc // 2], NN)
        pieces = [near]
        for s in range(2):
            pieces.append(product_rows(far, trans[op, 6, s * LANES : (s + 1) * LANES, :], NT))
        for i, piece in enumerate(pieces):
            high, low = halves(piece.T)
            root_w[op, 0, i * LANES : (i + 1) * LANES, :] = high
            root_w[op, 1, i * LANES : (i + 1) * LANES, :] = low

    def leaf_terms(op, value, sums=None, only_stack=False):
        high, low = halves(value)
        stacked[:, :COLS] = high
        stacked[:, COLS:] = low
        if only_stack:
            return
        both = jnp.dot(cols_side[op], stacked[...], preferred_element_type=F32)
        leaf = both[:, :COLS] + both[:, COLS:]
        rest = LANES - RANK
        if sums is None:
            leaf = jnp.pad(leaf, ((0, rest), (0, 0)))
        else:
            pad = jnp.zeros((rest - 8, COLS), F32)
            leaf = jnp.concatenate([leaf, sums, pad], axis=0)
        a_send[op] = leaf.T.reshape(GROUP, SLICE, LANES)

    def leaf_copies(op):
        return copies(
            GROUP, g, to_group, lambda k: a_send.at[op, (g + k) % GROUP],
            a_slot.at[op], a_ss.at[op], a_rs.at[op],
        )

    def down_copies(op):
        return copies(
            GROUP, g, to_group, lambda k: d_send.at[op, (g + k) % GROUP],
            d_slot.at[op], d_ss.at[op], d_rs.at[op],
        )

    def send_leaf(op):
        start(leaf_copies(op))
        a_slot[op, g] = a_send[op, g]

    def send_down(op, value):
        d_send[op] = value
        start(down_copies(op))
        d_slot[op, g] = d_send[op, g]

    def finished(group):
        arrived(group)
        left_device(group)

    def block_product(op):
        for t in range(WIDTH // TILE):
            both = jnp.dot(
                blocks[op, t * TILE : (t + 1) * TILE, :], stacked[...],
                preferred_element_type=F32,
            )
            direct[t * TILE : (t + 1) * TILE, :] = both[:, :COLS] + both[:, COLS:]

    def spread_down(op, target):
        high, low = halves(d_slot[op].reshape(COLS, LANES))
        spread = jnp.concatenate([high, low], axis=0)
        for t in range(WIDTH // TILE):
            part = slice(t * TILE, (t + 1) * TILE)
            both = lax.dot_general(rows_t[op, part, :], spread, NT, preferred_element_type=F32)
            target(part, direct[part, :] + both[:, :COLS] + both[:, COLS:])

    def tree(op, leaves, sums, while_z=None, while_x=None):
        c1 = upward(leaves(), op, 0)
        c1_ref[...] = c1
        c2 = upward(c1, op, 1)
        c2_ref[...] = c2
        c3 = upward(c2, op, 2)
        c3 = c3[0] + riding(leaves()) if sums else c3[0]
        z_send[op] = c3
        z = copies(
            DEEP, zc, to_deep, lambda k: z_send.at[op],
            z_slot.at[op], z_ss.at[op], z_rs.at[op],
        )
        start(z)
        z_slot[op, zc] = c3
        bridge0[...] = bridges(leaves(), op, 0)
        bridge1[...] = bridges(c1_ref[...], op, 1)
        bridge2[...] = bridges(c2_ref[...], op, 2)
        if while_z is not None:
            while_z()
        arrived(z)
        c4 = upward(z_slot[op], op, 3)
        c4_ref[...] = c4
        c5 = upward(c4, op, 4)
        c5_ref[...] = c5
        c6 = upward(c5, op, 5)
        c6 = c6[0] + riding(z_slot[op]) if sums else c6[0]
        x_send[op] = c6
        x = copies(
            OUTER, xc, to_outer, lambda k: x_send.at[op],
            x_slot.at[op], x_ss.at[op], x_rs.at[op],
        )
        start(x)
        x_slot[op, xc] = c6
        near3 = own_bridge(lambda n: z_slot[op, n], zc, op, 3)
        near4 = own_bridge(lambda n: c4_ref[n], zc // 2, op, 4)
        near5 = own_bridge(lambda n: c5_ref[n], zc // 4, op, 5)
        near = near3 + own_down(near4 + own_down(near5, zc // 2, op, 4), zc, op, 3)
        if while_x is not None:
            while_x()
        arrived(x)
        other = 2 * (1 - xc // 2)
        above = jnp.concatenate(
            [x_slot[op, xc + 1 - 2 * (xc % 2)], x_slot[op, other], x_slot[op, other + 1]], axis=1
        )
        high, low = halves(above)
        main = jnp.dot(
            jnp.concatenate([high, low], axis=0), root_w[op, 0], preferred_element_type=F32
        )
        rest = jnp.dot(high, root_w[op, 1], preferred_element_type=F32)
        d3 = near + main[:SLICE] + main[SLICE:] + rest
        d2 = downward(bridge2[...], d3.reshape(1, SLICE, LANES), op, 2)
        d1 = downward(bridge1[...], d2, op, 1)
        d0 = downward(bridge0[...], d1, op, 0)
        left_device(z)
        left_device(x)
        return d0

    partner = g + 1 - 2 * (g % 2)
    to_partner = (me // GROUP) * GROUP + partner

    def join_copy(op, source, where, k, to):
        return pltpu.make_async_remote_copy(
            src_ref=joins.at[op, source], dst_ref=joins.at[op, where],
            send_sem=j_ss.at[op, k], recv_sem=j_rs.at[op, k],
            device_id=(to,), device_id_type=MESH,
        )

    def join_copies(op):
        out = [join_copy(op, g, g, 0, to_partner)]
        into = [join_copy(op, g, partner, 0, to_partner)]
        for k in range(1, 4):
            out.append(join_copy(op, g, g, k, to_group(2 * k)))
            into.append(join_copy(op, g, (g + GROUP - 2 * k) % GROUP, k, to_group(2 * k)))
        return out, into

    def pass_copies(op):
        out, into = [], []
        for k in range(1, 4):
            mine = (g + GROUP - 2 * k) % GROUP
            theirs = (partner + GROUP - 2 * k) % GROUP
            out.append(join_copy(op, mine, mine, 3 + k, to_partner))
            into.append(join_copy(op, mine, theirs, 3 + k, to_partner))
        return out, into

    def begin_joins(op):
        own = lax.dot_general(rows_raw[op], cols_side[1 - op], NT, preferred_element_type=F32)
        joins[op, g] = jnp.pad(own, ((0, 0), (0, LANES - RANK)))
        for c in join_copies(op)[0]:
            c.start()

    def ready_joins(op, first):
        def one(k, carry):
            i = (first + 2 * k) % GROUP
            high, low = halves(jnp.pad(joins[op, i], ((0, LANES - RANK), (0, 0))))
            join_w[op, i, 0] = high
            join_w[op, i, 1] = low
            return carry

        lax.fori_loop(0, GROUP // 2, one, 0)

    def pass_joins(op):
        for came, further in zip(join_copies(op)[1][1:], pass_copies(op)[0]):
            came.wait_recv()
            further.start()
        ready_joins(op, g)

    def end_joins(op):
        join_copies(op)[1][0].wait_recv()
        for c in pass_copies(op)[1]:
            c.wait_recv()

        ready_joins(op, partner)
        for c in join_copies(op)[0] + pass_copies(op)[0]:
            c.wait_send()

    def joined_rows(op, x, i):
        high, low = halves(x)
        main = jnp.dot(
            jnp.concatenate([high, low], axis=0), join_w[op, i, 0], preferred_element_type=F32
        )
        return main[:SLICE] + main[SLICE:] + jnp.dot(
            high, join_w[op, i, 1], preferred_element_type=F32
        )

    def total_of(high, low, meanwhile):
        def gather(stage, rows, count, coord, target, slot, send_sem, recv_sem):
            r_send[stage] = rows
            group = copies(
                count, coord, target, lambda k: r_send.at[stage], slot, send_sem, recv_sem
            )
            start(group)
            slot[coord] = rows
            if stage == 0:
                meanwhile()
            arrived(group)
            half = SUMS
            pairs_in = [(slot[i, :half], slot[i, half:]) for i in range(count)]
            while len(pairs_in) > 1:
                pairs_in = [
                    add_exact(pairs_in[i], pairs_in[i + 1]) for i in range(0, len(pairs_in), 2)
                ]
            return group, jnp.concatenate(pairs_in[0], axis=0)

        rows = jnp.concatenate([high, low], axis=0)
        ra, rows = gather(0, rows, GROUP, g, to_group, ra_slot, ra_ss, ra_rs)
        rz, rows = gather(1, rows, DEEP, zc, to_deep, rz_slot, rz_ss, rz_rs)
        rx, rows = gather(2, rows, OUTER, xc, to_outer, rx_slot, rx_ss, rx_rs)
        for group in (ra, rz, rx):
            left_device(group)
        return rows

    def column_sum(x):
        return jnp.sum(x, axis=0, keepdims=True)

    def partial_sums(j):
        rows = [column_sum(basis[i] * mixed[...]) for i in range(ITERS)]
        rows.append(column_sum(basis[j] * basis[j]))
        rows.append(jnp.zeros((8 - len(rows), COLS), F32))
        return jnp.concatenate(rows, axis=0)

    def column_entries(sums, j):
        norm = jnp.sqrt(sums(ITERS) + EPSILON)
        entries = []
        for i in range(ITERS):
            entry = sums(i) / norm
            entry = jnp.where(i == j, entry / norm, entry)
            entries.append(jnp.where(i > j, jnp.zeros_like(entry), entry))
        return norm, 1.0 / norm, entries

    def arnoldi_column(totals, j):
        norm, scale, entries = column_entries(lambda i: totals[i : i + 1], j)
        place = jnp.maximum(j, 0) * (ITERS + 1)
        hs[place] = norm
        for i in range(ITERS):
            hs[place + 1 + i] = entries[i]
        return scale, entries

    def settle(j, last=False):
        d = down_copies(1)
        finished(d)
        totals = d_slot[1].reshape(COLS, LANES)[:, COLS:].T[RANK - COLS : RANK - COLS + 8]
        scale, entries = arnoldi_column(totals, j - 1)
        scale = jnp.where(j == 0, jnp.ones_like(scale), scale)
        before = jnp.maximum(j - 1, 0)
        basis[before] = basis[before] * scale
        if not last:
            applied[before] = mixed[...] * scale

        def finish(part, value):
            value = value * scale
            update = mixed[part, :] * scale
            for i in range(ITERS - 1):
                held = update if last and i == ITERS - 2 else applied[i, part, :]
                value = value - entries[i] * held
            for i in range(ITERS - 1):
                update = update - entries[i] * basis[i, part, :]
            basis[j, part, :] = update
            mixed[part, :] = value
            if not last:
                high, low = halves(value)
                stacked[part, :COLS] = high
                stacked[part, COLS:] = low

        def finish_images():
            images[before] = images[before] * scale
            image = images[j] * scale
            for i in range(ITERS - 1):
                image = image - entries[i] * images[i]
            images[j] = image

        spread_down(1, finish)
        return finish_images

    def iteration(j, carry):
        before = jnp.maximum(j - 1, 0)

        def at_first(*steps):
            @pl.when(j == 0)
            def _():
                for step in steps:
                    step()

        def in_m_tree():
            at_first(
                lambda: pad_tree(0, 3, LEVELS), lambda: compose(0),
                lambda: pad_tree(1, 0, LEVELS), lambda: turn_rows(0),
            )

            @pl.when(j > 0)
            def _():
                finish_images = settle(before)
                sums_ref[...] = partial_sums(before)
                block_product(0)
                leaf_terms(1, direct[...], sums_ref[...])
                send_leaf(1)
                finish_images()

        low = tree(
            0, lambda: fresh_m[...], False,
            while_z=in_m_tree, while_x=lambda: at_first(lambda: pass_joins(0)),
        )
        send_down(0, low)
        at_first(lambda: end_joins(0))
        finished(leaf_copies(1))
        for i in range(GROUP):
            fresh_a[i] = a_slot[1, i] + joined_rows(0, low[i], i)

        def in_a_tree():
            at_first(lambda: turn_rows(1), lambda: compose(1))
            d = down_copies(0)
            finished(d)

            def to_image(part, value):
                images[j, part, :] = value
                high, low = halves(value)
                stacked[part, :COLS] = high
                stacked[part, COLS:] = low

            spread_down(0, to_image)
            at_first(loads["e1"].wait)
            block_product(1)

            @pl.when(j < ITERS - 1)
            def _():
                leaf_terms(0, direct[...])
                send_leaf(0)

        low = tree(
            1, lambda: fresh_a[...], True,
            while_z=in_a_tree, while_x=lambda: at_first(lambda: pass_joins(1)),
        )
        send_down(1, low + riding(x_slot[1])[None])
        at_first(lambda: end_joins(1))

        @pl.when(j < ITERS - 1)
        def _():
            finished(leaf_copies(0))
            sums = jnp.sum(x_slot[1, :, :, COLS:], axis=0)
            norm, scale, entries = column_entries(
                lambda i: sums[:, RANK - COLS + i : RANK - COLS + i + 1], j - 1
            )
            scale = jnp.where(j == 0, jnp.ones_like(scale), scale)
            carried[before] = carried[before] * scale[None]
            for i in range(GROUP):
                value = (a_slot[0, i] + joined_rows(1, low[i], i)) * scale
                for earlier in range(ITERS - 2):
                    value = value - entries[earlier] * carried[earlier, i]
                fresh_m[i] = value
            carried[j] = fresh_m[...]

        return carry

    loads["rhs"].wait()
    loads["q0"].wait()
    leaf_terms(0, mixed[...])
    pl.semaphore_wait(barrier, len(peers))
    send_leaf(0)
    loads["p0"].wait()
    loads["q1"].wait()
    begin_joins(0)
    pad_tree(0, 0, 3)
    loads["e0"].wait()
    block_product(0)
    leaf_terms(1, direct[...], sums_ref[...])
    send_leaf(1)
    loads["p1"].wait()
    begin_joins(1)
    finished(leaf_copies(0))
    fresh_m[...] = a_slot[0]
    lax.fori_loop(0, ITERS, iteration, 0)
    finish_images = settle(ITERS - 1, last=True)

    earlier_norm = hs[(ITERS - 2) * (ITERS + 1)]
    shrink = 1.0 / earlier_norm
    which = [(0, 3), (1, 3), (2, 3), (2, 2), (3, 3), (0, 0), (0, 1), (0, 2), (1, 1), (1, 2)]
    step = 64

    def one_step(t, carry):
        rows = pl.ds(pl.multiple_of(t * step, step), step)
        parts = [basis[i, rows, :] for i in range(ITERS)] + [mixed[rows, :] * shrink]
        out = []
        for (first, second), total in zip(which, carry):
            term = jnp.sum((parts[first] * parts[second]).reshape(step // 8, 8, COLS), axis=0)
            high, low = two_sum(total[0], term)
            out.append((high, total[1] + low))
        return tuple(out)

    nothing = jnp.zeros((8, COLS), F32)
    sums = lax.fori_loop(0, WIDTH // step, one_step, ((nothing, nothing),) * len(which))
    highs, lows = [], []
    for total in sums:
        for shift in (4, 2, 1):
            total = add_exact(total, tuple(pltpu.roll(x, shift, 0) for x in total))
        highs.append(total[0][0:1])
        lows.append(total[1][0:1])
    rest = [jnp.zeros((SUMS - len(which), COLS), F32)]
    totals = total_of(
        jnp.concatenate(highs + rest, axis=0),
        jnp.concatenate(lows + rest, axis=0),
        finish_images,
    )
    inner = {
        pair: (totals[i : i + 1], totals[SUMS + i : SUMS + i + 1]) for i, pair in enumerate(which)
    }
    norm = jnp.sqrt(inner[2, 2][0] + EPSILON)
    hs[(ITERS - 1) * (ITERS + 1)] = norm
    lead = earlier_norm / norm
    weights_of = []
    for i in range(ITERS):
        entry = inner[i, ITERS][0] * lead
        if i == ITERS - 1:
            entry = entry / norm
        hs[(ITERS - 1) * (ITERS + 1) + 1 + i] = entry
        weights_of.append(-entry if i < ITERS - 1 else -(entry / norm))
    weights_of.append(lead)
    square = None
    for first, second in which:
        plain = (weights_of[first], jnp.zeros_like(norm))
        other = (weights_of[second], jnp.zeros_like(norm))
        term = times_exact(times_exact(plain, other), inner[first, second])
        if first != second:
            term = (2.0 * term[0], 2.0 * term[1])
        square = term if square is None else add_exact(square, term)
    last_norm = jnp.sqrt(jnp.maximum(square[0], jnp.zeros_like(norm)) + EPSILON)
    scale = 1.0 / norm
    zero = jnp.zeros((1, COLS), F32)
    entries = [[zero for column in range(ITERS)] for line in range(ITERS + 1)]
    for column in range(ITERS):
        for line in range(column + 1):
            entries[line][column] = hs[column * (ITERS + 1) + 1 + line]
        if column + 1 < ITERS:
            entries[column + 1][column] = hs[(column + 1) * (ITERS + 1)]
        else:
            entries[column + 1][column] = last_norm
    weights = least_squares(entries, hs[0])
    weights[ITERS - 1] = weights[ITERS - 1] * scale
    sol_ref[...] = weights[0] * images[0] + weights[1] * images[1] + weights[2] * images[2]
    for line in range(ITERS + 1):
        for column in range(ITERS):
            hess_ref[column, line : line + 1, :] = entries[line][column]


def solution(mesh):
    dma = pltpu.SemaphoreType.DMA
    tree = (2, GROUP, SLICE, LANES)
    scratch = [
        pltpu.VMEM((2, WIDTH, WIDTH), BF16),
        pltpu.VMEM((2, RANK, WIDTH), BF16),
        pltpu.VMEM((2, WIDTH, LANES), BF16),
        pltpu.VMEM((2, RANK, WIDTH), BF16),
        pltpu.VMEM((2, LEVELS, 2, RANK, RANK), BF16),
        pltpu.VMEM((2, LEVELS, 2, RANK, RANK), BF16),
        pltpu.VMEM((2, LEVELS, 2 * LANES, LANES), BF16),
        pltpu.VMEM((2, LEVELS, 2, LANES, LANES), BF16),
        pltpu.VMEM((ITERS, WIDTH, COLS), F32),
        pltpu.VMEM((ITERS, WIDTH, COLS), F32),
        pltpu.VMEM((WIDTH, COLS), F32),
        pltpu.VMEM((WIDTH, COLS), F32),
        pltpu.VMEM((WIDTH, 2 * COLS), BF16),
        pltpu.VMEM(tree, F32),
        pltpu.VMEM(tree, F32),
        pltpu.VMEM((2, SLICE, LANES), F32),
        pltpu.VMEM((2, DEEP, SLICE, LANES), F32),
        pltpu.VMEM((2, SLICE, LANES), F32),
        pltpu.VMEM((2, OUTER, SLICE, LANES), F32),
        pltpu.VMEM(tree, F32),
        pltpu.VMEM(tree, F32),
        pltpu.VMEM((4, SLICE, LANES), F32),
        pltpu.VMEM((2, SLICE, LANES), F32),
        pltpu.VMEM((4, SLICE, LANES), F32),
        pltpu.VMEM((2, SLICE, LANES), F32),
        pltpu.VMEM((8, SLICE, LANES), F32),
        pltpu.VMEM((4, SLICE, LANES), F32),
        pltpu.VMEM((2, SLICE, LANES), F32),
        pltpu.VMEM((3, 2 * SUMS, COLS), F32),
        pltpu.VMEM((GROUP, 2 * SUMS, COLS), F32),
        pltpu.VMEM((DEEP, 2 * SUMS, COLS), F32),
        pltpu.VMEM((OUTER, 2 * SUMS, COLS), F32),
        pltpu.VMEM((ITERS * (ITERS + 1), 1, COLS), F32),
        pltpu.VMEM((8, COLS), F32),
        pltpu.VMEM((2, GROUP, RANK, LANES), F32),
        pltpu.VMEM((2, GROUP, 2, LANES, LANES), BF16),
        pltpu.VMEM((ITERS,) + tree[1:], F32),
        pltpu.VMEM(tree[1:], F32),
        pltpu.VMEM(tree[1:], F32),
        pltpu.VMEM((ITERS - 1, WIDTH, COLS), F32),
        pltpu.VMEM((2, 2, 3 * LANES, LANES), BF16),
        dma((11,)),
        dma((2, GROUP - 1)),
        dma((2, GROUP - 1)),
        dma((2, DEEP - 1)),
        dma((2, DEEP - 1)),
        dma((2, OUTER - 1)),
        dma((2, OUTER - 1)),
        dma((2, GROUP - 1)),
        dma((2, GROUP - 1)),
        dma((GROUP - 1,)),
        dma((GROUP - 1,)),
        dma((DEEP - 1,)),
        dma((DEEP - 1,)),
        dma((OUTER - 1,)),
        dma((OUTER - 1,)),
        dma((2, 7)),
        dma((2, 7)),
    ]

    def hand_over(sol_in, hess_in, sol_out, hess_out):
        sol_out[...] = sol_in[...]
        hess_out[...] = hess_in[...]

    def on_device(*args):
        both = pl.pallas_call(
            kernel,
            out_shape=(
                jax.ShapeDtypeStruct((WIDTH, COLS), F32),
                jax.ShapeDtypeStruct((ITERS, ITERS + 1, COLS), F32),
            ),
            in_specs=[pl.BlockSpec(memory_space=pl.ANY)] * 11,
            out_specs=[pl.BlockSpec(memory_space=pltpu.VMEM)] * 2,
            scratch_shapes=scratch,
            compiler_params=pltpu.CompilerParams(
                collective_id=0, has_side_effects=True, vmem_limit_bytes=60 * 2**20
            ),
        )(*args)
        sol, hess = pl.pallas_call(
            hand_over,
            out_shape=tuple(jax.ShapeDtypeStruct(x.shape, x.dtype) for x in both),
            in_specs=[pl.BlockSpec(memory_space=pltpu.VMEM)] * 2,
            out_specs=[pl.BlockSpec(memory_space=pltpu.VMEM)] * 2,
        )(*both)
        return sol, jnp.swapaxes(hess, 0, 1)

    leaf = P("leaf", None)
    block = P("leaf", None, None)
    in_specs = (leaf, block, block, block, P(), P(), block, block, block, P(), P())
    return jax.shard_map(
        on_device, mesh=mesh, in_specs=in_specs, out_specs=(leaf, P()), check_vma=False
    )
```
